128 devices in a mesh: data: 1, model: 128 (over z, y, x, core).
Axes of the slice: x: 4, y: 4, z: 4, core: 2. Of those that a mesh axis runs over, the one named last changes fastest.
Arguments:
- hidden: bfloat16 [64, 4096], P('data')
- w_head: bfloat16 [4096, 32768], P(None, 'model')
- store_keys: bfloat16 [131072, 4096], P('model')
- store_tok: int32 [131072], P('model')
- range_bounds: int32 [128, 129], P('model')
- temperature: float32 [], replicated
- mix_weight: float32 [], replicated
Outputs:
- output: float32 [64, 32768], P('data', 'model')
All inputs are finite; a program needn't handle non-finite values.
Results may differ from the reference program's by a relative error of at most 0.001.
Values are sent between devices in bfloat16 or wider.
A program may use at most 1 GiB of HBM per device.

```python
import jax
import jax.numpy as jnp
from jax import lax

GROUP_SIZE = 128
BATCH_ROWS = 64
MODEL_DIM = 4096
VOCAB_SIZE = 32768
STORE_LOCAL = 1024


def draw_store_tokens(stream):
    shard_width = VOCAB_SIZE // GROUP_SIZE
    weight_key, first_key, second_key = jax.random.split(stream, 3)
    shard_ids = jnp.arange(GROUP_SIZE, dtype=jnp.int32)
    zipf_weight = (4 * GROUP_SIZE) // (shard_ids + 4)
    weights = jax.random.randint(weight_key, (GROUP_SIZE, GROUP_SIZE), 1, 5, jnp.int32) * zipf_weight[None, :]
    cum_weight = jnp.concatenate([jnp.zeros((GROUP_SIZE, 1), jnp.int32), jnp.cumsum(weights, axis=1)], axis=1)
    range_bounds = (STORE_LOCAL * cum_weight) // cum_weight[:, GROUP_SIZE:]
    positions = jnp.arange(STORE_LOCAL, dtype=jnp.int32)
    owner_shard = jax.vmap(lambda bound_row: jnp.searchsorted(bound_row[1:GROUP_SIZE], positions, side='right'))(range_bounds)
    column = jnp.minimum(
        jax.random.randint(first_key, (GROUP_SIZE, STORE_LOCAL), 0, shard_width, jnp.int32),
        jax.random.randint(second_key, (GROUP_SIZE, STORE_LOCAL), 0, shard_width, jnp.int32))
    store_tok = jnp.sort(owner_shard.astype(jnp.int32) * shard_width + column, axis=1)
    return store_tok.reshape(GROUP_SIZE * STORE_LOCAL).astype(jnp.int32), range_bounds.astype(jnp.int32)


def setup_inputs(seed: int = 0, part: int = 0) -> dict:
    root_key = jax.random.key(seed)
    streams = jax.random.split(root_key, 7)
    hidden = jax.random.normal(jax.random.fold_in(streams[0], part), (BATCH_ROWS, MODEL_DIM), jnp.float32)
    head_scale = 2.5 * MODEL_DIM ** -0.5

    def draw_head_rows(row_stream):
        draw = jax.random.normal(row_stream, (128, VOCAB_SIZE), jnp.float32)
        return (draw * head_scale).astype(jnp.bfloat16)

    w_head = lax.map(draw_head_rows, jax.random.split(streams[1], MODEL_DIM // 128)).reshape(MODEL_DIM, VOCAB_SIZE)
    spread = jax.random.uniform(streams[2], (GROUP_SIZE,), jnp.float32, -1.0, 1.0)
    key_scale = jnp.sqrt(1.0 + 2.5 * spread * MODEL_DIM ** -0.5)

    def draw_shard(stream_and_scale):
        shard_stream, shard_scale = stream_and_scale
        draw = jax.random.normal(shard_stream, (STORE_LOCAL, MODEL_DIM), jnp.float32)
        return (draw * shard_scale).astype(jnp.bfloat16)

    store_keys = lax.map(draw_shard, (jax.random.split(streams[3], GROUP_SIZE), key_scale))
    store_keys = store_keys.reshape(GROUP_SIZE * STORE_LOCAL, MODEL_DIM)
    store_tok, range_bounds = draw_store_tokens(streams[4])
    temperature = jax.random.uniform(streams[5], (), jnp.float32, 2.0, 3.0) * MODEL_DIM ** 0.5
    mix_weight = jax.random.uniform(streams[6], (), jnp.float32, 0.2, 0.7)
    return {'hidden': hidden.astype(jnp.bfloat16), 'w_head': w_head, 'store_keys': store_keys,
            'store_tok': store_tok, 'range_bounds': range_bounds,
            'temperature': temperature, 'mix_weight': mix_weight}


def reference(hidden, w_head, store_keys, store_tok, range_bounds, temperature, mix_weight):
    shard_width = VOCAB_SIZE // GROUP_SIZE
    keys_shards = store_keys.reshape(GROUP_SIZE, STORE_LOCAL, MODEL_DIM)

    def shard_scores(keys_local):
        keys_wide = keys_local.astype(jnp.float32)
        key_norm = jnp.sum(keys_wide * keys_wide, axis=1)
        cross_dot = jnp.dot(keys_local, hidden.T, preferred_element_type=jnp.float32)
        return (2.0 * cross_dot - key_norm[:, None]) / temperature

    scores = lax.map(shard_scores, keys_shards).reshape(GROUP_SIZE * STORE_LOCAL, BATCH_ROWS)
    row_max = jnp.max(scores, axis=0)
    kernel = jnp.exp(scores - row_max[None, :])
    knn_total = jnp.sum(kernel, axis=0)
    tok_grid = store_tok.reshape(GROUP_SIZE, STORE_LOCAL)
    owner = tok_grid // shard_width
    range_lo = jnp.take_along_axis(range_bounds, owner, axis=1)
    range_hi = jnp.take_along_axis(range_bounds, owner + 1, axis=1)
    positions = jnp.arange(STORE_LOCAL)[None, :]
    counted = (positions >= range_lo) & (positions < range_hi)
    segment = jnp.where(counted, tok_grid, VOCAB_SIZE).reshape(GROUP_SIZE * STORE_LOCAL)
    hist_full = jax.ops.segment_sum(kernel, segment, num_segments=VOCAB_SIZE + 1)[:VOCAB_SIZE]
    knn_prob = hist_full.T / knn_total[:, None]
    logits = jnp.dot(hidden, w_head, preferred_element_type=jnp.float32)
    lm_max = jnp.max(logits, axis=1, keepdims=True)
    lm_exp = jnp.exp(logits - lm_max)
    lm_prob = lm_exp / jnp.sum(lm_exp, axis=1, keepdims=True)
    return jnp.log(mix_weight * knn_prob + (1.0 - mix_weight) * lm_prob)
```

```python
import functools

import jax
import jax.numpy as jnp
from jax import lax
from jax.experimental import pallas as pl
from jax.experimental.pallas import tpu as pltpu
from jax.sharding import PartitionSpec as P

F32, BF16, I32 = jnp.float32, jnp.bfloat16, jnp.int32
SLOT_AXIS = (0, 1, 2, 0)
LN, EN = 128, 1024
NT = (((1,), (1,)), ((), ()))


def iota(shape, axis):
    return lax.broadcasted_iota(I32, shape, axis)


def coordinates(n):
    device = lax.axis_index('model')
    return device, device % 2, (device // 2) % n, (device // (2 * n)) % n, device // (2 * n * n)


def local_kernel(n, tok_ref, bounds_ref, tau_ref, hid_hbm, w_hbm, keys_hbm, rows_out, logits_out, tab_out,
                 hid, w, keys, score, dedup, onehot, lohot, e3, in_sem, key_sem):
    inner = 2 * n * n
    _, _, cx, cy, cz = coordinates(n)
    in_copies = (pltpu.make_async_copy(hid_hbm, hid, in_sem.at[0]), pltpu.make_async_copy(w_hbm, w, in_sem.at[1]))
    for c in in_copies:
        c.start()
    kchunk = LN
    nk = keys.shape[0] // kchunk

    def key_copy(c):
        rows = pl.ds(c * kchunk, kchunk)
        return pltpu.make_async_copy(keys_hbm.at[rows], keys.at[rows], key_sem.at[c])

    for c in range(nk):
        key_copy(c).start()

    lane = iota((8, LN), 1)
    sub = iota((8, LN), 0)
    pos = sub * LN + lane

    def prev(a):
        r = pltpu.roll(a, 1, 1)
        return jnp.where(lane == 0, pltpu.roll(r, 1, 0), r)

    tok = tok_ref[...]
    first = ((tok != prev(tok)) | (pos == 0)).astype(I32)
    c = first
    for sh in (1, 2, 4, 8, 16, 32, 64):
        c = c + jnp.where(lane >= sh, pltpu.roll(c, sh, 1), 0)
    tot = jnp.broadcast_to(c[:, 127:LN], (8, LN))
    acc = tot
    for sh in (1, 2, 4):
        acc = acc + jnp.where(sub >= sh, pltpu.roll(acc, sh, 0), 0)
    rank = c + acc - tot - 1

    owner = tok // 256
    bnd = bounds_ref[...]
    nb = bnd.shape[1] - 1
    lo_b = jnp.broadcast_to(bnd[:, :nb], (8, nb))
    hi_b = jnp.broadcast_to(bnd[:, 1:], (8, nb))
    if nb < LN:
        lo_b = jnp.concatenate([lo_b, jnp.zeros((8, LN - nb), I32)], axis=1)
        hi_b = jnp.concatenate([hi_b, jnp.zeros((8, LN - nb), I32)], axis=1)
    counted = (pos >= jnp.take_along_axis(lo_b, owner, axis=1)) & (pos < jnp.take_along_axis(hi_b, owner, axis=1))
    rank_d = jnp.where(counted, rank, -1)
    for t in range(8):
        rows = iota((EN, LN), 0)
        dedup[:, t * LN:(t + 1) * LN] = jnp.where(rank_d[t:t + 1, :] == rows, 1.0, 0.0).astype(BF16)

    h = tok // LN
    tile_first = ((h != prev(h)) | (pos == 0)).astype(I32)
    half = h % 2
    jc = owner % 2
    jp = ((owner // 2) % n, (owner // (2 * n)) % n, owner // (2 * n * n))
    lo = tok % LN
    val = (first * (rank % LN + 1) * (1 + 255 * half)).astype(F32)
    starts = [(tile_first * jnp.where(half == hf, part, 0)).astype(F32)
              for hf in range(2) for part in (rank // LN, rank % LN)]
    sub32 = iota((32, LN), 0)
    for t in range(8):
        cols = slice(t * LN, (t + 1) * LN)
        r = slice(t, t + 1)
        lohot[0:LN, cols] = jnp.where(lo[r, :] == iota((LN, LN), 0), val[r, :], 0.0).astype(BF16)
        lohot[LN:160, cols] = jnp.where(
            sub32 < 8, starts[0][r, :], jnp.where(sub32 < 16, starts[1][r, :], jnp.where(
                sub32 < 24, starts[2][r, :], starts[3][r, :]))).astype(BF16)
    coord = (cx, cy, cz)
    for a, (b2, b3) in enumerate(((2, 1), (2, 0), (1, 0))):
        row = ((jp[a] - coord[a] + n) % n) * inner + jp[b2] * (2 * n) + jp[b3] * 2 + jc
        for t in range(8):
            onehot[:, t * LN:(t + 1) * LN] = jnp.where(
                row[t:t + 1, :] == iota((LN, LN), 0), 1.0, 0.0).astype(BF16)
        tb = lax.dot_general(onehot[...], lohot[0:LN, :], NT, preferred_element_type=F32).astype(I32)
        us = lax.dot_general(lohot[LN:160, :], onehot[...], NT, preferred_element_type=F32).astype(I32)
        for d in range(n):
            tab_out[a, d, 0:inner, :] = tb[d * inner:(d + 1) * inner, :]
            for hf in range(2):
                tab_out[a, d, inner + hf:inner + hf + 1, :] = us[16 * hf:16 * hf + 1] * LN + us[16 * hf + 8:16 * hf + 9]

    for c in in_copies:
        c.wait()
    lg = jnp.dot(hid[...], w[...], preferred_element_type=F32)
    logits_out[...] = lg
    lm = jnp.max(lg, axis=1, keepdims=True)
    lz = jnp.sum(jnp.exp(lg - lm), axis=1, keepdims=True)

    tau = tau_ref[0]

    def score_step(c, carry):
        key_copy(2 * c).wait()
        key_copy(2 * c + 1).wait()
        rows = pl.ds(c * 256, 256)
        cross = lax.dot_general(hid[...], keys[rows, :], NT, preferred_element_type=F32)
        sq = jnp.zeros((256, LN), F32)
        for t in range(keys.shape[1] // LN):
            k = keys[rows, t * LN:(t + 1) * LN].astype(F32)
            sq = sq + k * k
        norm = jnp.sum(sq.T, axis=0, keepdims=True)
        sc = (2.0 * cross - norm) / tau
        score[2 * c] = sc[:, :LN]
        score[2 * c + 1] = sc[:, LN:]
        return carry

    lax.fori_loop(0, nk // 2, score_step, 0)

    sc = [score[t] for t in range(8)]
    m = jnp.max(functools.reduce(jnp.maximum, sc), axis=1, keepdims=True)
    z = jnp.zeros((64, LN), F32)
    for t in range(8):
        e = jnp.exp(sc[t] - m)
        z = z + e
        hi = e.astype(BF16)
        r1 = e - hi.astype(F32)
        mid = r1.astype(BF16)
        low = (r1 - mid.astype(F32)).astype(BF16)
        cols = slice(t * LN, (t + 1) * LN)
        e3[0:64, cols] = hi
        e3[64:LN, cols] = mid
        e3[LN:192, cols] = low
    z = jnp.sum(z, axis=1, keepdims=True)
    l64 = iota((64, LN), 1)
    stat = jnp.where(l64 == 0, m, jnp.where(l64 == 1, z, jnp.where(l64 == 2, lm, lz)))
    for q in range(8):
        rows_out[q // 4, q % 4, 8] = stat[q * 8:(q + 1) * 8, :]
    for c in range(4):
        dd = lax.dot_general(e3[...], dedup[c * 256:(c + 1) * 256, :], NT, preferred_element_type=F32)
        eu = dd[0:64] + (dd[64:LN] + dd[LN:192])
        for q in range(8):
            rows_out[q // 4, q % 4, 2 * c] = eu[q * 8:(q + 1) * 8, :LN]
            rows_out[q // 4, q % 4, 2 * c + 1] = eu[q * 8:(q + 1) * 8, LN:]


def exchange_kernel(n, own_rows, logits, own_tab, lam_ref, out_ref,
                    tab_pair, tab, tab_smem, lists0, lists1, lists2, lists3, part2, recv2, part3, recv3, fin, fin_in,
                    swap_sem, tab_send, tab_recv, smem_sem,
                    send1, recv1, send2, recv2_sem, send3, recv3_sem, fin_sem):
    inner = 2 * n * n
    block = 4 * n
    device, core, cx, cy, cz = coordinates(n)
    other = 1 - core
    partner = device + 1 - 2 * core
    coord = (cx + core * (cy - cx), cy + core * (cx - cy), cz)
    stride = (2 + core * (2 * n - 2), 2 * n + core * (2 - 2 * n), 2 * n * n)
    pcoord, pstride = (cx, cy, cz), (2, 2 * n, 2 * n * n)
    axis_of = (core, 1 - core, 2)
    row_stride = ((2, 2 * n), (2 * n, 2), (2 + core * (2 * n - 2), 2 * n + core * (2 - 2 * n)))

    def peer(v, d):
        return device + stride[v] * ((coord[v] + d) % n - coord[v])

    def remote(src, dst, ssem, rsem, dev):
        return pltpu.make_async_remote_copy(src_ref=src, dst_ref=dst, send_sem=ssem, recv_sem=rsem,
                                            device_id={'model': dev}, device_id_type=pl.DeviceIdType.MESH)

    lists = (lists0, lists1, lists2, lists3)
    far_first = sorted(range(1, n), key=lambda d: -min(d, n - d))
    lane = iota((8, LN), 1)

    barrier = pltpu.get_barrier_semaphore()
    partners = [partner] + [peer(v, d) for v in range(3) for d in range(1, n)]
    for p in partners:
        pl.semaphore_signal(barrier, inc=1, device_id={'model': p}, device_id_type=pl.DeviceIdType.MESH)
    pl.semaphore_wait(barrier, len(partners))

    tab_swap = remote(own_tab, tab_pair, swap_sem.at[0, 4], swap_sem.at[1, 4], partner)
    tab_swap.start()
    swaps = [remote(own_rows.at[other, s], lists[s].at[0], swap_sem.at[0, s], swap_sem.at[1, s], partner)
             for s in range(4)]
    for c in swaps:
        c.start()

    def tab_copy(a, d, l):
        src = own_tab if l == 0 else tab_pair
        return remote(src.at[a, d], tab.at[a, n - d - 1, l], tab_send.at[a, d - 1, l], tab_recv.at[a, n - d - 1, l],
                      device + pstride[a] * ((pcoord[a] + d) % n - pcoord[a]))

    def copy1(s, d, l):
        src = own_rows.at[core, s] if l == 0 else lists[s].at[0]
        return remote(src, lists[s].at[2 * (n - d) - 1 + l], send1.at[s, d - 1, l], recv1.at[s, n - d - 1, l],
                      peer(SLOT_AXIS[s], d))

    for d in far_first:
        for a in range(3):
            tab_copy(a, d, 0).start()
    for d in far_first:
        for s in range(4):
            copy1(s, d, 0).start()
    tab_swap.wait_recv()
    for d in far_first:
        for a in range(3):
            tab_copy(a, d, 1).start()
    for s in range(4):
        swaps[s].wait_recv()
        for d in far_first:
            copy1(s, d, 1).start()

    def tab_of(a, k, l):
        if k:
            return tab.at[a, k - 1, l]
        return (tab_pair if l else own_tab).at[a, 0]

    def list_of(s, k, l):
        if k == 0 and l == 0:
            return own_rows.at[core, s]
        return lists[s].at[2 * k - 1 + l]

    for d in range(1, n):
        for a in range(3):
            for l in range(2):
                tab_copy(a, d, l).wait_recv()
    smem_copies = [pltpu.make_async_copy(tab_of(a, k, l).at[pl.ds(inner, 2)], tab_smem.at[a, k, l], smem_sem.at[a, k, l])
                   for a in range(3) for k in range(n) for l in range(2)]
    for c in smem_copies:
        c.start()
    for c in smem_copies:
        c.wait()

    def stats(tiles):
        ms = [jnp.broadcast_to(t[:, 0:1], (8, LN)) for t in tiles]
        ls = [jnp.broadcast_to(t[:, 2:3], (8, LN)) for t in tiles]
        mm = functools.reduce(jnp.maximum, ms)
        ll = functools.reduce(jnp.maximum, ls)
        fs = [jnp.exp(a - mm) for a in ms]
        gs = [jnp.exp(a - ll) for a in ls]
        zz = sum(f * t[:, 1:2] for f, t in zip(fs, tiles))
        lzz = sum(g * t[:, 3:4] for g, t in zip(gs, tiles))
        return fs, jnp.where(lane == 0, mm, jnp.where(lane == 1, zz, jnp.where(lane == 2, ll, lzz)))

    def copy2(s, d):
        return remote(part2.at[s, d], recv2.at[s, n - d - 1], send2.at[s, d - 1], recv2_sem.at[s, n - d - 1],
                      peer((SLOT_AXIS[s] + 1) % 3, d))

    def copy3(s, d):
        return remote(part3.at[s, d], recv3.at[s, n - d - 1], send3.at[s, d - 1], recv3_sem.at[s, n - d - 1],
                      peer((SLOT_AXIS[s] + 2) % 3, d))

    src = [(k, l) for k in range(n) for l in range(2)]
    for s in range(4):
        v = SLOT_AXIS[s]
        a = axis_of[v]
        c2, c3 = coord[(v + 1) % 3], coord[(v + 2) % 3]
        s2, s3 = row_stride[v]
        for d in range(1, n):
            for l in range(2):
                copy1(s, d, l).wait_recv()
        fs, stat_tile = stats([list_of(s, k, l)[8] for k, l in src])
        for d2 in far_first + [0]:
            a2 = (c2 + d2) % n

            def pair_step(q, carry, s=s, a=a, a2=a2, c3=c3, s2=s2, s3=s3, d2=d2, fs=fs):
                row = a2 * s2 + ((c3 + q // 2) % n) * s3 + q % 2
                acc = [jnp.zeros((8, LN), F32)] * 2
                for i, (k, l) in enumerate(src):
                    entries = list_of(s, k, l)
                    packed = jnp.broadcast_to(tab_of(a, k, l)[pl.ds(row, 1), :], (8, LN))
                    for hf in range(2):
                        u = tab_smem[a, k, l, hf, ((n - k) % n) * inner + row]
                        kt = u // LN
                        merged = jnp.where(lane >= u % LN, entries[kt], entries[kt + 1])
                        idx = packed // 256 if hf else packed % 256
                        got = jnp.take_along_axis(merged, jnp.maximum(idx - 1, 0), axis=1)
                        acc[hf] = acc[hf] + jnp.where(idx > 0, got, 0.0) * fs[i]
                part2[s, d2, 2 * q] = acc[0]
                part2[s, d2, 2 * q + 1] = acc[1]
                return carry

            lax.fori_loop(0, 2 * n, pair_step, 0)
            part2[s, d2, block] = stat_tile
            if d2:
                copy2(s, d2).start()

    for s in range(4):
        for d in range(1, n):
            copy2(s, d).wait_recv()
        parts = [part2.at[s, 0]] + [recv2.at[s, k] for k in range(n - 1)]
        fs, stat_tile = stats([p[block] for p in parts])
        for d3 in far_first + [0]:
            for ch in range(4):
                part3[s, d3, ch] = sum(f * p[d3 * 4 + ch] for f, p in zip(fs, parts))
            part3[s, d3, 4] = stat_tile
            if d3:
                copy3(s, d3).start()

    for s in range(4):
        for d in range(1, n):
            copy3(s, d).wait_recv()
        parts = [part3.at[s, 0]] + [recv3.at[s, k] for k in range(n - 1)]
        fs, stat_tile = stats([p[4] for p in parts])
        for ch in range(4):
            fin[ch // 2, s, ch % 2] = sum(f * p[ch] for f, p in zip(fs, parts))
        for c in range(2):
            fin[c, s, 2] = stat_tile

    back = remote(fin.at[other], fin_in, fin_sem.at[0], fin_sem.at[1], partner)
    back.start()
    lam = lam_ref[0]

    def finish(block_ref, rows_half):
        for s in range(4):
            st = block_ref[s, 2]
            zz, ll, lzz = st[:, 1:2], st[:, 2:3], st[:, 3:4]
            rows = pl.ds(pl.multiple_of(rows_half * 32 + s * 8, 8), 8)
            for hf in range(2):
                cols = slice(hf * LN, (hf + 1) * LN)
                lm_exp = jnp.exp(logits[rows, cols] - ll)
                out_ref[rows, cols] = jnp.log(lam * (block_ref[s, hf] / zz) + (1.0 - lam) * (lm_exp / lzz))

    finish(fin.at[core], core)
    back.wait_recv()
    finish(fin_in, other)

    tab_swap.wait_send()
    for c in swaps:
        c.wait_send()
    back.wait_send()
    for d in range(1, n):
        for l in range(2):
            for a in range(3):
                tab_copy(a, d, l).wait_send()
            for s in range(4):
                copy1(s, d, l).wait_send()
        for s in range(4):
            copy2(s, d).wait_send()
            copy3(s, d).wait_send()


def step(n, hidden, w_local, keys_local, tok_local, bounds_local, tau, lam):
    tab_rows = 2 * n * n + 8
    block = 4 * n
    dim = hidden.shape[1]
    V, DMA = pltpu.VMEM, pltpu.SemaphoreType.DMA
    vm = pl.BlockSpec(memory_space=pltpu.VMEM)
    sm = pl.BlockSpec(memory_space=pltpu.SMEM)
    hbm = pl.BlockSpec(memory_space=pl.ANY)
    rows, logits, tab = pl.pallas_call(
        functools.partial(local_kernel, n),
        out_shape=(jax.ShapeDtypeStruct((2, 4, 9, 8, LN), F32), jax.ShapeDtypeStruct((64, 256), F32),
                   jax.ShapeDtypeStruct((3, n, tab_rows, LN), I32)),
        in_specs=[vm, vm, sm, hbm, hbm, hbm],
        out_specs=(vm, vm, vm),
        scratch_shapes=[
            V((64, dim), BF16), V((dim, 256), BF16), V((EN, dim), BF16), V((8, 64, LN), F32),
            V((EN, EN), BF16), V((LN, EN), BF16), V((160, EN), BF16), V((192, EN), BF16),
            DMA((2,)), DMA((8,))],
        name='local_scores',
    )(tok_local.reshape(8, LN), bounds_local, tau.reshape(1), hidden, w_local, keys_local)
    return pl.pallas_call(
        functools.partial(exchange_kernel, n),
        out_shape=jax.ShapeDtypeStruct((64, 256), F32),
        in_specs=[vm, vm, vm, sm],
        out_specs=vm,
        scratch_shapes=[
            V((3, n, tab_rows, LN), I32), V((3, n - 1, 2, tab_rows, LN), I32), pltpu.SMEM((3, n, 2, 2, LN), I32),
            *[V((2 * n - 1, 9, 8, LN), F32)] * 4, V((4, n, block + 1, 8, LN), F32), V((4, n - 1, block + 1, 8, LN), F32),
            V((4, n, 5, 8, LN), F32), V((4, n - 1, 5, 8, LN), F32), V((2, 4, 3, 8, LN), F32), V((4, 3, 8, LN), F32),
            DMA((2, 5)), DMA((3, n - 1, 2)), DMA((3, n - 1, 2)), DMA((3, n, 2)),
            DMA((4, n - 1, 2)), DMA((4, n - 1, 2)), DMA((4, n - 1)), DMA((4, n - 1)), DMA((4, n - 1)), DMA((4, n - 1)),
            DMA((2,))],
        compiler_params=pltpu.CompilerParams(collective_id=0, has_side_effects=True),
        name='exchange',
    )(rows, logits, tab, lam.reshape(1))


def solution(mesh):
    n = round((mesh.shape['model'] // 2) ** (1 / 3))
    return jax.shard_map(functools.partial(step, n), mesh=mesh,
                         in_specs=(P('data', None), P(None, 'model'), P('model', None), P('model'),
                                   P('model', None), P(), P()),
                         out_specs=P('data', 'model'), check_vma=False)
```

```python
import functools

import jax
import jax.numpy as jnp
from jax import lax
from jax.experimental import pallas as pl
from jax.experimental.pallas import tpu as pltpu
from jax.sharding import PartitionSpec as P

F32, BF16, I32 = jnp.float32, jnp.bfloat16, jnp.int32
GROUPS = ((0, 16), (16, 8), (24, 8))
HALF = 32
LN, EN = 128, 1024
NT = (((1,), (1,)), ((), ()))


def iota(shape, axis):
    return lax.broadcasted_iota(I32, shape, axis)


def coordinates(n):
    device = lax.axis_index('model')
    return device, device % 2, (device // 2) % n, (device // (2 * n)) % n, device // (2 * n * n)


def local_kernel(n, tok_ref, bounds_ref, tau_ref, hid_hbm, w_hbm, keys_hbm, rows0, rows1, rows2, stat_out, logits_out, tab_out,
                 hid, w, keys, score, dedup, onehot, lohot, e3, in_sem, key_sem):
    inner = 2 * n * n
    _, _, cx, cy, cz = coordinates(n)
    in_copies = (pltpu.make_async_copy(hid_hbm, hid, in_sem.at[0]), pltpu.make_async_copy(w_hbm, w, in_sem.at[1]))
    for c in in_copies:
        c.start()
    kchunk = LN
    nk = keys.shape[0] // kchunk

    def key_copy(c):
        rows = pl.ds(c * kchunk, kchunk)
        return pltpu.make_async_copy(keys_hbm.at[rows], keys.at[rows], key_sem.at[c])

    for c in range(nk):
        key_copy(c).start()

    lane = iota((8, LN), 1)
    sub = iota((8, LN), 0)
    pos = sub * LN + lane

    def prev(a):
        r = pltpu.roll(a, 1, 1)
        return jnp.where(lane == 0, pltpu.roll(r, 1, 0), r)

    tok = tok_ref[...]
    first = ((tok != prev(tok)) | (pos == 0)).astype(I32)
    c = first
    for sh in (1, 2, 4, 8, 16, 32, 64):
        c = c + jnp.where(lane >= sh, pltpu.roll(c, sh, 1), 0)
    tot = jnp.broadcast_to(c[:, 127:LN], (8, LN))
    acc = tot
    for sh in (1, 2, 4):
        acc = acc + jnp.where(sub >= sh, pltpu.roll(acc, sh, 0), 0)
    rank = c + acc - tot - 1

    owner = tok // 256
    bnd = bounds_ref[...]
    nb = bnd.shape[1] - 1
    lo_b = jnp.broadcast_to(bnd[:, :nb], (8, nb))
    hi_b = jnp.broadcast_to(bnd[:, 1:], (8, nb))
    if nb < LN:
        lo_b = jnp.concatenate([lo_b, jnp.zeros((8, LN - nb), I32)], axis=1)
        hi_b = jnp.concatenate([hi_b, jnp.zeros((8, LN - nb), I32)], axis=1)
    counted = (pos >= jnp.take_along_axis(lo_b, owner, axis=1)) & (pos < jnp.take_along_axis(hi_b, owner, axis=1))
    rank_d = jnp.where(counted, rank, -1)
    for t in range(8):
        rows = iota((EN, LN), 0)
        dedup[:, t * LN:(t + 1) * LN] = jnp.where(rank_d[t:t + 1, :] == rows, 1.0, 0.0).astype(BF16)

    h = tok // LN
    tile_first = ((h != prev(h)) | (pos == 0)).astype(I32)
    half = h % 2
    jc = owner % 2
    jp = ((owner // 2) % n, (owner // (2 * n)) % n, owner // (2 * n * n))
    lo = tok % LN
    val = (first * (rank % LN + LN) * (1 + 255 * half)).astype(F32)
    starts = [(tile_first * jnp.where(half == hf, part, 0)).astype(F32)
              for hf in range(2) for part in (rank // LN, rank % LN)]
    sub32 = iota((32, LN), 0)
    for t in range(8):
        cols = slice(t * LN, (t + 1) * LN)
        r = slice(t, t + 1)
        lohot[0:LN, cols] = jnp.where(lo[r, :] == iota((LN, LN), 0), val[r, :], 0.0).astype(BF16)
        lohot[LN:160, cols] = jnp.where(
            sub32 < 8, starts[0][r, :], jnp.where(sub32 < 16, starts[1][r, :], jnp.where(
                sub32 < 24, starts[2][r, :], starts[3][r, :]))).astype(BF16)
    coord = (cx, cy, cz)
    for a, (b2, b3) in enumerate(((2, 1), (2, 0), (1, 0))):
        row = ((jp[a] - coord[a] + n) % n) * inner + jp[b2] * (2 * n) + jp[b3] * 2 + jc
        for t in range(8):
            onehot[:, t * LN:(t + 1) * LN] = jnp.where(
                row[t:t + 1, :] == iota((LN, LN), 0), 1.0, 0.0).astype(BF16)
        tb = lax.dot_general(onehot[...], lohot[0:LN, :], NT, preferred_element_type=F32).astype(I32)
        us = lax.dot_general(lohot[LN:160, :], onehot[...], NT, preferred_element_type=F32).astype(I32)
        for d in range(n):
            tab_out[a, d, 0:inner, :] = tb[d * inner:(d + 1) * inner, :]
            for hf in range(2):
                tab_out[a, d, inner + hf:inner + hf + 1, :] = us[16 * hf:16 * hf + 1] * LN + us[16 * hf + 8:16 * hf + 9]

    for c in in_copies:
        c.wait()
    lg = jnp.dot(hid[...], w[...], preferred_element_type=F32)
    logits_out[...] = lg
    lm = jnp.max(lg, axis=1, keepdims=True)
    lz = jnp.sum(jnp.exp(lg - lm), axis=1, keepdims=True)

    tau = tau_ref[0]

    def score_step(c, carry):
        key_copy(2 * c).wait()
        key_copy(2 * c + 1).wait()
        rows = pl.ds(c * 256, 256)
        cross = lax.dot_general(hid[...], keys[rows, :], NT, preferred_element_type=F32)
        sq = jnp.zeros((256, LN), F32)
        for t in range(keys.shape[1] // LN):
            k = keys[rows, t * LN:(t + 1) * LN].astype(F32)
            sq = sq + k * k
        norm = jnp.sum(sq.T, axis=0, keepdims=True)
        sc = (2.0 * cross - norm) / tau
        score[2 * c] = sc[:, :LN]
        score[2 * c + 1] = sc[:, LN:]
        return carry

    lax.fori_loop(0, nk // 2, score_step, 0)

    sc = [score[t] for t in range(8)]
    m = jnp.max(functools.reduce(jnp.maximum, sc), axis=1, keepdims=True)
    z = jnp.zeros((64, LN), F32)
    for t in range(8):
        e = jnp.exp(sc[t] - m)
        z = z + e
        hi = e.astype(BF16)
        r1 = e - hi.astype(F32)
        mid = r1.astype(BF16)
        low = (r1 - mid.astype(F32)).astype(BF16)
        cols = slice(t * LN, (t + 1) * LN)
        e3[0:64, cols] = hi
        e3[64:LN, cols] = mid
        e3[LN:192, cols] = low
    z = jnp.sum(z, axis=1, keepdims=True)
    l64 = iota((64, LN), 1)
    stat = jnp.where(l64 == 0, m, jnp.where(l64 == 1, z, jnp.where(l64 == 2, lm, lz)))
    row_outs = (rows0, rows1, rows2)
    for h in range(2):
        stat_out[h] = stat[h * HALF:(h + 1) * HALF]
        for out, (r0, nr) in zip(row_outs, GROUPS):
            out[h, 8] = stat[h * HALF + r0:h * HALF + r0 + nr]
    for c in range(4):
        dd = lax.dot_general(e3[...], dedup[c * 256:(c + 1) * 256, :], NT, preferred_element_type=F32)
        eu = dd[0:64] + (dd[64:LN] + dd[LN:192])
        for h in range(2):
            for out, (r0, nr) in zip(row_outs, GROUPS):
                for t in range(2):
                    out[h, 2 * c + t] = eu[h * HALF + r0:h * HALF + r0 + nr, t * LN:(t + 1) * LN]


def exchange_kernel(n, own0, own1, own2, own_stat, logits, own_tab, lam_ref, out_ref,
                    tab_pair, tab, tab_smem, list0, list1, list2, scaled0, scaled1, scaled2,
                    part20, part21, part22, relay0, relay1, relay2, recv20, recv21, recv22,
                    part30, part31, part32, recv30, recv31, recv32, fin, fin_in, stat_buf, stat_in,
                    swap_sem, tab_send, tab_recv, smem_sem, stat_send, stat_recv,
                    send1, recv1, send2, recv2_sem, send_relay, recv_relay, send3, recv3_sem):
    inner = 2 * n * n
    block = 4 * n
    device, core, cx, cy, cz = coordinates(n)
    other = 1 - core
    partner = device + 1 - 2 * core
    pcoord, pstride = (cx, cy, cz), (2, 2 * n, 2 * n * n)
    coord = (cx + core * (cy - cx), cy + core * (cx - cy), cz)
    stride = (2 + core * (2 * n - 2), 2 * n + core * (2 - 2 * n), 2 * n * n)
    axis_of = (core, other, 2)
    row_stride = ((2, 2 * n), (2 * n, 2), (2 + core * (2 * n - 2), 2 * n + core * (2 - 2 * n)))
    own, lists, scaled = (own0, own1, own2), (list0, list1, list2), (scaled0, scaled1, scaled2)
    part2, relay, recv2 = (part20, part21, part22), (relay0, relay1, relay2), (recv20, recv21, recv22)
    part3, recv3 = (part30, part31, part32), (recv30, recv31, recv32)

    def wrap(a):
        return lax.rem(a, n)

    def peer(v, d):
        return device + stride[v] * (wrap(coord[v] + d) - coord[v])

    def axis_peer(a, d):
        return device + pstride[a] * (wrap(pcoord[a] + d) - pcoord[a])

    def remote(src, dst, ssem, rsem, dev):
        return pltpu.make_async_remote_copy(src_ref=src, dst_ref=dst, send_sem=ssem, recv_sem=rsem,
                                            device_id={'model': dev}, device_id_type=pl.DeviceIdType.MESH)

    near = (1, n - 1) if n > 2 else (1,)
    far = tuple(range(2, n - 1))
    order = (1, 2, 0)
    sends = []

    def go(c):
        c.start()
        sends.append(c)

    barrier = pltpu.get_barrier_semaphore()
    partners = [partner] + [peer(v, d) for v in range(3) for d in range(1, n)]
    for p in partners:
        pl.semaphore_signal(barrier, inc=1, device_id={'model': p}, device_id_type=pl.DeviceIdType.MESH)
    for g in range(3):
        for i in range(2 * n):
            scaled[g][i, 8] = jnp.zeros(scaled[g].shape[2:], F32)
    pl.semaphore_wait(barrier, len(partners))

    stat_swap = remote(own_stat.at[other], stat_in.at[0], swap_sem.at[0, 0], swap_sem.at[1, 0], partner)
    tab_swap = remote(own_tab, tab_pair, swap_sem.at[0, 1], swap_sem.at[1, 1], partner)
    row_swap = [remote(own[g].at[other], lists[g].at[0], swap_sem.at[0, 2 + g], swap_sem.at[1, 2 + g], partner)
                for g in range(3)]
    go(stat_swap)
    go(tab_swap)
    for g in order:
        go(row_swap[g])

    def tab_copy(a, d, l):
        src = own_tab if l == 0 else tab_pair
        return remote(src.at[a, d], tab.at[a, n - d - 1, l], tab_send.at[a, d - 1, l], tab_recv.at[a, n - d - 1, l],
                      axis_peer(a, d))

    def row_copy(g, d, l):
        src = own[g].at[core] if l == 0 else lists[g].at[0]
        return remote(src, lists[g].at[2 * (n - d) - 1 + l], send1.at[g, d - 1, l], recv1.at[g, n - d - 1, l], peer(g, d))

    def row_relay(g, l):
        frm, to = (n - 1, 1) if l == 0 else (1, n - 1)
        return remote(lists[g].at[2 * frm - 1 + l], lists[g].at[3 + l], send1.at[g, 1, l], recv1.at[g, 1, l], peer(g, to))

    for d in far + near:
        for a in range(3):
            go(tab_copy(a, d, 0))
    for d in near:
        for g in order:
            go(row_copy(g, d, 0))

    def combine(tiles):
        ln = iota((HALF, LN), 1)
        ms = [jnp.broadcast_to(t[:, 0:1], (HALF, LN)) for t in tiles]
        ls = [jnp.broadcast_to(t[:, 2:3], (HALF, LN)) for t in tiles]
        mm = functools.reduce(jnp.maximum, ms)
        ll = functools.reduce(jnp.maximum, ls)
        zz = sum(jnp.exp(a - mm) * t[:, 1:2] for a, t in zip(ms, tiles))
        lzz = sum(jnp.exp(a - ll) * t[:, 3:4] for a, t in zip(ls, tiles))
        return jnp.where(ln == 0, mm, jnp.where(ln == 1, zz, jnp.where(ln == 2, ll, lzz)))

    def stat_copy(v, d):
        return remote(stat_buf.at[v], stat_in.at[1 + v * (n - 1) + n - d - 1], stat_send.at[v, d - 1],
                      stat_recv.at[v, n - d - 1], peer(v, d))

    def stat_round(v):
        for d in range(1, n):
            stat_copy(v, d).wait_recv()
        stat_buf[v + 1] = combine([stat_buf[v]] + [stat_in[1 + v * (n - 1) + k] for k in range(n - 1)])
        if v < 2:
            for d in range(1, n):
                go(stat_copy(v + 1, d))

    stat_swap.wait_recv()
    stat_buf[0] = combine([own_stat[core], stat_in[0]])
    for d in range(1, n):
        go(stat_copy(0, d))
    tab_swap.wait_recv()
    for d in far + near:
        for a in range(3):
            go(tab_copy(a, d, 1))
    for g in order:
        row_swap[g].wait_recv()
        for d in near:
            go(row_copy(g, d, 1))
    stat_round(0)
    for g in order:
        for d in near:
            for l in range(2):
                row_copy(g, d, l).wait_recv()
        if far:
            for l in range(2):
                go(row_relay(g, l))
    stat_round(1)

    def tab_of(a, k, l):
        if k:
            return tab.at[a, k - 1, l]
        return (tab_pair if l else own_tab).at[a, 0]

    def list_of(g, k, l):
        if k == 0 and l == 0:
            return own[g].at[core]
        return lists[g].at[2 * k - 1 + l]

    for d in range(1, n):
        for l in range(2):
            for a in range(3):
                tab_copy(a, d, l).wait_recv()
    smem_copies = [pltpu.make_async_copy(tab_of(a, k, l).at[pl.ds(inner, 2)], tab_smem.at[a, k, l], smem_sem.at[a, k, l])
                   for a in range(3) for k in range(n) for l in range(2)]
    for c in smem_copies:
        c.start()
    stat_round(2)
    stat_back = remote(stat_buf.at[3], stat_in.at[3 * n - 2], swap_sem.at[0, 5], swap_sem.at[1, 5], partner)
    go(stat_back)
    for c in smem_copies:
        c.wait()

    src = [(k, l) for k in range(n) for l in range(2)]
    for g in order:
        if far:
            for l in range(2):
                row_relay(g, l).wait_recv()

    def scale(g):
        r0, nr = GROUPS[g]
        mm = stat_buf[3, r0:r0 + nr, 0:1]
        for i, (k, l) in enumerate(src):
            rows = list_of(g, k, l)
            f = jnp.broadcast_to(jnp.exp(rows[8][:, 0:1] - mm), (nr, LN))
            for t in range(8):
                scaled[g][i, t] = rows[t] * f

    def partial_hist(g, d2):
        nr = GROUPS[g][1]
        a = axis_of[g]
        c2, c3 = coord[(g + 1) % 3], coord[(g + 2) % 3]
        s2, s3 = row_stride[g]
        base = wrap(c2 + d2) * s2
        ln = iota((nr, LN), 1)

        def pair_step(q, carry):
            d3 = lax.div(q, 2)
            c = q - 2 * d3
            row = base + wrap(c3 + d3) * s3 + c
            acc = [jnp.zeros((nr, LN), F32)] * 2
            for i, (k, l) in enumerate(src):
                packed = jnp.broadcast_to(tab_of(a, k, l)[pl.ds(row, 1), :], (nr, LN))
                for hf in range(2):
                    u = tab_smem[a, k, l, hf, ((n - k) % n) * inner + row]
                    kt = lax.shift_right_logical(u, 7)
                    merged = jnp.where(ln >= (u & 127), scaled[g][i, kt], scaled[g][i, kt + 1])
                    code = lax.shift_right_logical(packed, 8) if hf else packed
                    got = jnp.take_along_axis(merged, code & 127, axis=1)
                    acc[hf] = acc[hf] + jnp.where((code & LN) != 0, got, 0.0)
            part2[g][d2, 2 * q] = acc[0]
            part2[g][d2, 2 * q + 1] = acc[1]
            return carry

        lax.fori_loop(0, 2 * n, pair_step, 0, unroll=2)

    def copy2(g, d):
        i = 0 if d == 1 else 1
        return remote(part2[g].at[d], recv2[g].at[i], send2.at[g, i], recv2_sem.at[g, i], peer((g + 1) % 3, d))

    halves = (pl.ds(0, block // 2), pl.ds(block // 2, block // 2))

    def copy2_relay(g, i):
        return remote(part2[g].at[2, halves[i]], relay[g].at[i], send_relay.at[g, i], recv_relay.at[g, i],
                      peer((g + 1) % 3, near[i]))

    def copy3(g, d):
        return remote(part3[g].at[d], recv3[g].at[n - d - 1], send3.at[g, d - 1], recv3_sem.at[g, n - d - 1],
                      peer((g + 2) % 3, d))

    for g in order:
        scale(g)
        for d2 in far:
            partial_hist(g, d2)
            for i in range(2):
                go(copy2_relay(g, i))
    for g in order:
        for d2 in near:
            partial_hist(g, d2)
    for g in order:
        for i, d2 in enumerate(near):
            if far:
                copy2_relay(g, i).wait_recv()
                for t in range(block // 2):
                    q = i * (block // 2) + t
                    part2[g][d2, q] = part2[g][d2, q] + relay[g][i, t]
            go(copy2(g, d2))
    for g in order:
        partial_hist(g, 0)

    for g in order:
        for d in near:
            copy2(g, d).wait_recv()
        for d3 in far + near + (0,):
            for ch in range(4):
                q = d3 * 4 + ch
                part3[g][d3, ch] = part2[g][0, q] + sum(recv2[g][i, q] for i in range(len(near)))
            if d3:
                go(copy3(g, d3))

    for g in order:
        r0, nr = GROUPS[g]
        for d in range(1, n):
            copy3(g, d).wait_recv()
        for ch in range(4):
            fin[ch // 2, ch % 2, r0:r0 + nr] = part3[g][0, ch] + sum(recv3[g][k, ch] for k in range(n - 1))

    back = remote(fin.at[other], fin_in, swap_sem.at[0, 6], swap_sem.at[1, 6], partner)
    go(back)
    lam = lam_ref[0]

    def finish(block_ref, st, rows_half):
        zz, ll, lzz = st[:, 1:2], st[:, 2:3], st[:, 3:4]
        rows = pl.ds(pl.multiple_of(rows_half * HALF, 8), HALF)
        for hf in range(2):
            cols = slice(hf * LN, (hf + 1) * LN)
            lm_exp = jnp.exp(logits[rows, cols] - ll)
            out_ref[rows, cols] = jnp.log(lam * (block_ref[hf] / zz) + (1.0 - lam) * (lm_exp / lzz))

    finish(fin.at[core], stat_buf[3], core)
    stat_back.wait_recv()
    back.wait_recv()
    finish(fin_in, stat_in[3 * n - 2], other)
    for c in sends:
        c.wait_send()


def step(n, hidden, w_local, keys_local, tok_local, bounds_local, tau, lam):
    tab_rows = 2 * n * n + 8
    block = 4 * n
    dim = hidden.shape[1]
    V, DMA = pltpu.VMEM, pltpu.SemaphoreType.DMA
    vm = pl.BlockSpec(memory_space=pltpu.VMEM)
    sm = pl.BlockSpec(memory_space=pltpu.SMEM)
    hbm = pl.BlockSpec(memory_space=pl.ANY)
    *rows, stat, logits, tab = pl.pallas_call(
        functools.partial(local_kernel, n),
        out_shape=tuple(jax.ShapeDtypeStruct((2, 9, nr, LN), F32) for _, nr in GROUPS) + (
            jax.ShapeDtypeStruct((2, HALF, LN), F32), jax.ShapeDtypeStruct((64, 256), F32),
            jax.ShapeDtypeStruct((3, n, tab_rows, LN), I32)),
        in_specs=[vm, vm, sm, hbm, hbm, hbm],
        out_specs=(vm,) * 6,
        scratch_shapes=[
            V((64, dim), BF16), V((dim, 256), BF16), V((EN, dim), BF16), V((8, 64, LN), F32),
            V((EN, EN), BF16), V((LN, EN), BF16), V((160, EN), BF16), V((192, EN), BF16),
            DMA((2,)), DMA((8,))],
        name='local_scores',
    )(tok_local.reshape(8, LN), bounds_local, tau.reshape(1), hidden, w_local, keys_local)

    def per_group(*lead):
        return [V((*lead, nr, LN), F32) for _, nr in GROUPS]

    m = n - 1
    return pl.pallas_call(
        functools.partial(exchange_kernel, n),
        out_shape=jax.ShapeDtypeStruct((64, 256), F32),
        in_specs=[vm] * 6 + [sm],
        out_specs=vm,
        scratch_shapes=[
            V((3, n, tab_rows, LN), I32), V((3, m, 2, tab_rows, LN), I32), pltpu.SMEM((3, n, 2, 2, LN), I32),
            *per_group(2 * n - 1, 9), *per_group(2 * n, 9), *per_group(n, block), *per_group(2, block // 2),
            *per_group(2, block), *per_group(n, 4), *per_group(m, 4),
            V((2, 2, HALF, LN), F32), V((2, HALF, LN), F32), V((4, HALF, LN), F32), V((3 * n - 1, HALF, LN), F32),
            DMA((2, 7)), DMA((3, m, 2)), DMA((3, m, 2)), DMA((3, n, 2)), DMA((3, m)), DMA((3, m)),
            DMA((3, m, 2)), DMA((3, m, 2)), DMA((3, 2)), DMA((3, 2)), DMA((3, 2)), DMA((3, 2)), DMA((3, m)), DMA((3, m))],
        compiler_params=pltpu.CompilerParams(collective_id=0, has_side_effects=True),
        name='exchange',
    )(*rows, stat, logits, tab, lam.reshape(1))


def solution(mesh):
    n = round((mesh.shape['model'] // 2) ** (1 / 3))
    return jax.shard_map(functools.partial(step, n), mesh=mesh,
                         in_specs=(P('data', None), P(None, 'model'), P('model', None), P('model'),
                                   P('model', None), P(), P()),
                         out_specs=P('data', 'model'), check_vma=False)
```

```python
import functools

import jax
import jax.numpy as jnp
from jax import lax
from jax.experimental import pallas as pl
from jax.experimental.pallas import tpu as pltpu
from jax.sharding import PartitionSpec as P

F32, BF16, I32 = jnp.float32, jnp.bfloat16, jnp.int32
GROUPS = ((0, 16), (16, 8), (24, 8))
UNROLL = 2
HALF = 32
LN, EN = 128, 1024
NT = (((1,), (1,)), ((), ()))


def iota(shape, axis):
    return lax.broadcasted_iota(I32, shape, axis)


def coordinates(n):
    device = lax.axis_index('model')
    return device, device % 2, (device // 2) % n, (device // (2 * n)) % n, device // (2 * n * n)


def local_kernel(n, tok_ref, bounds_ref, tau_ref, hid_hbm, w_hbm, keys_hbm, rows0, rows1, rows2, logits_out, tab_out,
                 hid, w, keys, score, dedup, onehot, lohot, e3, in_sem, key_sem):
    inner = 2 * n * n
    _, _, cx, cy, cz = coordinates(n)
    in_copies = (pltpu.make_async_copy(hid_hbm, hid, in_sem.at[0]), pltpu.make_async_copy(w_hbm, w, in_sem.at[1]))
    for c in in_copies:
        c.start()
    kchunk = LN
    nk = keys.shape[0] // kchunk

    def key_copy(c):
        rows = pl.ds(c * kchunk, kchunk)
        return pltpu.make_async_copy(keys_hbm.at[rows], keys.at[rows], key_sem.at[c])

    for c in range(nk):
        key_copy(c).start()

    lane = iota((8, LN), 1)
    sub = iota((8, LN), 0)
    pos = sub * LN + lane

    def prev(a):
        r = pltpu.roll(a, 1, 1)
        return jnp.where(lane == 0, pltpu.roll(r, 1, 0), r)

    tok = tok_ref[...]
    first = ((tok != prev(tok)) | (pos == 0)).astype(I32)
    c = first
    for sh in (1, 2, 4, 8, 16, 32, 64):
        c = c + jnp.where(lane >= sh, pltpu.roll(c, sh, 1), 0)
    tot = jnp.broadcast_to(c[:, 127:LN], (8, LN))
    acc = tot
    for sh in (1, 2, 4):
        acc = acc + jnp.where(sub >= sh, pltpu.roll(acc, sh, 0), 0)
    rank = c + acc - tot - 1

    owner = tok // 256
    bnd = bounds_ref[...]
    nb = bnd.shape[1] - 1
    lo_b = jnp.broadcast_to(bnd[:, :nb], (8, nb))
    hi_b = jnp.broadcast_to(bnd[:, 1:], (8, nb))
    if nb < LN:
        lo_b = jnp.concatenate([lo_b, jnp.zeros((8, LN - nb), I32)], axis=1)
        hi_b = jnp.concatenate([hi_b, jnp.zeros((8, LN - nb), I32)], axis=1)
    counted = (pos >= jnp.take_along_axis(lo_b, owner, axis=1)) & (pos < jnp.take_along_axis(hi_b, owner, axis=1))
    rank_d = jnp.where(counted, rank, -1)
    for t in range(8):
        rows = iota((EN, LN), 0)
        dedup[:, t * LN:(t + 1) * LN] = jnp.where(rank_d[t:t + 1, :] == rows, 1.0, 0.0).astype(BF16)

    h = tok // LN
    tile_first = ((h != prev(h)) | (pos == 0)).astype(I32)
    half = h % 2
    jc = owner % 2
    jp = ((owner // 2) % n, (owner // (2 * n)) % n, owner // (2 * n * n))
    lo = tok % LN
    val = (first * (rank % LN + LN) * (1 + 255 * half)).astype(F32)
    starts = [(tile_first * jnp.where(half == hf, part, 0)).astype(F32)
              for hf in range(2) for part in (rank // LN, rank % LN)]
    sub32 = iota((32, LN), 0)
    for t in range(8):
        cols = slice(t * LN, (t + 1) * LN)
        r = slice(t, t + 1)
        lohot[0:LN, cols] = jnp.where(lo[r, :] == iota((LN, LN), 0), val[r, :], 0.0).astype(BF16)
        lohot[LN:160, cols] = jnp.where(
            sub32 < 8, starts[0][r, :], jnp.where(sub32 < 16, starts[1][r, :], jnp.where(
                sub32 < 24, starts[2][r, :], starts[3][r, :]))).astype(BF16)
    coord = (cx, cy, cz)
    for a, (b2, b3) in enumerate(((2, 1), (2, 0), (1, 0))):
        row = ((jp[a] - coord[a] + n) % n) * inner + jp[b2] * (2 * n) + jp[b3] * 2 + jc
        for t in range(8):
            onehot[:, t * LN:(t + 1) * LN] = jnp.where(
                row[t:t + 1, :] == iota((LN, LN), 0), 1.0, 0.0).astype(BF16)
        tb = lax.dot_general(onehot[...], lohot[0:LN, :], NT, preferred_element_type=F32).astype(I32)
        us = lax.dot_general(lohot[LN:160, :], onehot[...], NT, preferred_element_type=F32).astype(I32)
        for d in range(n):
            tab_out[a, d, 0:inner, :] = tb[d * inner:(d + 1) * inner, :]
            for hf in range(2):
                tab_out[a, d, inner + hf:inner + hf + 1, :] = us[16 * hf:16 * hf + 1] * LN + us[16 * hf + 8:16 * hf + 9]

    for c in in_copies:
        c.wait()
    lg = jnp.dot(hid[...], w[...], preferred_element_type=F32)
    logits_out[...] = lg
    lm = jnp.max(lg, axis=1, keepdims=True)
    lz = jnp.sum(jnp.exp(lg - lm), axis=1, keepdims=True)

    tau = tau_ref[0]

    def score_step(c, carry):
        key_copy(2 * c).wait()
        key_copy(2 * c + 1).wait()
        rows = pl.ds(c * 256, 256)
        cross = lax.dot_general(hid[...], keys[rows, :], NT, preferred_element_type=F32)
        sq = jnp.zeros((256, LN), F32)
        for t in range(keys.shape[1] // LN):
            k = keys[rows, t * LN:(t + 1) * LN].astype(F32)
            sq = sq + k * k
        norm = jnp.sum(sq.T, axis=0, keepdims=True)
        sc = (2.0 * cross - norm) / tau
        score[2 * c] = sc[:, :LN]
        score[2 * c + 1] = sc[:, LN:]
        return carry

    lax.fori_loop(0, nk // 2, score_step, 0)

    sc = [score[t] for t in range(8)]
    m = jnp.max(functools.reduce(jnp.maximum, sc), axis=1, keepdims=True)
    z = jnp.zeros((64, LN), F32)
    for t in range(8):
        e = jnp.exp(sc[t] - m)
        z = z + e
        hi = e.astype(BF16)
        r1 = e - hi.astype(F32)
        mid = r1.astype(BF16)
        low = (r1 - mid.astype(F32)).astype(BF16)
        cols = slice(t * LN, (t + 1) * LN)
        e3[0:64, cols] = hi
        e3[64:LN, cols] = mid
        e3[LN:192, cols] = low
    z = jnp.sum(z, axis=1, keepdims=True)
    l64 = iota((64, LN), 1)
    stat = jnp.where(l64 == 0, m, jnp.where(l64 == 1, z, jnp.where(l64 == 2, lm, lz)))
    row_outs = (rows0, rows1, rows2)
    for h in range(2):
        for out, (r0, nr) in zip(row_outs, GROUPS):
            out[h, 8] = stat[h * HALF + r0:h * HALF + r0 + nr]
    for c in range(4):
        dd = lax.dot_general(e3[...], dedup[c * 256:(c + 1) * 256, :], NT, preferred_element_type=F32)
        eu = dd[0:64] + (dd[64:LN] + dd[LN:192])
        for h in range(2):
            for out, (r0, nr) in zip(row_outs, GROUPS):
                for t in range(2):
                    out[h, 2 * c + t] = eu[h * HALF + r0:h * HALF + r0 + nr, t * LN:(t + 1) * LN]


def exchange_kernel(n, own0, own1, own2, logits, own_tab, lam_ref, out_ref,
                    tab_pair, tab, tab_smem, list0, list1, list2, scaled0, scaled1, scaled2,
                    part20, part21, part22, relay0, relay1, relay2, recv20, recv21, recv22,
                    part30, part31, part32, recv30, recv31, recv32, fin, fin_in,
                    swap_sem, tab_send, tab_recv, smem_sem,
                    send1, recv1, send2, recv2_sem, send_relay, recv_relay, send3, recv3_sem):
    inner = 2 * n * n
    mid = 2 * n
    block = 2 * mid
    device, core, cx, cy, cz = coordinates(n)
    other = 1 - core
    partner = device + 1 - 2 * core
    pcoord, pstride = (cx, cy, cz), (2, 2 * n, 2 * n * n)

    def axes_of(c):
        return ((cx + c * (cy - cx), cy + c * (cx - cy), cz), (2 + c * (2 * n - 2), 2 * n + c * (2 - 2 * n), 2 * n * n))

    coord, stride = axes_of(core)
    coord_o, stride_o = axes_of(other)
    axis_of = (core, other, 2)
    row_stride = ((2, 2 * n), (2 * n, 2), (stride[0], stride[1]))
    own, lists, scaled = (own0, own1, own2), (list0, list1, list2), (scaled0, scaled1, scaled2)
    part2, relay, recv2 = (part20, part21, part22), (relay0, relay1, relay2), (recv20, recv21, recv22)
    part3, recv3 = (part30, part31, part32), (recv30, recv31, recv32)

    def wrap(a):
        return lax.rem(a, n)

    def peer(v, d):
        return device + stride[v] * (wrap(coord[v] + d) - coord[v])

    def peer_other(v, d):
        return partner + stride_o[v] * (wrap(coord_o[v] + d) - coord_o[v])

    def axis_peer(start, a, d):
        return start + pstride[a] * (wrap(pcoord[a] + d) - pcoord[a])

    def remote(src, dst, ssem, rsem, dev):
        return pltpu.make_async_remote_copy(src_ref=src, dst_ref=dst, send_sem=ssem, recv_sem=rsem,
                                            device_id={'model': dev}, device_id_type=pl.DeviceIdType.MESH)

    near = (1, n - 1) if n > 2 else (1,)
    far = tuple(range(2, n - 1))
    order = (1, 2, 0)
    sends = []

    def go(c):
        c.start()
        sends.append(c)

    barrier = pltpu.get_barrier_semaphore()
    partners = [partner] + [axis_peer(start, a, d) for start in (device, partner) for a in range(3) for d in range(1, n)]
    for p in partners:
        pl.semaphore_signal(barrier, inc=1, device_id={'model': p}, device_id_type=pl.DeviceIdType.MESH)
    for g in range(3):
        for i in range(2 * n):
            scaled[g][i, 8] = jnp.zeros(scaled[g].shape[2:], F32)
    pl.semaphore_wait(barrier, len(partners))

    tab_swap = remote(own_tab.at[:, 0], tab_pair, swap_sem.at[0, 0], swap_sem.at[1, 0], partner)
    row_swap = [remote(own[g].at[other], lists[g].at[0], swap_sem.at[0, 1 + g], swap_sem.at[1, 1 + g], partner)
                for g in range(3)]

    def tab_copy(a, d, l):
        return remote(own_tab.at[a, d], tab.at[a, n - d - 1, l], tab_send.at[a, d - 1, l], tab_recv.at[a, n - d - 1, l],
                      axis_peer(partner if l else device, a, d))

    def row_copy(g, d, l):
        return remote(own[g].at[other if l else core], lists[g].at[2 * (n - d) - 1 + l], send1.at[g, d - 1, l],
                      recv1.at[g, n - d - 1, l], peer_other(g, d) if l else peer(g, d))

    def row_relay(g, l):
        frm, to = (n - 1, 1) if l == 0 else (1, n - 1)
        return remote(lists[g].at[2 * frm - 1 + l], lists[g].at[3 + l], send1.at[g, 1, l], recv1.at[g, 1, l], peer(g, to))

    for g in order:
        for d in near:
            for l in range(2):
                go(row_copy(g, d, l))
    for g in order:
        go(row_swap[g])
    go(tab_swap)
    for d in far + near:
        for a in range(3):
            for l in range(2):
                go(tab_copy(a, d, l))

    def stats(tiles, counted=None):
        shape = tiles[0].shape
        ln = iota(shape, 1)
        counted = counted or tiles
        ms = [jnp.broadcast_to(t[:, 0:1], shape) for t in tiles]
        ls = [jnp.broadcast_to(t[:, 2:3], shape) for t in tiles]
        mm = functools.reduce(jnp.maximum, ms)
        ll = functools.reduce(jnp.maximum, ls)
        fs = [jnp.exp(a - mm) for a in ms]
        zz = sum(f * t[:, 1:2] for f, t in zip(fs, counted))
        lzz = sum(jnp.exp(a - ll) * t[:, 3:4] for a, t in zip(ls, counted))
        return fs, jnp.where(ln == 0, mm, jnp.where(ln == 1, zz, jnp.where(ln == 2, ll, lzz)))

    for g in order:
        for d in near:
            for l in range(2):
                row_copy(g, d, l).wait_recv()
        if far:
            for l in range(2):
                go(row_relay(g, l))
        row_swap[g].wait_recv()

    def tab_of(a, k, l):
        if k:
            return tab.at[a, k - 1, l]
        return tab_pair.at[a] if l else own_tab.at[a, 0]

    def list_of(g, k, l):
        if k == 0 and l == 0:
            return own[g].at[core]
        return lists[g].at[2 * k - 1 + l]

    tab_swap.wait_recv()
    for d in range(1, n):
        for l in range(2):
            for a in range(3):
                tab_copy(a, d, l).wait_recv()
    smem_copies = [pltpu.make_async_copy(tab_of(axis_of[g], k, l).at[pl.ds(inner, 2)], tab_smem.at[g, k, l],
                                         smem_sem.at[g, k, l])
                   for g in range(3) for k in range(n) for l in range(2)]
    for c in smem_copies:
        c.start()
    for c in smem_copies:
        c.wait()

    src = [(k, l) for k in range(n) for l in range(2)]

    def partial_hist(g, d2):
        nr = GROUPS[g][1]
        a = axis_of[g]
        c2, c3 = coord[(g + 1) % 3], coord[(g + 2) % 3]
        s2, s3 = row_stride[g]
        base = wrap(c2 + d2) * s2
        ln = iota((nr, LN), 1)

        def pair_step(q, carry):
            d3 = lax.div(q, 2)
            c = q - 2 * d3
            row = base + wrap(c3 + d3) * s3 + c
            acc = [jnp.zeros((nr, LN), F32)] * 2
            for i, (k, l) in enumerate(src):
                packed = jnp.broadcast_to(tab_of(a, k, l)[pl.ds(row, 1), :], (nr, LN))
                for hf in range(2):
                    u = tab_smem[g, k, l, hf, ((n - k) % n) * inner + row]
                    kt = lax.shift_right_logical(u, 7)
                    merged = jnp.where(ln >= (u & 127), scaled[g][i, kt], scaled[g][i, kt + 1])
                    code = lax.shift_right_logical(packed, 8) if hf else packed
                    got = jnp.take_along_axis(merged, code & 127, axis=1, mode='promise_in_bounds')
                    acc[hf] = acc[hf] + jnp.where((code & LN) != 0, got, 0.0)
            t = 2 * q + lax.div(q, n)
            part2[g][d2, t] = acc[0]
            part2[g][d2, t + 1] = acc[1]
            return carry

        lax.fori_loop(0, mid, pair_step, 0, unroll=UNROLL)

    halves = (pl.ds(0, mid + 1), pl.ds(mid, mid + 1))

    def copy2(g, d):
        i = 0 if d == 1 else 1
        return remote(part2[g].at[d], recv2[g].at[i], send2.at[g, i], recv2_sem.at[g, i], peer((g + 1) % 3, d))

    def copy2_relay(g, i):
        return remote(part2[g].at[2, halves[i]], relay[g].at[i], send_relay.at[g, i], recv_relay.at[g, i],
                      peer((g + 1) % 3, near[i]))

    def copy3(g, d):
        return remote(part3[g].at[d], recv3[g].at[n - d - 1], send3.at[g, d - 1], recv3_sem.at[g, n - d - 1],
                      peer((g + 2) % 3, d))

    group_stat = {}
    for g in order:
        if far:
            for l in range(2):
                row_relay(g, l).wait_recv()
        fs, group_stat[g] = stats([list_of(g, k, l)[8] for k, l in src])
        for i, (k, l) in enumerate(src):
            rows = list_of(g, k, l)
            for t in range(8):
                scaled[g][i, t] = rows[t] * fs[i]
        for d2 in far + near + (0,):
            part2[g][d2, mid] = group_stat[g]
        for d2 in far:
            partial_hist(g, d2)
            for i in range(2):
                go(copy2_relay(g, i))
    for g in order:
        for d2 in near:
            partial_hist(g, d2)
    for g in order:
        for i, d2 in enumerate(near):
            if far:
                copy2_relay(g, i).wait_recv()
                there = relay[g][i, 0 if i else mid]
                zero = jnp.zeros(there.shape, F32)
                fs, tile = stats([group_stat[g], there], [group_stat[g], zero if i else there])
                for t in range(block + 1):
                    r = t - i * mid
                    if t == mid:
                        part2[g][d2, t] = tile
                    elif 0 <= r <= mid:
                        part2[g][d2, t] = part2[g][d2, t] * fs[0] + relay[g][i, r] * fs[1]
                    else:
                        part2[g][d2, t] = part2[g][d2, t] * fs[0]
            go(copy2(g, d2))
    for g in order:
        partial_hist(g, 0)

    for g in order:
        for d in near:
            copy2(g, d).wait_recv()
        parts = [part2[g].at[0]] + [recv2[g].at[i] for i in range(len(near))]
        fs, tile = stats([p[mid] for p in parts])
        for d3 in far + near + (0,):
            for ch in range(4):
                q = d3 * 4 + ch
                q = q + q // mid
                part3[g][d3, ch] = sum(p[q] * f for p, f in zip(parts, fs))
            part3[g][d3, 4] = tile
            if d3:
                go(copy3(g, d3))

    for g in order:
        r0, nr = GROUPS[g]
        for d in range(1, n):
            copy3(g, d).wait_recv()
        parts = [part3[g].at[0]] + [recv3[g].at[k] for k in range(n - 1)]
        fs, tile = stats([p[4] for p in parts])
        for ch in range(4):
            fin[ch // 2, ch % 2, r0:r0 + nr] = sum(p[ch] * f for p, f in zip(parts, fs))
        for c in range(2):
            fin[c, 2, r0:r0 + nr] = tile

    back = remote(fin.at[other], fin_in, swap_sem.at[0, 4], swap_sem.at[1, 4], partner)
    go(back)
    lam = lam_ref[0]

    def finish(block_ref, rows_half):
        st = block_ref[2]
        zz, ll, lzz = st[:, 1:2], st[:, 2:3], st[:, 3:4]
        rows = pl.ds(pl.multiple_of(rows_half * HALF, 8), HALF)
        for hf in range(2):
            cols = slice(hf * LN, (hf + 1) * LN)
            lm_exp = jnp.exp(logits[rows, cols] - ll)
            out_ref[rows, cols] = jnp.log(lam * (block_ref[hf] / zz) + (1.0 - lam) * (lm_exp / lzz))

    finish(fin.at[core], core)
    back.wait_recv()
    finish(fin_in, other)
    for c in sends:
        c.wait_send()


def step(n, hidden, w_local, keys_local, tok_local, bounds_local, tau, lam):
    tab_rows = 2 * n * n + 8
    block = 4 * n
    dim = hidden.shape[1]
    V, DMA = pltpu.VMEM, pltpu.SemaphoreType.DMA
    vm = pl.BlockSpec(memory_space=pltpu.VMEM)
    sm = pl.BlockSpec(memory_space=pltpu.SMEM)
    hbm = pl.BlockSpec(memory_space=pl.ANY)
    *rows, logits, tab = pl.pallas_call(
        functools.partial(local_kernel, n),
        out_shape=tuple(jax.ShapeDtypeStruct((2, 9, nr, LN), F32) for _, nr in GROUPS) + (
            jax.ShapeDtypeStruct((64, 256), F32),
            jax.ShapeDtypeStruct((3, n, tab_rows, LN), I32)),
        in_specs=[vm, vm, sm, hbm, hbm, hbm],
        out_specs=(vm,) * 5,
        scratch_shapes=[
            V((64, dim), BF16), V((dim, 256), BF16), V((EN, dim), BF16), V((8, 64, LN), F32),
            V((EN, EN), BF16), V((LN, EN), BF16), V((160, EN), BF16), V((192, EN), BF16),
            DMA((2,)), DMA((8,))],
        name='local_scores',
    )(tok_local.reshape(8, LN), bounds_local, tau.reshape(1), hidden, w_local, keys_local)

    def per_group(*lead):
        return [V((*lead, nr, LN), F32) for _, nr in GROUPS]

    m = n - 1
    return pl.pallas_call(
        functools.partial(exchange_kernel, n),
        out_shape=jax.ShapeDtypeStruct((64, 256), F32),
        in_specs=[vm] * 5 + [sm],
        out_specs=vm,
        scratch_shapes=[
            V((3, tab_rows, LN), I32), V((3, m, 2, tab_rows, LN), I32), pltpu.SMEM((3, n, 2, 2, LN), I32),
            *per_group(2 * n - 1, 9), *per_group(2 * n, 9), *per_group(n, block + 1), *per_group(2, block // 2 + 1),
            *per_group(2, block + 1), *per_group(n, 5), *per_group(m, 5),
            V((2, 3, HALF, LN), F32), V((3, HALF, LN), F32),
            DMA((2, 5)), DMA((3, m, 2)), DMA((3, m, 2)), DMA((3, n, 2)),
            DMA((3, m, 2)), DMA((3, m, 2)), DMA((3, 2)), DMA((3, 2)), DMA((3, 2)), DMA((3, 2)), DMA((3, m)), DMA((3, m))],
        compiler_params=pltpu.CompilerParams(collective_id=0, has_side_effects=True),
        name='exchange',
    )(*rows, logits, tab, lam.reshape(1))


def solution(mesh):
    n = round((mesh.shape['model'] // 2) ** (1 / 3))
    return jax.shard_map(functools.partial(step, n), mesh=mesh,
                         in_specs=(P('data', None), P(None, 'model'), P('model', None), P('model'),
                                   P('model', None), P(), P()),
                         out_specs=P('data', 'model'), check_vma=False)
```

```python
import functools

import jax
import jax.numpy as jnp
from jax import lax
from jax.experimental import pallas as pl
from jax.experimental.pallas import tpu as pltpu
from jax.sharding import PartitionSpec as P

F32, BF16, I32 = jnp.float32, jnp.bfloat16, jnp.int32
GROUPS = ((0, 16), (16, 8), (24, 8))
UNROLL = 4
AHEAD = 4
HALF = 32
LN, EN = 128, 1024
NT = (((1,), (1,)), ((), ()))


def iota(shape, axis):
    return lax.broadcasted_iota(I32, shape, axis)


def coordinates(n):
    device = lax.axis_index('model')
    return device, device % 2, (device // 2) % n, (device // (2 * n)) % n, device // (2 * n * n)


def local_kernel(n, tok_ref, bounds_ref, tau_ref, hid_hbm, w_hbm, keys_hbm, rows0, rows1, rows2, logits_out, tab_out,
                 hid, w, keys, score, dedup, onehot, lohot, e3, in_sem, key_sem):
    inner = 2 * n * n
    _, _, cx, cy, cz = coordinates(n)
    in_copies = (pltpu.make_async_copy(hid_hbm, hid, in_sem.at[0]), pltpu.make_async_copy(w_hbm, w, in_sem.at[1]))
    for c in in_copies:
        c.start()
    kchunk = LN
    nk = keys.shape[0] // kchunk

    def key_copy(c):
        rows = pl.ds(c * kchunk, kchunk)
        return pltpu.make_async_copy(keys_hbm.at[rows], keys.at[rows], key_sem.at[c])

    for c in range(AHEAD):
        key_copy(c).start()

    lane = iota((8, LN), 1)
    sub = iota((8, LN), 0)
    pos = sub * LN + lane

    def prev(a):
        r = pltpu.roll(a, 1, 1)
        return jnp.where(lane == 0, pltpu.roll(r, 1, 0), r)

    tok = tok_ref[...]
    first = ((tok != prev(tok)) | (pos == 0)).astype(I32)
    c = first
    for sh in (1, 2, 4, 8, 16, 32, 64):
        c = c + jnp.where(lane >= sh, pltpu.roll(c, sh, 1), 0)
    tot = jnp.broadcast_to(c[:, 127:LN], (8, LN))
    acc = tot
    for sh in (1, 2, 4):
        acc = acc + jnp.where(sub >= sh, pltpu.roll(acc, sh, 0), 0)
    rank = c + acc - tot - 1

    owner = tok // 256
    bnd = bounds_ref[...]
    nb = bnd.shape[1] - 1
    lo_b = jnp.broadcast_to(bnd[:, :nb], (8, nb))
    hi_b = jnp.broadcast_to(bnd[:, 1:], (8, nb))
    if nb < LN:
        lo_b = jnp.concatenate([lo_b, jnp.zeros((8, LN - nb), I32)], axis=1)
        hi_b = jnp.concatenate([hi_b, jnp.zeros((8, LN - nb), I32)], axis=1)
    counted = (pos >= jnp.take_along_axis(lo_b, owner, axis=1)) & (pos < jnp.take_along_axis(hi_b, owner, axis=1))
    rank_d = jnp.where(counted, rank, -1)
    small = iota((LN, LN), 0).astype(F32).astype(BF16)
    one, none = jnp.ones((LN, LN), BF16), jnp.zeros((LN, LN), BF16)

    def hot(row, value=one):
        return jnp.where(jnp.broadcast_to(row.astype(F32).astype(BF16), (LN, LN)) == small, value, none)

    for t in range(8):
        for r in range(8):
            dedup[r * LN:(r + 1) * LN, t * LN:(t + 1) * LN] = hot(rank_d[t:t + 1, :] - r * LN)

    h = tok // LN
    tile_first = ((h != prev(h)) | (pos == 0)).astype(I32)
    half = h % 2
    jc = owner % 2
    jp = ((owner // 2) % n, (owner // (2 * n)) % n, owner // (2 * n * n))
    lo = tok % LN
    val = (first * (rank % LN + LN) * (1 + 255 * half)).astype(F32)
    starts = [(tile_first * jnp.where(half == hf, part, 0)).astype(F32)
              for hf in range(2) for part in (rank // LN, rank % LN)]
    sub32 = iota((32, LN), 0)
    for t in range(8):
        cols = slice(t * LN, (t + 1) * LN)
        r = slice(t, t + 1)
        lohot[0:LN, cols] = hot(lo[r, :], jnp.broadcast_to(val[r, :].astype(BF16), (LN, LN)))
        lohot[LN:160, cols] = jnp.where(
            sub32 < 8, starts[0][r, :], jnp.where(sub32 < 16, starts[1][r, :], jnp.where(
                sub32 < 24, starts[2][r, :], starts[3][r, :]))).astype(BF16)
    coord = (cx, cy, cz)
    for a, (b2, b3) in enumerate(((2, 1), (2, 0), (1, 0))):
        row = ((jp[a] - coord[a] + n) % n) * inner + jp[b2] * (2 * n) + jp[b3] * 2 + jc
        for t in range(8):
            onehot[:, t * LN:(t + 1) * LN] = hot(row[t:t + 1, :])
        tb = lax.dot_general(onehot[...], lohot[0:LN, :], NT, preferred_element_type=F32).astype(I32)
        us = lax.dot_general(lohot[LN:160, :], onehot[...], NT, preferred_element_type=F32).astype(I32)
        for d in range(n):
            tab_out[a, d, 0:inner, :] = tb[d * inner:(d + 1) * inner, :]
            for hf in range(2):
                tab_out[a, d, inner + hf:inner + hf + 1, :] = us[16 * hf:16 * hf + 1] * LN + us[16 * hf + 8:16 * hf + 9]

    for c in in_copies:
        c.wait()
    lg = jnp.dot(hid[...], w[...], preferred_element_type=F32)
    logits_out[...] = lg
    lm = jnp.max(lg, axis=1, keepdims=True)
    lz = jnp.sum(jnp.exp(lg - lm), axis=1, keepdims=True)

    tau = tau_ref[0]

    def score_step(c, carry):
        for i in range(2):
            key_copy(2 * c + i).wait()

            @pl.when(2 * c + i + AHEAD < nk)
            def _():
                key_copy(2 * c + i + AHEAD).start()

        rows = pl.ds(c * 256, 256)
        cross = lax.dot_general(hid[...], keys[rows, :], NT, preferred_element_type=F32)
        sq = jnp.zeros((256, LN), F32)
        for t in range(keys.shape[1] // LN):
            k = keys[rows, t * LN:(t + 1) * LN].astype(F32)
            sq = sq + k * k
        norm = jnp.sum(sq.T, axis=0, keepdims=True)
        sc = (2.0 * cross - norm) / tau
        score[2 * c] = sc[:, :LN]
        score[2 * c + 1] = sc[:, LN:]
        return carry

    lax.fori_loop(0, nk // 2, score_step, 0)

    sc = [score[t] for t in range(8)]
    m = jnp.max(functools.reduce(jnp.maximum, sc), axis=1, keepdims=True)
    z = jnp.zeros((64, LN), F32)
    for t in range(8):
        e = jnp.exp(sc[t] - m)
        z = z + e
        hi = e.astype(BF16)
        r1 = e - hi.astype(F32)
        mid = r1.astype(BF16)
        low = (r1 - mid.astype(F32)).astype(BF16)
        cols = slice(t * LN, (t + 1) * LN)
        e3[0:64, cols] = hi
        e3[64:LN, cols] = mid
        e3[LN:192, cols] = low
    z = jnp.sum(z, axis=1, keepdims=True)
    l64 = iota((64, LN), 1)
    stat = jnp.where(l64 == 0, m, jnp.where(l64 == 1, z, jnp.where(l64 == 2, lm, lz)))
    row_outs = (rows0, rows1, rows2)
    for h in range(2):
        for out, (r0, nr) in zip(row_outs, GROUPS):
            out[h, 8] = stat[h * HALF + r0:h * HALF + r0 + nr]
    for c in range(4):
        dd = lax.dot_general(e3[...], dedup[c * 256:(c + 1) * 256, :], NT, preferred_element_type=F32)
        eu = dd[0:64] + (dd[64:LN] + dd[LN:192])
        for h in range(2):
            for out, (r0, nr) in zip(row_outs, GROUPS):
                for t in range(2):
                    out[h, 2 * c + t] = eu[h * HALF + r0:h * HALF + r0 + nr, t * LN:(t + 1) * LN]


def exchange_kernel(n, own0, own1, own2, logits, own_tab, lam_ref, out_ref,
                    tab_pair, tab, tab_smem, list0, list1, list2, scaled0, scaled1, scaled2,
                    part20, part21, part22, relay0, relay1, relay2, recv20, recv21, recv22,
                    part30, part31, part32, recv30, recv31, recv32, fin, fin_in,
                    swap_sem, tab_send, tab_recv, smem_sem,
                    send1, recv1, send2, recv2_sem, send_relay, recv_relay, send3, recv3_sem):
    inner = 2 * n * n
    mid = 2 * n
    block = 2 * mid
    device, core, cx, cy, cz = coordinates(n)
    other = 1 - core
    partner = device + 1 - 2 * core
    pcoord, pstride = (cx, cy, cz), (2, 2 * n, 2 * n * n)

    def axes_of(c):
        return ((cx + c * (cy - cx), cy + c * (cx - cy), cz), (2 + c * (2 * n - 2), 2 * n + c * (2 - 2 * n), 2 * n * n))

    coord, stride = axes_of(core)
    coord_o, stride_o = axes_of(other)
    axis_of = (core, other, 2)
    row_stride = ((2, 2 * n), (2 * n, 2), (stride[0], stride[1]))
    own, lists, scaled = (own0, own1, own2), (list0, list1, list2), (scaled0, scaled1, scaled2)
    part2, relay, recv2 = (part20, part21, part22), (relay0, relay1, relay2), (recv20, recv21, recv22)
    part3, recv3 = (part30, part31, part32), (recv30, recv31, recv32)

    def wrap(a):
        return lax.rem(a, n)

    def peer(v, d):
        return device + stride[v] * (wrap(coord[v] + d) - coord[v])

    def peer_other(v, d):
        return partner + stride_o[v] * (wrap(coord_o[v] + d) - coord_o[v])

    def axis_peer(start, a, d):
        return start + pstride[a] * (wrap(pcoord[a] + d) - pcoord[a])

    def remote(src, dst, ssem, rsem, dev):
        return pltpu.make_async_remote_copy(src_ref=src, dst_ref=dst, send_sem=ssem, recv_sem=rsem,
                                            device_id={'model': dev}, device_id_type=pl.DeviceIdType.MESH)

    near = (1, n - 1) if n > 2 else (1,)
    far = tuple(range(2, n - 1))
    order = (1, 2, 0)
    sends = []

    def go(c):
        c.start()
        sends.append(c)

    barrier = pltpu.get_barrier_semaphore()
    partners = [partner] + [axis_peer(start, a, d) for start in (device, partner) for a in range(3) for d in range(1, n)]
    for p in partners:
        pl.semaphore_signal(barrier, inc=1, device_id={'model': p}, device_id_type=pl.DeviceIdType.MESH)
    for g in range(3):
        for i in range(2 * n):
            scaled[g][i, 8] = jnp.zeros(scaled[g].shape[2:], F32)
    pl.semaphore_wait(barrier, len(partners))

    tab_swap = remote(own_tab.at[:, 0], tab_pair, swap_sem.at[0, 0], swap_sem.at[1, 0], partner)
    row_swap = [remote(own[g].at[other], lists[g].at[0], swap_sem.at[0, 1 + g], swap_sem.at[1, 1 + g], partner)
                for g in range(3)]

    def tab_copy(a, d, l):
        return remote(own_tab.at[a, d], tab.at[a, n - d - 1, l], tab_send.at[a, d - 1, l], tab_recv.at[a, n - d - 1, l],
                      axis_peer(partner if l else device, a, d))

    def row_copy(g, d, l):
        return remote(own[g].at[other if l else core], lists[g].at[2 * (n - d) - 1 + l], send1.at[g, d - 1, l],
                      recv1.at[g, n - d - 1, l], peer_other(g, d) if l else peer(g, d))

    def row_relay(g, l):
        frm, to = (n - 1, 1) if l == 0 else (1, n - 1)
        return remote(lists[g].at[2 * frm - 1 + l], lists[g].at[3 + l], send1.at[g, 1, l], recv1.at[g, 1, l], peer(g, to))

    for g in order:
        for d in near:
            for l in range(2):
                go(row_copy(g, d, l))
    for g in order:
        go(row_swap[g])
    go(tab_swap)
    for d in far + near:
        for a in range(3):
            for l in range(2):
                go(tab_copy(a, d, l))

    def stats(tiles, counted=None):
        shape = tiles[0].shape
        ln = iota(shape, 1)
        counted = counted or tiles
        ms = [jnp.broadcast_to(t[:, 0:1], shape) for t in tiles]
        ls = [jnp.broadcast_to(t[:, 2:3], shape) for t in tiles]
        mm = functools.reduce(jnp.maximum, ms)
        ll = functools.reduce(jnp.maximum, ls)
        fs = [jnp.exp(a - mm) for a in ms]
        zz = sum(f * t[:, 1:2] for f, t in zip(fs, counted))
        lzz = sum(jnp.exp(a - ll) * t[:, 3:4] for a, t in zip(ls, counted))
        return fs, jnp.where(ln == 0, mm, jnp.where(ln == 1, zz, jnp.where(ln == 2, ll, lzz)))

    for g in order:
        for d in near:
            for l in range(2):
                row_copy(g, d, l).wait_recv()
        if far:
            for l in range(2):
                go(row_relay(g, l))
        row_swap[g].wait_recv()

    def tab_of(a, k, l):
        if k:
            return tab.at[a, k - 1, l]
        return tab_pair.at[a] if l else own_tab.at[a, 0]

    def list_of(g, k, l):
        if k == 0 and l == 0:
            return own[g].at[core]
        return lists[g].at[2 * k - 1 + l]

    tab_swap.wait_recv()
    for d in range(1, n):
        for l in range(2):
            for a in range(3):
                tab_copy(a, d, l).wait_recv()
    smem_copies = [pltpu.make_async_copy(tab_of(axis_of[g], k, l).at[pl.ds(inner, 2)], tab_smem.at[g, k, l],
                                         smem_sem.at[g, k, l])
                   for g in range(3) for k in range(n) for l in range(2)]
    for c in smem_copies:
        c.start()
    for c in smem_copies:
        c.wait()

    src = [(k, l) for k in range(n) for l in range(2)]

    def partial_hist(g, d2):
        nr = GROUPS[g][1]
        a = axis_of[g]
        c2, c3 = coord[(g + 1) % 3], coord[(g + 2) % 3]
        s2, s3 = row_stride[g]
        base = wrap(c2 + d2) * s2
        ln = iota((nr, LN), 1)

        def pair_step(q, carry):
            d3 = lax.div(q, 2)
            c = q - 2 * d3
            row = base + wrap(c3 + d3) * s3 + c
            acc = [jnp.zeros((nr, LN), F32)] * 2
            for i, (k, l) in enumerate(src):
                packed = jnp.broadcast_to(tab_of(a, k, l)[pl.ds(row, 1), :], (nr, LN))
                for hf in range(2):
                    u = tab_smem[g, k, l, hf, ((n - k) % n) * inner + row]
                    kt = lax.shift_right_logical(u, 7)
                    merged = jnp.where(ln >= (u & 127), scaled[g][i, kt], scaled[g][i, kt + 1])
                    code = lax.shift_right_logical(packed, 8) if hf else packed
                    got = jnp.take_along_axis(merged, code & 127, axis=1, mode='promise_in_bounds')
                    acc[hf] = acc[hf] + jnp.where((code & LN) != 0, got, 0.0)
            t = 2 * q + lax.div(q, n)
            part2[g][d2, t] = acc[0]
            part2[g][d2, t + 1] = acc[1]
            return carry

        lax.fori_loop(0, mid, pair_step, 0, unroll=UNROLL)

    halves = (pl.ds(0, mid + 1), pl.ds(mid, mid + 1))

    def copy2(g, d):
        i = 0 if d == 1 else 1
        return remote(part2[g].at[d], recv2[g].at[i], send2.at[g, i], recv2_sem.at[g, i], peer((g + 1) % 3, d))

    def copy2_relay(g, i):
        return remote(part2[g].at[2, halves[i]], relay[g].at[i], send_relay.at[g, i], recv_relay.at[g, i],
                      peer((g + 1) % 3, near[i]))

    def copy3(g, d):
        return remote(part3[g].at[d], recv3[g].at[n - d - 1], send3.at[g, d - 1], recv3_sem.at[g, n - d - 1],
                      peer((g + 2) % 3, d))

    group_stat = {}
    for g in order:
        if far:
            for l in range(2):
                row_relay(g, l).wait_recv()
        fs, group_stat[g] = stats([list_of(g, k, l)[8] for k, l in src])
        for i, (k, l) in enumerate(src):
            rows = list_of(g, k, l)
            for t in range(8):
                scaled[g][i, t] = rows[t] * fs[i]
        for d2 in far + near + (0,):
            part2[g][d2, mid] = group_stat[g]
        for d2 in far:
            partial_hist(g, d2)
            for i in range(2):
                go(copy2_relay(g, i))
    for g in order:
        for d2 in near:
            partial_hist(g, d2)
    for g in order:
        for i, d2 in enumerate(near):
            if far:
                copy2_relay(g, i).wait_recv()
                there = relay[g][i, 0 if i else mid]
                zero = jnp.zeros(there.shape, F32)
                fs, tile = stats([group_stat[g], there], [group_stat[g], zero if i else there])
                for t in range(block + 1):
                    r = t - i * mid
                    if t == mid:
                        part2[g][d2, t] = tile
                    elif 0 <= r <= mid:
                        part2[g][d2, t] = part2[g][d2, t] * fs[0] + relay[g][i, r] * fs[1]
                    else:
                        part2[g][d2, t] = part2[g][d2, t] * fs[0]
            go(copy2(g, d2))
    for g in order:
        partial_hist(g, 0)

    for g in order:
        for d in near:
            copy2(g, d).wait_recv()
        parts = [part2[g].at[0]] + [recv2[g].at[i] for i in range(len(near))]
        fs, tile = stats([p[mid] for p in parts])
        for d3 in far + near + (0,):
            for ch in range(4):
                q = d3 * 4 + ch
                q = q + q // mid
                part3[g][d3, ch] = sum(p[q] * f for p, f in zip(parts, fs))
            part3[g][d3, 4] = tile
            if d3:
                go(copy3(g, d3))

    for g in order:
        r0, nr = GROUPS[g]
        for d in range(1, n):
            copy3(g, d).wait_recv()
        parts = [part3[g].at[0]] + [recv3[g].at[k] for k in range(n - 1)]
        fs, tile = stats([p[4] for p in parts])
        for ch in range(4):
            fin[ch // 2, ch % 2, r0:r0 + nr] = sum(p[ch] * f for p, f in zip(parts, fs))
        for c in range(2):
            fin[c, 2, r0:r0 + nr] = tile

    back = remote(fin.at[other], fin_in, swap_sem.at[0, 4], swap_sem.at[1, 4], partner)
    go(back)
    lam = lam_ref[0]

    def finish(block_ref, rows_half):
        st = block_ref[2]
        zz, ll, lzz = st[:, 1:2], st[:, 2:3], st[:, 3:4]
        rows = pl.ds(pl.multiple_of(rows_half * HALF, 8), HALF)
        for hf in range(2):
            cols = slice(hf * LN, (hf + 1) * LN)
            lm_exp = jnp.exp(logits[rows, cols] - ll)
            out_ref[rows, cols] = jnp.log(lam * (block_ref[hf] / zz) + (1.0 - lam) * (lm_exp / lzz))

    finish(fin.at[core], core)
    back.wait_recv()
    finish(fin_in, other)
    for c in sends:
        c.wait_send()


def step(n, hidden, w_local, keys_local, tok_local, bounds_local, tau, lam):
    tab_rows = 2 * n * n + 8
    block = 4 * n
    dim = hidden.shape[1]
    V, DMA = pltpu.VMEM, pltpu.SemaphoreType.DMA
    vm = pl.BlockSpec(memory_space=pltpu.VMEM)
    sm = pl.BlockSpec(memory_space=pltpu.SMEM)
    hbm = pl.BlockSpec(memory_space=pl.ANY)
    *rows, logits, tab = pl.pallas_call(
        functools.partial(local_kernel, n),
        out_shape=tuple(pltpu.VMEM((2, 9, nr, LN), F32) for _, nr in GROUPS) + (
            pltpu.VMEM((64, 256), F32),
            pltpu.VMEM((3, n, tab_rows, LN), I32)),
        in_specs=[vm, vm, sm, hbm, hbm, hbm],
        out_specs=(vm,) * 5,
        scratch_shapes=[
            V((64, dim), BF16), V((dim, 256), BF16), V((EN, dim), BF16), V((8, 64, LN), F32),
            V((EN, EN), BF16), V((LN, EN), BF16), V((160, EN), BF16), V((192, EN), BF16),
            DMA((2,)), DMA((8,))],
        name='local_scores',
    )(tok_local.reshape(8, LN), bounds_local, tau.reshape(1), hidden, w_local, keys_local)

    def per_group(*lead):
        return [V((*lead, nr, LN), F32) for _, nr in GROUPS]

    m = n - 1
    return pl.pallas_call(
        functools.partial(exchange_kernel, n),
        out_shape=jax.ShapeDtypeStruct((64, 256), F32),
        in_specs=[vm] * 5 + [sm],
        out_specs=vm,
        scratch_shapes=[
            V((3, tab_rows, LN), I32), V((3, m, 2, tab_rows, LN), I32), pltpu.SMEM((3, n, 2, 2, LN), I32),
            *per_group(2 * n - 1, 9), *per_group(2 * n, 9), *per_group(n, block + 1), *per_group(2, block // 2 + 1),
            *per_group(2, block + 1), *per_group(n, 5), *per_group(m, 5),
            V((2, 3, HALF, LN), F32), V((3, HALF, LN), F32),
            DMA((2, 5)), DMA((3, m, 2)), DMA((3, m, 2)), DMA((3, n, 2)),
            DMA((3, m, 2)), DMA((3, m, 2)), DMA((3, 2)), DMA((3, 2)), DMA((3, 2)), DMA((3, 2)), DMA((3, m)), DMA((3, m))],
        compiler_params=pltpu.CompilerParams(collective_id=0, has_side_effects=True),
        name='exchange',
    )(*[pltpu.with_memory_space_constraint(x, pltpu.VMEM) for x in (*rows, logits, tab)], lam.reshape(1))


def solution(mesh):
    n = round((mesh.shape['model'] // 2) ** (1 / 3))
    return jax.shard_map(functools.partial(step, n), mesh=mesh,
                         in_specs=(P('data', None), P(None, 'model'), P('model', None), P('model'),
                                   P('model', None), P(), P()),
                         out_specs=P('data', 'model'), check_vma=False)
```

```python
import functools

import jax
import jax.numpy as jnp
from jax import lax
from jax.experimental import pallas as pl
from jax.experimental.pallas import tpu as pltpu
from jax.sharding import PartitionSpec as P

F32, BF16, I32 = jnp.float32, jnp.bfloat16, jnp.int32
GROUPS = ((0, 16), (16, 8), (24, 8))
UNROLL = 4
AHEAD = 4
HALF = 32
LN, EN = 128, 1024
NT = (((1,), (1,)), ((), ()))


def iota(shape, axis):
    return lax.broadcasted_iota(I32, shape, axis)


def coordinates(n):
    device = lax.axis_index('model')
    return device, device % 2, (device // 2) % n, (device // (2 * n)) % n, device // (2 * n * n)


def local_kernel(n, tok_hbm, bounds_hbm, tau_hbm, hid_hbm, w_hbm, keys_hbm, rows0, rows1, rows2, logits_out, tab_out,
                 tok_ref, bounds_ref, tau_ref, hid, w, keys, score, dedup, onehot, lohot, e3, in_sem, key_sem):
    inner = 2 * n * n
    _, _, cx, cy, cz = coordinates(n)
    operands = ((tok_hbm, tok_ref), (bounds_hbm, bounds_ref), (tau_hbm, tau_ref), (hid_hbm, hid), (w_hbm, w))
    in_copies = [pltpu.make_async_copy(a, b, in_sem.at[i]) for i, (a, b) in enumerate(operands)]
    for c in in_copies[:-1]:
        c.start()
    kchunk = LN
    nk = keys.shape[0] // kchunk

    def key_copy(c):
        rows = pl.ds(c * kchunk, kchunk)
        return pltpu.make_async_copy(keys_hbm.at[rows], keys.at[rows], key_sem.at[c])

    for c in range(AHEAD):
        key_copy(c).start()

    lane = iota((8, LN), 1)
    sub = iota((8, LN), 0)
    pos = sub * LN + lane

    def prev(a):
        r = pltpu.roll(a, 1, 1)
        return jnp.where(lane == 0, pltpu.roll(r, 1, 0), r)

    in_copies[0].wait()
    tok = tok_ref[...]
    first = ((tok != prev(tok)) | (pos == 0)).astype(I32)
    c = first
    for sh in (1, 2, 4, 8, 16, 32, 64):
        c = c + jnp.where(lane >= sh, pltpu.roll(c, sh, 1), 0)
    tot = jnp.broadcast_to(c[:, 127:LN], (8, LN))
    acc = tot
    for sh in (1, 2, 4):
        acc = acc + jnp.where(sub >= sh, pltpu.roll(acc, sh, 0), 0)
    rank = c + acc - tot - 1

    owner = tok // 256
    in_copies[1].wait()
    bnd = bounds_ref[...]
    nb = bnd.shape[1] - 1
    lo_b = jnp.broadcast_to(bnd[:, :nb], (8, nb))
    hi_b = jnp.broadcast_to(bnd[:, 1:], (8, nb))
    if nb < LN:
        lo_b = jnp.concatenate([lo_b, jnp.zeros((8, LN - nb), I32)], axis=1)
        hi_b = jnp.concatenate([hi_b, jnp.zeros((8, LN - nb), I32)], axis=1)
    counted = (pos >= jnp.take_along_axis(lo_b, owner, axis=1)) & (pos < jnp.take_along_axis(hi_b, owner, axis=1))
    rank_d = jnp.where(counted, rank, -1)
    small = iota((LN, LN), 0).astype(F32).astype(BF16)
    one, none = jnp.ones((LN, LN), BF16), jnp.zeros((LN, LN), BF16)

    def hot(row, value=one):
        return jnp.where(jnp.broadcast_to(row.astype(F32).astype(BF16), (LN, LN)) == small, value, none)

    for t in range(8):
        for r in range(8):
            dedup[r * LN:(r + 1) * LN, t * LN:(t + 1) * LN] = hot(rank_d[t:t + 1, :] - r * LN)

    h = tok // LN
    tile_first = ((h != prev(h)) | (pos == 0)).astype(I32)
    half = h % 2
    jc = owner % 2
    jp = ((owner // 2) % n, (owner // (2 * n)) % n, owner // (2 * n * n))
    lo = tok % LN
    val = (first * (rank % LN + LN) * (1 + 255 * half)).astype(F32)
    starts = [(tile_first * jnp.where(half == hf, part, 0)).astype(F32)
              for hf in range(2) for part in (rank // LN, rank % LN)]
    sub32 = iota((32, LN), 0)
    for t in range(8):
        cols = slice(t * LN, (t + 1) * LN)
        r = slice(t, t + 1)
        lohot[0:LN, cols] = hot(lo[r, :], jnp.broadcast_to(val[r, :].astype(BF16), (LN, LN)))
        lohot[LN:160, cols] = jnp.where(
            sub32 < 8, starts[0][r, :], jnp.where(sub32 < 16, starts[1][r, :], jnp.where(
                sub32 < 24, starts[2][r, :], starts[3][r, :]))).astype(BF16)
    coord = (cx, cy, cz)
    for a, (b2, b3) in enumerate(((2, 1), (2, 0), (1, 0))):
        row = ((jp[a] - coord[a] + n) % n) * inner + jp[b2] * (2 * n) + jp[b3] * 2 + jc
        for t in range(8):
            onehot[:, t * LN:(t + 1) * LN] = hot(row[t:t + 1, :])
        tb = lax.dot_general(onehot[...], lohot[0:LN, :], NT, preferred_element_type=F32).astype(I32)
        us = lax.dot_general(lohot[LN:160, :], onehot[...], NT, preferred_element_type=F32).astype(I32)
        for d in range(n):
            tab_out[a, d, 0:inner, :] = tb[d * inner:(d + 1) * inner, :]
            for hf in range(2):
                tab_out[a, d, inner + hf:inner + hf + 1, :] = us[16 * hf:16 * hf + 1] * LN + us[16 * hf + 8:16 * hf + 9]

    in_copies[-1].start()
    for c in in_copies[2:-1]:
        c.wait()
    tau = tau_ref[0]

    def score_step(c, carry):
        for i in range(2):
            key_copy(2 * c + i).wait()

            @pl.when(2 * c + i + AHEAD < nk)
            def _():
                key_copy(2 * c + i + AHEAD).start()

        rows = pl.ds(c * 256, 256)
        cross = lax.dot_general(hid[...], keys[rows, :], NT, preferred_element_type=F32)
        sq = jnp.zeros((256, LN), F32)
        for t in range(keys.shape[1] // LN):
            k = keys[rows, t * LN:(t + 1) * LN].astype(F32)
            sq = sq + k * k
        norm = jnp.sum(sq.T, axis=0, keepdims=True)
        sc = (2.0 * cross - norm) / tau
        score[2 * c] = sc[:, :LN]
        score[2 * c + 1] = sc[:, LN:]
        return carry

    lax.fori_loop(0, nk // 2, score_step, 0)

    in_copies[-1].wait()
    lg = jnp.dot(hid[...], w[...], preferred_element_type=F32)
    logits_out[...] = lg
    lm = jnp.max(lg, axis=1, keepdims=True)
    lz = jnp.sum(jnp.exp(lg - lm), axis=1, keepdims=True)

    sc = [score[t] for t in range(8)]
    m = jnp.max(functools.reduce(jnp.maximum, sc), axis=1, keepdims=True)
    z = jnp.zeros((64, LN), F32)
    for t in range(8):
        e = jnp.exp(sc[t] - m)
        z = z + e
        hi = e.astype(BF16)
        r1 = e - hi.astype(F32)
        mid = r1.astype(BF16)
        low = (r1 - mid.astype(F32)).astype(BF16)
        cols = slice(t * LN, (t + 1) * LN)
        e3[0:64, cols] = hi
        e3[64:LN, cols] = mid
        e3[LN:192, cols] = low
    z = jnp.sum(z, axis=1, keepdims=True)
    l64 = iota((64, LN), 1)
    stat = jnp.where(l64 == 0, m, jnp.where(l64 == 1, z, jnp.where(l64 == 2, lm, lz)))
    row_outs = (rows0, rows1, rows2)
    for h in range(2):
        for out, (r0, nr) in zip(row_outs, GROUPS):
            out[h, 8] = stat[h * HALF + r0:h * HALF + r0 + nr]
    for c in range(4):
        dd = lax.dot_general(e3[...], dedup[c * 256:(c + 1) * 256, :], NT, preferred_element_type=F32)
        eu = dd[0:64] + (dd[64:LN] + dd[LN:192])
        for h in range(2):
            for out, (r0, nr) in zip(row_outs, GROUPS):
                for t in range(2):
                    out[h, 2 * c + t] = eu[h * HALF + r0:h * HALF + r0 + nr, t * LN:(t + 1) * LN]


def exchange_kernel(n, own0, own1, own2, own_tab, lam_hbm, hist_out, stat_out,
                    lam_ref, lam_sem, tab_pair, tab, tab_smem, list0, list1, list2, scaled0, scaled1, scaled2,
                    part20, part21, part22, relay0, relay1, relay2, recv20, recv21, recv22,
                    part30, part31, part32, recv30, recv31, recv32,
                    swap_sem, tab_send, tab_recv, smem_sem,
                    send1, recv1, send2, recv2_sem, send_relay, recv_relay, send3, recv3_sem):
    inner = 2 * n * n
    mid = 2 * n
    block = 2 * mid
    device, core, cx, cy, cz = coordinates(n)
    other = 1 - core
    partner = device + 1 - 2 * core
    pcoord, pstride = (cx, cy, cz), (2, 2 * n, 2 * n * n)

    def axes_of(c):
        return ((cx + c * (cy - cx), cy + c * (cx - cy), cz), (2 + c * (2 * n - 2), 2 * n + c * (2 - 2 * n), 2 * n * n))

    coord, stride = axes_of(core)
    coord_o, stride_o = axes_of(other)
    axis_of = (core, other, 2)
    row_stride = ((2, 2 * n), (2 * n, 2), (stride[0], stride[1]))
    own, lists, scaled = (own0, own1, own2), (list0, list1, list2), (scaled0, scaled1, scaled2)
    part2, relay, recv2 = (part20, part21, part22), (relay0, relay1, relay2), (recv20, recv21, recv22)
    part3, recv3 = (part30, part31, part32), (recv30, recv31, recv32)

    def wrap(a):
        return lax.rem(a, n)

    def peer(v, d):
        return device + stride[v] * (wrap(coord[v] + d) - coord[v])

    def peer_other(v, d):
        return partner + stride_o[v] * (wrap(coord_o[v] + d) - coord_o[v])

    def axis_peer(start, a, d):
        return start + pstride[a] * (wrap(pcoord[a] + d) - pcoord[a])

    def remote(src, dst, ssem, rsem, dev):
        return pltpu.make_async_remote_copy(src_ref=src, dst_ref=dst, send_sem=ssem, recv_sem=rsem,
                                            device_id={'model': dev}, device_id_type=pl.DeviceIdType.MESH)

    near = (1, n - 1) if n > 2 else (1,)
    far = tuple(range(2, n - 1))
    order = (1, 2, 0)
    sends = []

    def go(c):
        c.start()
        sends.append(c)

    lam_copy = pltpu.make_async_copy(lam_hbm, lam_ref, lam_sem)
    lam_copy.start()
    barrier = pltpu.get_barrier_semaphore()
    partners = [partner] + [axis_peer(start, a, d) for start in (device, partner) for a in range(3) for d in range(1, n)]
    for p in partners:
        pl.semaphore_signal(barrier, inc=1, device_id={'model': p}, device_id_type=pl.DeviceIdType.MESH)
    for g in range(3):
        for i in range(2 * n):
            scaled[g][i, 8] = jnp.zeros(scaled[g].shape[2:], F32)
    pl.semaphore_wait(barrier, len(partners))

    tab_swap = remote(own_tab.at[:, 0], tab_pair, swap_sem.at[0, 0], swap_sem.at[1, 0], partner)
    row_swap = [remote(own[g].at[other], lists[g].at[0], swap_sem.at[0, 1 + g], swap_sem.at[1, 1 + g], partner)
                for g in range(3)]

    def tab_copy(a, d, l):
        return remote(own_tab.at[a, d], tab.at[a, n - d - 1, l], tab_send.at[a, d - 1, l], tab_recv.at[a, n - d - 1, l],
                      axis_peer(partner if l else device, a, d))

    def row_copy(g, d, l):
        return remote(own[g].at[other if l else core], lists[g].at[2 * (n - d) - 1 + l], send1.at[g, d - 1, l],
                      recv1.at[g, n - d - 1, l], peer_other(g, d) if l else peer(g, d))

    def row_relay(g, l):
        frm, to = (n - 1, 1) if l == 0 else (1, n - 1)
        return remote(lists[g].at[2 * frm - 1 + l], lists[g].at[3 + l], send1.at[g, 1, l], recv1.at[g, 1, l], peer(g, to))

    for g in order:
        for d in near:
            for l in range(2):
                go(row_copy(g, d, l))
    for g in order:
        go(row_swap[g])
    go(tab_swap)
    for d in far + near:
        for a in range(3):
            for l in range(2):
                go(tab_copy(a, d, l))

    def stats(tiles, counted=None):
        shape = tiles[0].shape
        ln = iota(shape, 1)
        counted = counted or tiles
        ms = [jnp.broadcast_to(t[:, 0:1], shape) for t in tiles]
        ls = [jnp.broadcast_to(t[:, 2:3], shape) for t in tiles]
        mm = functools.reduce(jnp.maximum, ms)
        ll = functools.reduce(jnp.maximum, ls)
        fs = [jnp.exp(a - mm) for a in ms]
        zz = sum(f * t[:, 1:2] for f, t in zip(fs, counted))
        lzz = sum(jnp.exp(a - ll) * t[:, 3:4] for a, t in zip(ls, counted))
        return fs, jnp.where(ln == 0, mm, jnp.where(ln == 1, zz, jnp.where(ln == 2, ll, lzz)))

    for g in order:
        for d in near:
            for l in range(2):
                row_copy(g, d, l).wait_recv()
        if far:
            for l in range(2):
                go(row_relay(g, l))
        row_swap[g].wait_recv()

    def tab_of(a, k, l):
        if k:
            return tab.at[a, k - 1, l]
        return tab_pair.at[a] if l else own_tab.at[a, 0]

    def list_of(g, k, l):
        if k == 0 and l == 0:
            return own[g].at[core]
        return lists[g].at[2 * k - 1 + l]

    tab_swap.wait_recv()
    for d in range(1, n):
        for l in range(2):
            for a in range(3):
                tab_copy(a, d, l).wait_recv()
    smem_copies = [pltpu.make_async_copy(tab_of(axis_of[g], k, l).at[pl.ds(inner, 2)], tab_smem.at[g, k, l],
                                         smem_sem.at[g, k, l])
                   for g in range(3) for k in range(n) for l in range(2)]
    for c in smem_copies:
        c.start()
    for c in smem_copies:
        c.wait()

    src = [(k, l) for k in range(n) for l in range(2)]

    def partial_hist(g, d2):
        nr = GROUPS[g][1]
        a = axis_of[g]
        c2, c3 = coord[(g + 1) % 3], coord[(g + 2) % 3]
        s2, s3 = row_stride[g]
        base = wrap(c2 + d2) * s2
        ln = iota((nr, LN), 1)

        def pair_step(q, carry):
            d3 = lax.div(q, 2)
            c = q - 2 * d3
            row = base + wrap(c3 + d3) * s3 + c
            acc = [jnp.zeros((nr, LN), F32)] * 2
            for i, (k, l) in enumerate(src):
                packed = jnp.broadcast_to(tab_of(a, k, l)[pl.ds(row, 1), :], (nr, LN))
                for hf in range(2):
                    u = tab_smem[g, k, l, hf, ((n - k) % n) * inner + row]
                    kt = lax.shift_right_logical(u, 7)
                    merged = jnp.where(ln >= (u & 127), scaled[g][i, kt], scaled[g][i, kt + 1])
                    code = lax.shift_right_logical(packed, 8) if hf else packed
                    got = jnp.take_along_axis(merged, code & 127, axis=1, mode='promise_in_bounds')
                    acc[hf] = acc[hf] + jnp.where((code & LN) != 0, got, 0.0)
            t = 2 * q + lax.div(q, n)
            part2[g][d2, t] = acc[0]
            part2[g][d2, t + 1] = acc[1]
            return carry

        lax.fori_loop(0, mid, pair_step, 0, unroll=UNROLL)

    halves = (pl.ds(0, mid + 1), pl.ds(mid, mid + 1))

    def copy2(g, d):
        i = 0 if d == 1 else 1
        return remote(part2[g].at[d], recv2[g].at[i], send2.at[g, i], recv2_sem.at[g, i], peer((g + 1) % 3, d))

    def copy2_relay(g, i):
        return remote(part2[g].at[2, halves[i]], relay[g].at[i], send_relay.at[g, i], recv_relay.at[g, i],
                      peer((g + 1) % 3, near[i]))

    def copy3(g, d, l):
        return remote(part3[g].at[d, other if l else core], recv3[g].at[n - d - 1, l], send3.at[g, d, l],
                      recv3_sem.at[g, n - d - 1, l], peer((g + 2) % 3, d) + l * (partner - device))

    group_stat = {}
    for g in order:
        if far:
            for l in range(2):
                row_relay(g, l).wait_recv()
        fs, group_stat[g] = stats([list_of(g, k, l)[8] for k, l in src])
        for i, (k, l) in enumerate(src):
            rows = list_of(g, k, l)
            for t in range(8):
                scaled[g][i, t] = rows[t] * fs[i]
        for d2 in far + near + (0,):
            part2[g][d2, mid] = group_stat[g]
        for d2 in far:
            partial_hist(g, d2)
            for i in range(2):
                go(copy2_relay(g, i))
    for g in order:
        for d2 in near:
            partial_hist(g, d2)
        for i, d2 in enumerate(near):
            if far:
                copy2_relay(g, i).wait_recv()
                there = relay[g][i, 0 if i else mid]
                zero = jnp.zeros(there.shape, F32)
                fs, tile = stats([group_stat[g], there], [group_stat[g], zero if i else there])
                for t in range(block + 1):
                    r = t - i * mid
                    if t == mid:
                        part2[g][d2, t] = tile
                    elif 0 <= r <= mid:
                        part2[g][d2, t] = part2[g][d2, t] * fs[0] + relay[g][i, r] * fs[1]
                    else:
                        part2[g][d2, t] = part2[g][d2, t] * fs[0]
            go(copy2(g, d2))
    for g in order:
        partial_hist(g, 0)

    for g in order:
        for d in near:
            copy2(g, d).wait_recv()
        parts = [part2[g].at[0]] + [recv2[g].at[i] for i in range(len(near))]
        fs, tile = stats([p[mid] for p in parts])
        for d3 in far + near + (0,):
            for ch in range(4):
                q = d3 * 4 + ch
                q = q + q // mid
                part3[g][d3, ch // 2, ch % 2] = sum(p[q] * f for p, f in zip(parts, fs))
            for c in range(2):
                part3[g][d3, c, 2] = tile
            for l in range(2):
                if d3 or l:
                    go(copy3(g, d3, l))

    lam_copy.wait()
    for l in range(2):
        for g in order:
            r0, nr = GROUPS[g]
            for d in range(l == 0, n):
                copy3(g, d, l).wait_recv()
            parts = [recv3[g].at[k, l] for k in range(n - 1)] + [recv3[g].at[n - 1, 1] if l else part3[g].at[0, core]]
            fs, tile = stats([p[2] for p in parts])
            rows = pl.ds(pl.multiple_of((other if l else core) * HALF + r0, 8), nr)
            for hf in range(2):
                hist_out[hf, rows] = sum(p[hf] * f for p, f in zip(parts, fs))
            stat_out[rows] = jnp.where(iota((nr, LN), 1) == 4, lam_ref[0], tile)
    for c in sends:
        c.wait_send()


def mixture_kernel(hist, stat, logits, out_ref):
    zz, ll, lzz, lam = (stat[:, i:i + 1] for i in range(1, 5))
    for hf in range(2):
        cols = slice(hf * LN, (hf + 1) * LN)
        lm_exp = jnp.exp(logits[:, cols] - ll)
        out_ref[:, cols] = jnp.log(lam * (hist[hf] / zz) + (1.0 - lam) * (lm_exp / lzz))


def step(n, hidden, w_local, keys_local, tok_local, bounds_local, tau, lam):
    tab_rows = 2 * n * n + 8
    block = 4 * n
    dim = hidden.shape[1]
    V, DMA = pltpu.VMEM, pltpu.SemaphoreType.DMA
    vm = pl.BlockSpec(memory_space=pltpu.VMEM)
    hbm = pl.BlockSpec(memory_space=pl.ANY)
    *rows, logits, tab = pl.pallas_call(
        functools.partial(local_kernel, n),
        out_shape=tuple(pltpu.VMEM((2, 9, nr, LN), F32) for _, nr in GROUPS) + (
            pltpu.VMEM((64, 256), F32),
            pltpu.VMEM((3, n, tab_rows, LN), I32)),
        in_specs=[hbm] * 6,
        out_specs=(vm,) * 5,
        scratch_shapes=[
            V((8, LN), I32), V(bounds_local.shape, I32), pltpu.SMEM((1,), F32), V((64, dim), BF16), V((dim, 256), BF16), V((EN, dim), BF16), V((8, 64, LN), F32),
            V((EN, EN), BF16), V((LN, EN), BF16), V((160, EN), BF16), V((192, EN), BF16),
            DMA((5,)), DMA((8,))],
        name='local_scores',
    )(tok_local.reshape(8, LN), bounds_local, tau.reshape(1), hidden, w_local, keys_local)

    def per_group(*lead):
        return [V((*lead, nr, LN), F32) for _, nr in GROUPS]

    def in_vmem(*arrays):
        return [pltpu.with_memory_space_constraint(x, pltpu.VMEM) for x in arrays]

    m = n - 1
    hist, stat = pl.pallas_call(
        functools.partial(exchange_kernel, n),
        out_shape=(V((2, 64, LN), F32), V((64, LN), F32)),
        in_specs=[vm] * 4 + [hbm],
        out_specs=(vm, vm),
        scratch_shapes=[
            pltpu.SMEM((1,), F32), DMA(()), V((3, tab_rows, LN), I32), V((3, m, 2, tab_rows, LN), I32),
            pltpu.SMEM((3, n, 2, 2, LN), I32),
            *per_group(2 * n - 1, 9), *per_group(2 * n, 9), *per_group(n, block + 1), *per_group(2, block // 2 + 1),
            *per_group(2, block + 1), *per_group(n, 2, 3), *per_group(n, 2, 3),
            DMA((2, 4)), DMA((3, m, 2)), DMA((3, m, 2)), DMA((3, n, 2)),
            DMA((3, m, 2)), DMA((3, m, 2)), DMA((3, 2)), DMA((3, 2)), DMA((3, 2)), DMA((3, 2)),
            DMA((3, n, 2)), DMA((3, n, 2))],
        compiler_params=pltpu.CompilerParams(collective_id=0, has_side_effects=True),
        name='exchange',
    )(*in_vmem(*rows, tab), lam.reshape(1))
    return pl.pallas_call(
        mixture_kernel, out_shape=jax.ShapeDtypeStruct((64, 256), F32), in_specs=[vm] * 3, out_specs=vm, name='mixture',
    )(*in_vmem(hist, stat, logits))


def solution(mesh):
    n = round((mesh.shape['model'] // 2) ** (1 / 3))
    return jax.shard_map(functools.partial(step, n), mesh=mesh,
                         in_specs=(P('data', None), P(None, 'model'), P('model', None), P('model'),
                                   P('model', None), P(), P()),
                         out_specs=P('data', 'model'), check_vma=False)
```

```python
import functools

import jax
import jax.numpy as jnp
from jax import lax
from jax.experimental import pallas as pl
from jax.experimental.pallas import tpu as pltpu
from jax.sharding import PartitionSpec as P

F32, BF16, I32 = jnp.float32, jnp.bfloat16, jnp.int32
GROUPS = ((0, 16), (16, 8), (24, 8))
UNROLL = 4
AHEAD = 4
HALF = 32
LN, EN = 128, 1024
NT = (((1,), (1,)), ((), ()))


def iota(shape, axis):
    return lax.broadcasted_iota(I32, shape, axis)


def coordinates(n):
    device = lax.axis_index('model')
    return device, device % 2, (device // 2) % n, (device // (2 * n)) % n, device // (2 * n * n)


def local_kernel(n, tok_hbm, bounds_hbm, tau_hbm, hid_hbm, w_hbm, keys_hbm, rows0, rows1, rows2, logits_out, tab_out,
                 tok_ref, bounds_ref, tau_ref, hid, w, keys, score, dedup, onehot, lohot, e3, in_sem, key_sem):
    inner = 2 * n * n
    _, _, cx, cy, cz = coordinates(n)
    operands = ((tok_hbm, tok_ref), (bounds_hbm, bounds_ref), (tau_hbm, tau_ref), (hid_hbm, hid), (w_hbm, w))
    in_copies = [pltpu.make_async_copy(a, b, in_sem.at[i]) for i, (a, b) in enumerate(operands)]
    for c in in_copies[:-1]:
        c.start()
    kchunk = LN
    nk = keys.shape[0] // kchunk

    def key_copy(c):
        rows = pl.ds(c * kchunk, kchunk)
        return pltpu.make_async_copy(keys_hbm.at[rows], keys.at[rows], key_sem.at[c])

    for c in range(AHEAD):
        key_copy(c).start()

    lane = iota((8, LN), 1)
    sub = iota((8, LN), 0)
    pos = sub * LN + lane

    def prev(a):
        r = pltpu.roll(a, 1, 1)
        return jnp.where(lane == 0, pltpu.roll(r, 1, 0), r)

    in_copies[0].wait()
    tok = tok_ref[...]
    first = ((tok != prev(tok)) | (pos == 0)).astype(I32)
    c = first
    for sh in (1, 2, 4, 8, 16, 32, 64):
        c = c + jnp.where(lane >= sh, pltpu.roll(c, sh, 1), 0)
    tot = jnp.broadcast_to(c[:, 127:LN], (8, LN))
    acc = tot
    for sh in (1, 2, 4):
        acc = acc + jnp.where(sub >= sh, pltpu.roll(acc, sh, 0), 0)
    rank = c + acc - tot - 1

    owner = tok // 256
    in_copies[1].wait()
    bnd = bounds_ref[...]
    nb = bnd.shape[1] - 1
    lo_b = jnp.broadcast_to(bnd[:, :nb], (8, nb))
    hi_b = jnp.broadcast_to(bnd[:, 1:], (8, nb))
    if nb < LN:
        lo_b = jnp.concatenate([lo_b, jnp.zeros((8, LN - nb), I32)], axis=1)
        hi_b = jnp.concatenate([hi_b, jnp.zeros((8, LN - nb), I32)], axis=1)
    counted = (pos >= jnp.take_along_axis(lo_b, owner, axis=1)) & (pos < jnp.take_along_axis(hi_b, owner, axis=1))
    rank_d = jnp.where(counted, rank, -1)
    small = iota((LN, LN), 0).astype(F32).astype(BF16)
    one, none = jnp.ones((LN, LN), BF16), jnp.zeros((LN, LN), BF16)

    def hot(row, value=one):
        return jnp.where(jnp.broadcast_to(row.astype(F32).astype(BF16), (LN, LN)) == small, value, none)

    for t in range(8):
        for r in range(8):
            dedup[r * LN:(r + 1) * LN, t * LN:(t + 1) * LN] = hot(rank_d[t:t + 1, :] - r * LN)

    h = tok // LN
    tile_first = ((h != prev(h)) | (pos == 0)).astype(I32)
    half = h % 2
    jc = owner % 2
    jp = ((owner // 2) % n, (owner // (2 * n)) % n, owner // (2 * n * n))
    lo = tok % LN
    val = (first * (rank % LN + LN) * (1 + 255 * half)).astype(F32)
    starts = [(tile_first * jnp.where(half == hf, part, 0)).astype(F32)
              for hf in range(2) for part in (rank // LN, rank % LN)]
    sub32 = iota((32, LN), 0)
    for t in range(8):
        cols = slice(t * LN, (t + 1) * LN)
        r = slice(t, t + 1)
        lohot[0:LN, cols] = hot(lo[r, :], jnp.broadcast_to(val[r, :].astype(BF16), (LN, LN)))
        lohot[LN:160, cols] = jnp.where(
            sub32 < 8, starts[0][r, :], jnp.where(sub32 < 16, starts[1][r, :], jnp.where(
                sub32 < 24, starts[2][r, :], starts[3][r, :]))).astype(BF16)
    coord = (cx, cy, cz)
    for a, (b2, b3) in enumerate(((2, 1), (2, 0), (1, 0))):
        row = ((jp[a] - coord[a] + n) % n) * inner + jp[b2] * (2 * n) + jp[b3] * 2 + jc
        for t in range(8):
            onehot[:, t * LN:(t + 1) * LN] = hot(row[t:t + 1, :])
        tb = lax.dot_general(onehot[...], lohot[0:LN, :], NT, preferred_element_type=F32).astype(I32)
        us = lax.dot_general(lohot[LN:160, :], onehot[...], NT, preferred_element_type=F32).astype(I32)
        for d in range(n):
            tab_out[a, d, 0:inner, :] = tb[d * inner:(d + 1) * inner, :]
            for hf in range(2):
                tab_out[a, d, inner + hf:inner + hf + 1, :] = us[16 * hf:16 * hf + 1] * LN + us[16 * hf + 8:16 * hf + 9]

    in_copies[-1].start()
    for c in in_copies[2:-1]:
        c.wait()
    tau = tau_ref[0]

    def score_step(c, carry):
        for i in range(2):
            key_copy(2 * c + i).wait()

            @pl.when(2 * c + i + AHEAD < nk)
            def _():
                key_copy(2 * c + i + AHEAD).start()

        rows = pl.ds(c * 256, 256)
        cross = lax.dot_general(hid[...], keys[rows, :], NT, preferred_element_type=F32)
        sq = jnp.zeros((256, LN), F32)
        for t in range(keys.shape[1] // LN):
            k = keys[rows, t * LN:(t + 1) * LN].astype(F32)
            sq = sq + k * k
        norm = jnp.sum(sq.T, axis=0, keepdims=True)
        sc = (2.0 * cross - norm) / tau
        score[2 * c] = sc[:, :LN]
        score[2 * c + 1] = sc[:, LN:]
        return carry

    lax.fori_loop(0, nk // 2, score_step, 0)

    in_copies[-1].wait()
    lg = jnp.dot(hid[...], w[...], preferred_element_type=F32)
    logits_out[...] = lg
    lm = jnp.max(lg, axis=1, keepdims=True)
    lz = jnp.sum(jnp.exp(lg - lm), axis=1, keepdims=True)

    sc = [score[t] for t in range(8)]
    m = jnp.max(functools.reduce(jnp.maximum, sc), axis=1, keepdims=True)
    z = jnp.zeros((64, LN), F32)
    for t in range(8):
        e = jnp.exp(sc[t] - m)
        z = z + e
        hi = e.astype(BF16)
        r1 = e - hi.astype(F32)
        mid = r1.astype(BF16)
        low = (r1 - mid.astype(F32)).astype(BF16)
        cols = slice(t * LN, (t + 1) * LN)
        e3[0:64, cols] = hi
        e3[64:LN, cols] = mid
        e3[LN:192, cols] = low
    z = jnp.sum(z, axis=1, keepdims=True)
    l64 = iota((64, LN), 1)
    stat = jnp.where(l64 == 0, m, jnp.where(l64 == 1, z, jnp.where(l64 == 2, lm, lz)))
    row_outs = (rows0, rows1, rows2)
    for h in range(2):
        for out, (r0, nr) in zip(row_outs, GROUPS):
            out[h, 8] = stat[h * HALF + r0:h * HALF + r0 + nr]
    for c in range(4):
        dd = lax.dot_general(e3[...], dedup[c * 256:(c + 1) * 256, :], NT, preferred_element_type=F32)
        eu = dd[0:64] + (dd[64:LN] + dd[LN:192])
        for h in range(2):
            for out, (r0, nr) in zip(row_outs, GROUPS):
                for t in range(2):
                    out[h, 2 * c + t] = eu[h * HALF + r0:h * HALF + r0 + nr, t * LN:(t + 1) * LN]


def exchange_kernel(n, own0, own1, own2, own_tab, lam_hbm, hist_out, stat_out,
                    lam_ref, lam_sem, tab_pair, tab, tab_smem, list0, list1, list2, scaled0, scaled1, scaled2,
                    part20, part21, part22, relay0, relay1, relay2, recv20, recv21, recv22,
                    part30, part31, part32, recv30, recv31, recv32,
                    swap_sem, tab_send, tab_recv, smem_sem,
                    send1, recv1, send2, recv2_sem, send_relay, recv_relay, send3, recv3_sem):
    inner = 2 * n * n
    mid = 2 * n
    block = 2 * mid
    device, core, cx, cy, cz = coordinates(n)
    other = 1 - core
    partner = device + 1 - 2 * core
    pcoord, pstride = (cx, cy, cz), (2, 2 * n, 2 * n * n)

    def axes_of(c):
        return ((cx + c * (cy - cx), cy + c * (cx - cy), cz), (2 + c * (2 * n - 2), 2 * n + c * (2 - 2 * n), 2 * n * n))

    coord, stride = axes_of(core)
    coord_o, stride_o = axes_of(other)
    axis_of = (core, other, 2)
    row_stride = ((2, 2 * n), (2 * n, 2), (stride[0], stride[1]))
    own, lists, scaled = (own0, own1, own2), (list0, list1, list2), (scaled0, scaled1, scaled2)
    part2, relay, recv2 = (part20, part21, part22), (relay0, relay1, relay2), (recv20, recv21, recv22)
    part3, recv3 = (part30, part31, part32), (recv30, recv31, recv32)

    def wrap(a):
        return lax.rem(a, n)

    def peer(v, d):
        return device + stride[v] * (wrap(coord[v] + d) - coord[v])

    def peer_other(v, d):
        return partner + stride_o[v] * (wrap(coord_o[v] + d) - coord_o[v])

    def axis_peer(start, a, d):
        return start + pstride[a] * (wrap(pcoord[a] + d) - pcoord[a])

    def remote(src, dst, ssem, rsem, dev):
        return pltpu.make_async_remote_copy(src_ref=src, dst_ref=dst, send_sem=ssem, recv_sem=rsem,
                                            device_id={'model': dev}, device_id_type=pl.DeviceIdType.MESH)

    near = (1, n - 1) if n > 2 else (1,)
    far = tuple(range(2, n - 1))
    order = (1, 2, 0)
    sends = []

    def go(c):
        c.start()
        sends.append(c)

    lam_copy = pltpu.make_async_copy(lam_hbm, lam_ref, lam_sem)
    lam_copy.start()
    barrier = pltpu.get_barrier_semaphore()
    partners = [partner] + [axis_peer(start, a, d) for start in (device, partner) for a in range(3) for d in range(1, n)]
    for p in partners:
        pl.semaphore_signal(barrier, inc=1, device_id={'model': p}, device_id_type=pl.DeviceIdType.MESH)
    for g in range(3):
        for i in range(2 * n):
            scaled[g][i, 8] = jnp.zeros(scaled[g].shape[2:], F32)
    pl.semaphore_wait(barrier, len(partners))

    tab_swap = remote(own_tab.at[:, 0], tab_pair, swap_sem.at[0, 0], swap_sem.at[1, 0], partner)
    row_swap = [remote(own[g].at[other], lists[g].at[0], swap_sem.at[0, 1 + g], swap_sem.at[1, 1 + g], partner)
                for g in range(3)]

    def tab_copy(a, d):
        return remote(own_tab.at[a, d], tab.at[a, n - d - 1, 0], tab_send.at[a, d - 1, 0], tab_recv.at[a, n - d - 1, 0],
                      axis_peer(device, a, d))

    def tab_share(a, d):
        i = n - d - 1
        return remote(tab.at[a, i, 0], tab.at[a, i, 1], tab_send.at[a, i, 1], tab_recv.at[a, i, 1], partner)

    def row_copy(g, d, l):
        return remote(own[g].at[other if l else core], lists[g].at[2 * (n - d) - 1 + l], send1.at[g, d - 1, l],
                      recv1.at[g, n - d - 1, l], peer_other(g, d) if l else peer(g, d))

    def row_relay(g, l):
        frm, to = (n - 1, 1) if l == 0 else (1, n - 1)
        return remote(lists[g].at[2 * frm - 1 + l], lists[g].at[3 + l], send1.at[g, 1, l], recv1.at[g, 1, l], peer(g, to))

    onward = [(d, l) for l, d in enumerate(near)]
    rest = [(d, l) for d in near for l in range(2) if (d, l) not in onward]
    for pairs in (onward, rest):
        for g in order:
            for d, l in pairs:
                go(row_copy(g, d, l))
    for g in order:
        go(row_swap[g])
    go(tab_swap)
    for d in far + near:
        for a in range(3):
            go(tab_copy(a, d))

    def stats(tiles, counted=None):
        shape = tiles[0].shape
        ln = iota(shape, 1)
        counted = counted or tiles
        ms = [jnp.broadcast_to(t[:, 0:1], shape) for t in tiles]
        ls = [jnp.broadcast_to(t[:, 2:3], shape) for t in tiles]
        mm = functools.reduce(jnp.maximum, ms)
        ll = functools.reduce(jnp.maximum, ls)
        fs = [jnp.exp(a - mm) for a in ms]
        zz = sum(f * t[:, 1:2] for f, t in zip(fs, counted))
        lzz = sum(jnp.exp(a - ll) * t[:, 3:4] for a, t in zip(ls, counted))
        return fs, jnp.where(ln == 0, mm, jnp.where(ln == 1, zz, jnp.where(ln == 2, ll, lzz)))

    for g in order:
        if far:
            for l in range(2):
                row_copy(g, near[l], l).wait_recv()
                go(row_relay(g, l))

    def tab_of(a, k, l):
        if k:
            return tab.at[a, k - 1, l]
        return tab_pair.at[a] if l else own_tab.at[a, 0]

    def list_of(g, k, l):
        if k == 0 and l == 0:
            return own[g].at[core]
        return lists[g].at[2 * k - 1 + l]

    for d in near + far:
        for a in range(3):
            tab_copy(a, d).wait_recv()
            go(tab_share(a, d))
    tab_swap.wait_recv()
    for d in near + far:
        for a in range(3):
            tab_share(a, d).wait_recv()
    smem_copies = [pltpu.make_async_copy(tab_of(axis_of[g], k, l).at[pl.ds(inner, 2)], tab_smem.at[g, k, l],
                                         smem_sem.at[g, k, l])
                   for g in range(3) for k in range(n) for l in range(2)]
    for c in smem_copies:
        c.start()
    for c in smem_copies:
        c.wait()

    src = [(k, l) for k in range(n) for l in range(2)]

    def partial_hist(g, d2):
        nr = GROUPS[g][1]
        a = axis_of[g]
        c2, c3 = coord[(g + 1) % 3], coord[(g + 2) % 3]
        s2, s3 = row_stride[g]
        base = wrap(c2 + d2) * s2
        ln = iota((nr, LN), 1)

        def pair_step(q, carry):
            d3 = lax.div(q, 2)
            c = q - 2 * d3
            row = base + wrap(c3 + d3) * s3 + c
            acc = [jnp.zeros((nr, LN), F32)] * 2
            for i, (k, l) in enumerate(src):
                packed = jnp.broadcast_to(tab_of(a, k, l)[pl.ds(row, 1), :], (nr, LN))
                for hf in range(2):
                    u = tab_smem[g, k, l, hf, ((n - k) % n) * inner + row]
                    kt = lax.shift_right_logical(u, 7)
                    merged = jnp.where(ln >= (u & 127), scaled[g][i, kt], scaled[g][i, kt + 1])
                    code = lax.shift_right_logical(packed, 8) if hf else packed
                    got = jnp.take_along_axis(merged, code & 127, axis=1, mode='promise_in_bounds')
                    acc[hf] = acc[hf] + jnp.where((code & LN) != 0, got, 0.0)
            t = 2 * q + 2 * lax.div(q, n)
            part2[g][d2, t] = acc[0]
            part2[g][d2, t + 1] = acc[1]
            return carry

        lax.fori_loop(0, mid, pair_step, 0, unroll=UNROLL)

    halves = (pl.ds(0, mid + 1), pl.ds(mid + 1, mid + 1))
    stat_at = (mid, 0)

    def copy2(g, i, h):
        return remote(part2[g].at[near[i], halves[h]], recv2[g].at[i, h], send2.at[g, i, h], recv2_sem.at[g, i, h],
                      peer((g + 1) % 3, near[i]))

    def copy2_relay(g, i):
        return remote(part2[g].at[2, halves[i]], relay[g].at[i], send_relay.at[g, i], recv_relay.at[g, i],
                      peer((g + 1) % 3, near[i]))

    def copy3(g, d, l):
        return remote(part3[g].at[d, other if l else core], recv3[g].at[n - d - 1, l], send3.at[g, d, l],
                      recv3_sem.at[g, n - d - 1, l], peer((g + 2) % 3, d) + l * (partner - device))

    group_stat = {}
    for g in order:
        row_swap[g].wait_recv()
        for d, l in rest if far else onward + rest:
            row_copy(g, d, l).wait_recv()
        if far:
            for l in range(2):
                row_relay(g, l).wait_recv()
        fs, group_stat[g] = stats([list_of(g, k, l)[8] for k, l in src])
        for i, (k, l) in enumerate(src):
            rows = list_of(g, k, l)
            for t in range(8):
                scaled[g][i, t] = rows[t] * fs[i]
        for d2 in far + near + (0,):
            for h in range(2):
                part2[g][d2, mid + h] = group_stat[g]
        for d2 in far:
            partial_hist(g, d2)
            for i in range(2):
                go(copy2_relay(g, i))
    for g in order:
        for i, d2 in enumerate(near):
            partial_hist(g, d2)
            go(copy2(g, i, 1 - i))
        for i, d2 in enumerate(near):
            if far:
                copy2_relay(g, i).wait_recv()
                there = relay[g][i, stat_at[i]]
                zero = jnp.zeros(there.shape, F32)
                fs, tile = stats([group_stat[g], there], [group_stat[g], zero if i else there])
                for t in range(mid + 1):
                    r = t + i * (mid + 1)
                    part2[g][d2, r] = tile if t == stat_at[i] else part2[g][d2, r] * fs[0] + relay[g][i, t] * fs[1]
            go(copy2(g, i, i))
    for g in order:
        partial_hist(g, 0)

    for g in order:
        for i in range(len(near)):
            for h in range(2):
                copy2(g, i, h).wait_recv()
        keys2 = [(i, (i + j) % 2) for j in range(2) for i in range(len(near))]
        there = [recv2[g][i, h, stat_at[h]] for i, h in keys2]
        zero = jnp.zeros(there[0].shape, F32)
        fs, tile = stats([group_stat[g]] + there, [group_stat[g]] + there[:len(near)] + [zero] * len(near))
        factor = dict(zip(keys2, fs[1:]))
        for d3 in far + near + (0,):
            for ch in range(4):
                q = d3 * 4 + ch
                h = q // mid
                part3[g][d3, ch // 2, ch % 2] = part2[g][0, q + 2 * h] * fs[0] + sum(
                    recv2[g][i, h, q % mid + h] * factor[i, h] for i in range(len(near)))
            for c in range(2):
                part3[g][d3, c, 2] = tile
            for l in range(2):
                if d3 or l:
                    go(copy3(g, d3, l))

    lam_copy.wait()
    for l in range(2):
        for g in order:
            r0, nr = GROUPS[g]
            for d in range(l == 0, n):
                copy3(g, d, l).wait_recv()
            parts = [recv3[g].at[k, l] for k in range(n - 1)] + [recv3[g].at[n - 1, 1] if l else part3[g].at[0, core]]
            fs, tile = stats([p[2] for p in parts])
            rows = pl.ds(pl.multiple_of((other if l else core) * HALF + r0, 8), nr)
            for hf in range(2):
                hist_out[hf, rows] = sum(p[hf] * f for p, f in zip(parts, fs))
            stat_out[rows] = jnp.where(iota((nr, LN), 1) == 4, lam_ref[0], tile)
    for c in sends:
        c.wait_send()


def mixture_kernel(hist, stat, logits, out_ref):
    zz, ll, lzz, lam = (stat[:, i:i + 1] for i in range(1, 5))
    for hf in range(2):
        cols = slice(hf * LN, (hf + 1) * LN)
        lm_exp = jnp.exp(logits[:, cols] - ll)
        out_ref[:, cols] = jnp.log(lam * (hist[hf] / zz) + (1.0 - lam) * (lm_exp / lzz))


def step(n, hidden, w_local, keys_local, tok_local, bounds_local, tau, lam):
    tab_rows = 2 * n * n + 8
    block = 4 * n
    dim = hidden.shape[1]
    V, DMA = pltpu.VMEM, pltpu.SemaphoreType.DMA
    vm = pl.BlockSpec(memory_space=pltpu.VMEM)
    hbm = pl.BlockSpec(memory_space=pl.ANY)
    *rows, logits, tab = pl.pallas_call(
        functools.partial(local_kernel, n),
        out_shape=tuple(pltpu.VMEM((2, 9, nr, LN), F32) for _, nr in GROUPS) + (
            pltpu.VMEM((64, 256), F32),
            pltpu.VMEM((3, n, tab_rows, LN), I32)),
        in_specs=[hbm] * 6,
        out_specs=(vm,) * 5,
        scratch_shapes=[
            V((8, LN), I32), V(bounds_local.shape, I32), pltpu.SMEM((1,), F32), V((64, dim), BF16), V((dim, 256), BF16), V((EN, dim), BF16), V((8, 64, LN), F32),
            V((EN, EN), BF16), V((LN, EN), BF16), V((160, EN), BF16), V((192, EN), BF16),
            DMA((5,)), DMA((8,))],
        name='local_scores',
    )(tok_local.reshape(8, LN), bounds_local, tau.reshape(1), hidden, w_local, keys_local)

    def per_group(*lead):
        return [V((*lead, nr, LN), F32) for _, nr in GROUPS]

    def in_vmem(*arrays):
        return [pltpu.with_memory_space_constraint(x, pltpu.VMEM) for x in arrays]

    m = n - 1
    hist, stat = pl.pallas_call(
        functools.partial(exchange_kernel, n),
        out_shape=(V((2, 64, LN), F32), V((64, LN), F32)),
        in_specs=[vm] * 4 + [hbm],
        out_specs=(vm, vm),
        scratch_shapes=[
            pltpu.SMEM((1,), F32), DMA(()), V((3, tab_rows, LN), I32), V((3, m, 2, tab_rows, LN), I32),
            pltpu.SMEM((3, n, 2, 2, LN), I32),
            *per_group(2 * n - 1, 9), *per_group(2 * n, 9), *per_group(n, block + 2), *per_group(2, block // 2 + 1),
            *per_group(2, 2, block // 2 + 1), *per_group(n, 2, 3), *per_group(n, 2, 3),
            DMA((2, 4)), DMA((3, m, 2)), DMA((3, m, 2)), DMA((3, n, 2)),
            DMA((3, m, 2)), DMA((3, m, 2)), DMA((3, 2, 2)), DMA((3, 2, 2)), DMA((3, 2)), DMA((3, 2)),
            DMA((3, n, 2)), DMA((3, n, 2))],
        compiler_params=pltpu.CompilerParams(collective_id=0, has_side_effects=True),
        name='exchange',
    )(*in_vmem(*rows, tab), lam.reshape(1))
    return pl.pallas_call(
        mixture_kernel, out_shape=jax.ShapeDtypeStruct((64, 256), F32), in_specs=[vm] * 3, out_specs=vm, name='mixture',
    )(*in_vmem(hist, stat, logits))


def solution(mesh):
    n = round((mesh.shape['model'] // 2) ** (1 / 3))
    return jax.shard_map(functools.partial(step, n), mesh=mesh,
                         in_specs=(P('data', None), P(None, 'model'), P('model', None), P('model'),
                                   P('model', None), P(), P()),
                         out_specs=P('data', 'model'), check_vma=False)
```

```python
import functools

import jax
import jax.numpy as jnp
from jax import lax
from jax.experimental import pallas as pl
from jax.experimental.pallas import tpu as pltpu
from jax.sharding import PartitionSpec as P

F32, BF16, I32 = jnp.float32, jnp.bfloat16, jnp.int32
GROUPS = ((0, 16), (16, 8), (24, 8))
UNROLL = 4
AHEAD = 4
HALF = 32
LN, EN = 128, 1024
NT = (((1,), (1,)), ((), ()))


def iota(shape, axis):
    return lax.broadcasted_iota(I32, shape, axis)


def coordinates(n):
    device = lax.axis_index('model')
    return device, device % 2, (device // 2) % n, (device // (2 * n)) % n, device // (2 * n * n)


def local_kernel(n, tok_hbm, bounds_hbm, tau_hbm, hid_hbm, w_hbm, keys_hbm, score, dedup, logits_out, tab_out,
                 tok_ref, bounds_ref, tau_ref, hid, w, keys, onehot, lohot, in_sem, key_sem):
    inner = 2 * n * n
    _, _, cx, cy, cz = coordinates(n)
    operands = ((tok_hbm, tok_ref), (bounds_hbm, bounds_ref), (tau_hbm, tau_ref), (hid_hbm, hid), (w_hbm, w))
    in_copies = [pltpu.make_async_copy(a, b, in_sem.at[i]) for i, (a, b) in enumerate(operands)]
    for c in in_copies[:-1]:
        c.start()
    kchunk = LN
    nk = keys.shape[0] // kchunk

    def key_copy(c):
        rows = pl.ds(c * kchunk, kchunk)
        return pltpu.make_async_copy(keys_hbm.at[rows], keys.at[rows], key_sem.at[c])

    for c in range(AHEAD):
        key_copy(c).start()

    lane = iota((8, LN), 1)
    sub = iota((8, LN), 0)
    pos = sub * LN + lane

    def prev(a):
        r = pltpu.roll(a, 1, 1)
        return jnp.where(lane == 0, pltpu.roll(r, 1, 0), r)

    in_copies[0].wait()
    tok = tok_ref[...]
    first = ((tok != prev(tok)) | (pos == 0)).astype(I32)
    c = first
    for sh in (1, 2, 4, 8, 16, 32, 64):
        c = c + jnp.where(lane >= sh, pltpu.roll(c, sh, 1), 0)
    tot = jnp.broadcast_to(c[:, 127:LN], (8, LN))
    acc = tot
    for sh in (1, 2, 4):
        acc = acc + jnp.where(sub >= sh, pltpu.roll(acc, sh, 0), 0)
    rank = c + acc - tot - 1

    owner = tok // 256
    in_copies[1].wait()
    bnd = bounds_ref[...]
    nb = bnd.shape[1] - 1
    lo_b = jnp.broadcast_to(bnd[:, :nb], (8, nb))
    hi_b = jnp.broadcast_to(bnd[:, 1:], (8, nb))
    if nb < LN:
        lo_b = jnp.concatenate([lo_b, jnp.zeros((8, LN - nb), I32)], axis=1)
        hi_b = jnp.concatenate([hi_b, jnp.zeros((8, LN - nb), I32)], axis=1)
    counted = (pos >= jnp.take_along_axis(lo_b, owner, axis=1)) & (pos < jnp.take_along_axis(hi_b, owner, axis=1))
    rank_d = jnp.where(counted, rank, -1)
    small = iota((LN, LN), 0).astype(F32).astype(BF16)
    one, none = jnp.ones((LN, LN), BF16), jnp.zeros((LN, LN), BF16)

    def hot(row, value=one):
        return jnp.where(jnp.broadcast_to(row.astype(F32).astype(BF16), (LN, LN)) == small, value, none)

    for t in range(8):
        for r in range(8):
            dedup[r * LN:(r + 1) * LN, t * LN:(t + 1) * LN] = hot(rank_d[t:t + 1, :] - r * LN)

    h = tok // LN
    tile_first = ((h != prev(h)) | (pos == 0)).astype(I32)
    half = h % 2
    jc = owner % 2
    jp = ((owner // 2) % n, (owner // (2 * n)) % n, owner // (2 * n * n))
    lo = tok % LN
    val = (first * (rank % LN + LN) * (1 + 255 * half)).astype(F32)
    starts = [(tile_first * jnp.where(half == hf, part, 0)).astype(F32)
              for hf in range(2) for part in (rank // LN, rank % LN)]
    sub32 = iota((32, LN), 0)
    for t in range(8):
        cols = slice(t * LN, (t + 1) * LN)
        r = slice(t, t + 1)
        lohot[0:LN, cols] = hot(lo[r, :], jnp.broadcast_to(val[r, :].astype(BF16), (LN, LN)))
        lohot[LN:160, cols] = jnp.where(
            sub32 < 8, starts[0][r, :], jnp.where(sub32 < 16, starts[1][r, :], jnp.where(
                sub32 < 24, starts[2][r, :], starts[3][r, :]))).astype(BF16)
    coord = (cx, cy, cz)
    for a, (b2, b3) in enumerate(((2, 1), (2, 0), (1, 0))):
        row = ((jp[a] - coord[a] + n) % n) * inner + jp[b2] * (2 * n) + jp[b3] * 2 + jc
        for t in range(8):
            onehot[:, t * LN:(t + 1) * LN] = hot(row[t:t + 1, :])
        tb = lax.dot_general(onehot[...], lohot[0:LN, :], NT, preferred_element_type=F32).astype(I32)
        us = lax.dot_general(lohot[LN:160, :], onehot[...], NT, preferred_element_type=F32).astype(I32)
        for d in range(n):
            tab_out[a, d, 0:inner, :] = tb[d * inner:(d + 1) * inner, :]
            for hf in range(2):
                tab_out[a, d, inner + hf:inner + hf + 1, :] = us[16 * hf:16 * hf + 1] * LN + us[16 * hf + 8:16 * hf + 9]

    in_copies[-1].start()
    for c in in_copies[2:-1]:
        c.wait()
    tau = tau_ref[0]

    def score_step(c, carry):
        for i in range(2):
            key_copy(2 * c + i).wait()

            @pl.when(2 * c + i + AHEAD < nk)
            def _():
                key_copy(2 * c + i + AHEAD).start()

        rows = pl.ds(c * 256, 256)
        cross = lax.dot_general(hid[...], keys[rows, :], NT, preferred_element_type=F32)
        sq = jnp.zeros((256, LN), F32)
        for t in range(keys.shape[1] // LN):
            k = keys[rows, t * LN:(t + 1) * LN].astype(F32)
            sq = sq + k * k
        norm = jnp.sum(sq.T, axis=0, keepdims=True)
        sc = (2.0 * cross - norm) / tau
        score[2 * c] = sc[:, :LN]
        score[2 * c + 1] = sc[:, LN:]
        return carry

    lax.fori_loop(0, nk // 2, score_step, 0)

    in_copies[-1].wait()
    lg = jnp.dot(hid[...], w[...], preferred_element_type=F32)
    logits_out[...] = lg


def exchange_kernel(n, score, dedup, logits, own_tab, lam_hbm, hist_out, stat_out, e3, own0, own1, own2,
                    lam_ref, lam_sem, tab_pair, tab, tab_smem, list0, list1, list2, scaled0, scaled1, scaled2,
                    part20, part21, part22, relay0, relay1, relay2, recv20, recv21, recv22,
                    part30, part31, part32, recv30, recv31, recv32,
                    swap_sem, tab_send, tab_recv, smem_sem,
                    send1, recv1, send2, recv2_sem, send_relay, recv_relay, send3, recv3_sem):
    inner = 2 * n * n
    mid = 2 * n
    block = 2 * mid
    device, core, cx, cy, cz = coordinates(n)
    other = 1 - core
    partner = device + 1 - 2 * core
    pcoord, pstride = (cx, cy, cz), (2, 2 * n, 2 * n * n)

    def axes_of(c):
        return ((cx + c * (cy - cx), cy + c * (cx - cy), cz), (2 + c * (2 * n - 2), 2 * n + c * (2 - 2 * n), 2 * n * n))

    coord, stride = axes_of(core)
    coord_o, stride_o = axes_of(other)
    axis_of = (core, other, 2)
    row_stride = ((2, 2 * n), (2 * n, 2), (stride[0], stride[1]))
    own, lists, scaled = (own0, own1, own2), (list0, list1, list2), (scaled0, scaled1, scaled2)
    part2, relay, recv2 = (part20, part21, part22), (relay0, relay1, relay2), (recv20, recv21, recv22)
    part3, recv3 = (part30, part31, part32), (recv30, recv31, recv32)

    def wrap(a):
        return lax.rem(a, n)

    def peer(v, d):
        return device + stride[v] * (wrap(coord[v] + d) - coord[v])

    def peer_other(v, d):
        return partner + stride_o[v] * (wrap(coord_o[v] + d) - coord_o[v])

    def axis_peer(start, a, d):
        return start + pstride[a] * (wrap(pcoord[a] + d) - pcoord[a])

    def remote(src, dst, ssem, rsem, dev):
        return pltpu.make_async_remote_copy(src_ref=src, dst_ref=dst, send_sem=ssem, recv_sem=rsem,
                                            device_id={'model': dev}, device_id_type=pl.DeviceIdType.MESH)

    near = (1, n - 1) if n > 2 else (1,)
    far = tuple(range(2, n - 1))
    order = (1, 2, 0)
    sends = []

    def go(c):
        c.start()
        sends.append(c)

    lam_copy = pltpu.make_async_copy(lam_hbm, lam_ref, lam_sem)
    lam_copy.start()
    barrier = pltpu.get_barrier_semaphore()
    partners = [partner] + [axis_peer(start, a, d) for start in (device, partner) for a in range(3) for d in range(1, n)]
    for p in partners:
        pl.semaphore_signal(barrier, inc=1, device_id={'model': p}, device_id_type=pl.DeviceIdType.MESH)
    for g in range(3):
        for i in range(2 * n):
            scaled[g][i, 8] = jnp.zeros(scaled[g].shape[2:], F32)
    lg = logits[...]
    lm = jnp.max(lg, axis=1, keepdims=True)
    lz = jnp.sum(jnp.exp(lg - lm), axis=1, keepdims=True)
    sc = [score[t] for t in range(8)]
    m = jnp.max(functools.reduce(jnp.maximum, sc), axis=1, keepdims=True)
    z = jnp.zeros((64, LN), F32)
    for t in range(8):
        e = jnp.exp(sc[t] - m)
        z = z + e
        hi = e.astype(BF16)
        r1 = e - hi.astype(F32)
        middle = r1.astype(BF16)
        low = (r1 - middle.astype(F32)).astype(BF16)
        cols = slice(t * LN, (t + 1) * LN)
        e3[0:64, cols] = hi
        e3[64:LN, cols] = middle
        e3[LN:192, cols] = low
    z = jnp.sum(z, axis=1, keepdims=True)
    l64 = iota((64, LN), 1)
    stat = jnp.where(l64 == 0, m, jnp.where(l64 == 1, z, jnp.where(l64 == 2, lm, lz)))
    for h in range(2):
        for out, (r0, nr) in zip(own, GROUPS):
            out[h, 8] = stat[h * HALF + r0:h * HALF + r0 + nr]
    for c in range(4):
        dd = lax.dot_general(e3[...], dedup[c * 256:(c + 1) * 256, :], NT, preferred_element_type=F32)
        eu = dd[0:64] + (dd[64:LN] + dd[LN:192])
        for h in range(2):
            for out, (r0, nr) in zip(own, GROUPS):
                for t in range(2):
                    out[h, 2 * c + t] = eu[h * HALF + r0:h * HALF + r0 + nr, t * LN:(t + 1) * LN]
    pl.semaphore_wait(barrier, len(partners))

    tab_swap = remote(own_tab.at[:, 0], tab_pair, swap_sem.at[0, 0], swap_sem.at[1, 0], partner)
    row_swap = [remote(own[g].at[other], lists[g].at[0], swap_sem.at[0, 1 + g], swap_sem.at[1, 1 + g], partner)
                for g in range(3)]

    def tab_copy(a, d):
        return remote(own_tab.at[a, d], tab.at[a, n - d - 1, 0], tab_send.at[a, d - 1, 0], tab_recv.at[a, n - d - 1, 0],
                      axis_peer(device, a, d))

    def tab_share(a, d):
        i = n - d - 1
        return remote(tab.at[a, i, 0], tab.at[a, i, 1], tab_send.at[a, i, 1], tab_recv.at[a, i, 1], partner)

    def row_copy(g, d, l):
        return remote(own[g].at[other if l else core], lists[g].at[2 * (n - d) - 1 + l], send1.at[g, d - 1, l],
                      recv1.at[g, n - d - 1, l], peer_other(g, d) if l else peer(g, d))

    def row_relay(g, l):
        frm, to = (n - 1, 1) if l == 0 else (1, n - 1)
        return remote(lists[g].at[2 * frm - 1 + l], lists[g].at[3 + l], send1.at[g, 1, l], recv1.at[g, 1, l], peer(g, to))

    onward = [(d, l) for l, d in enumerate(near)]
    rest = [(d, l) for d in near for l in range(2) if (d, l) not in onward]
    for pairs in (onward, rest):
        for g in order:
            for d, l in pairs:
                go(row_copy(g, d, l))
    for g in order:
        go(row_swap[g])
    go(tab_swap)
    for d in far + near:
        for a in range(3):
            go(tab_copy(a, d))

    def stats(tiles, counted=None):
        shape = tiles[0].shape
        ln = iota(shape, 1)
        counted = counted or tiles
        ms = [jnp.broadcast_to(t[:, 0:1], shape) for t in tiles]
        ls = [jnp.broadcast_to(t[:, 2:3], shape) for t in tiles]
        mm = functools.reduce(jnp.maximum, ms)
        ll = functools.reduce(jnp.maximum, ls)
        fs = [jnp.exp(a - mm) for a in ms]
        zz = sum(f * t[:, 1:2] for f, t in zip(fs, counted))
        lzz = sum(jnp.exp(a - ll) * t[:, 3:4] for a, t in zip(ls, counted))
        return fs, jnp.where(ln == 0, mm, jnp.where(ln == 1, zz, jnp.where(ln == 2, ll, lzz)))

    for g in order:
        if far:
            for l in range(2):
                row_copy(g, near[l], l).wait_recv()
                go(row_relay(g, l))

    def tab_of(a, k, l):
        if k:
            return tab.at[a, k - 1, l]
        return tab_pair.at[a] if l else own_tab.at[a, 0]

    def list_of(g, k, l):
        if k == 0 and l == 0:
            return own[g].at[core]
        return lists[g].at[2 * k - 1 + l]

    for d in near + far:
        for a in range(3):
            tab_copy(a, d).wait_recv()
            go(tab_share(a, d))
    tab_swap.wait_recv()
    for d in near + far:
        for a in range(3):
            tab_share(a, d).wait_recv()
    smem_copies = [pltpu.make_async_copy(tab_of(axis_of[g], k, l).at[pl.ds(inner, 2)], tab_smem.at[g, k, l],
                                         smem_sem.at[g, k, l])
                   for g in range(3) for k in range(n) for l in range(2)]
    for c in smem_copies:
        c.start()
    for c in smem_copies:
        c.wait()

    src = [(k, l) for k in range(n) for l in range(2)]

    def partial_hist(g, d2):
        nr = GROUPS[g][1]
        a = axis_of[g]
        c2, c3 = coord[(g + 1) % 3], coord[(g + 2) % 3]
        s2, s3 = row_stride[g]
        base = wrap(c2 + d2) * s2
        ln = iota((nr, LN), 1)

        def pair_step(q, carry):
            d3 = lax.div(q, 2)
            c = q - 2 * d3
            row = base + wrap(c3 + d3) * s3 + c
            acc = [jnp.zeros((nr, LN), F32)] * 2
            for i, (k, l) in enumerate(src):
                packed = jnp.broadcast_to(tab_of(a, k, l)[pl.ds(row, 1), :], (nr, LN))
                for hf in range(2):
                    u = tab_smem[g, k, l, hf, ((n - k) % n) * inner + row]
                    kt = lax.shift_right_logical(u, 7)
                    merged = jnp.where(ln >= (u & 127), scaled[g][i, kt], scaled[g][i, kt + 1])
                    code = lax.shift_right_logical(packed, 8) if hf else packed
                    got = jnp.take_along_axis(merged, code & 127, axis=1, mode='promise_in_bounds')
                    acc[hf] = acc[hf] + jnp.where((code & LN) != 0, got, 0.0)
            t = 2 * q + 2 * lax.div(q, n)
            part2[g][d2, t] = acc[0]
            part2[g][d2, t + 1] = acc[1]
            return carry

        lax.fori_loop(0, mid, pair_step, 0, unroll=UNROLL)

    halves = (pl.ds(0, mid + 1), pl.ds(mid + 1, mid + 1))
    stat_at = (mid, 0)

    def copy2(g, i, h):
        return remote(part2[g].at[near[i], halves[h]], recv2[g].at[i, h], send2.at[g, i, h], recv2_sem.at[g, i, h],
                      peer((g + 1) % 3, near[i]))

    def copy2_relay(g, i):
        return remote(part2[g].at[2, halves[i]], relay[g].at[i], send_relay.at[g, i], recv_relay.at[g, i],
                      peer((g + 1) % 3, near[i]))

    def copy3(g, d, l):
        return remote(part3[g].at[d, other if l else core], recv3[g].at[n - d - 1, l], send3.at[g, d, l],
                      recv3_sem.at[g, n - d - 1, l], peer((g + 2) % 3, d) + l * (partner - device))

    group_stat = {}
    for g in order:
        row_swap[g].wait_recv()
        for d, l in rest if far else onward + rest:
            row_copy(g, d, l).wait_recv()
        if far:
            for l in range(2):
                row_relay(g, l).wait_recv()
        fs, group_stat[g] = stats([list_of(g, k, l)[8] for k, l in src])
        for i, (k, l) in enumerate(src):
            rows = list_of(g, k, l)
            for t in range(8):
                scaled[g][i, t] = rows[t] * fs[i]
        for d2 in far + near + (0,):
            for h in range(2):
                part2[g][d2, mid + h] = group_stat[g]
        for d2 in far:
            partial_hist(g, d2)
            for i in range(2):
                go(copy2_relay(g, i))
    for g in order:
        for i, d2 in enumerate(near):
            partial_hist(g, d2)
            go(copy2(g, i, 1 - i))
        for i, d2 in enumerate(near):
            if far:
                copy2_relay(g, i).wait_recv()
                there = relay[g][i, stat_at[i]]
                zero = jnp.zeros(there.shape, F32)
                fs, tile = stats([group_stat[g], there], [group_stat[g], zero if i else there])
                for t in range(mid + 1):
                    r = t + i * (mid + 1)
                    part2[g][d2, r] = tile if t == stat_at[i] else part2[g][d2, r] * fs[0] + relay[g][i, t] * fs[1]
            go(copy2(g, i, i))
    for g in order:
        partial_hist(g, 0)

    for g in order:
        for i in range(len(near)):
            for h in range(2):
                copy2(g, i, h).wait_recv()
        keys2 = [(i, (i + j) % 2) for j in range(2) for i in range(len(near))]
        there = [recv2[g][i, h, stat_at[h]] for i, h in keys2]
        zero = jnp.zeros(there[0].shape, F32)
        fs, tile = stats([group_stat[g]] + there, [group_stat[g]] + there[:len(near)] + [zero] * len(near))
        factor = dict(zip(keys2, fs[1:]))
        for d3 in far + near + (0,):
            for ch in range(4):
                q = d3 * 4 + ch
                h = q // mid
                part3[g][d3, ch // 2, ch % 2] = part2[g][0, q + 2 * h] * fs[0] + sum(
                    recv2[g][i, h, q % mid + h] * factor[i, h] for i in range(len(near)))
            for c in range(2):
                part3[g][d3, c, 2] = tile
            for l in range(2):
                if d3 or l:
                    go(copy3(g, d3, l))

    lam_copy.wait()
    for l in range(2):
        for g in order:
            r0, nr = GROUPS[g]
            for d in range(l == 0, n):
                copy3(g, d, l).wait_recv()
            parts = [recv3[g].at[k, l] for k in range(n - 1)] + [recv3[g].at[n - 1, 1] if l else part3[g].at[0, core]]
            fs, tile = stats([p[2] for p in parts])
            rows = pl.ds(pl.multiple_of((other if l else core) * HALF + r0, 8), nr)
            for hf in range(2):
                hist_out[hf, rows] = sum(p[hf] * f for p, f in zip(parts, fs))
            stat_out[rows] = jnp.where(iota((nr, LN), 1) == 4, lam_ref[0], tile)
    for c in sends:
        c.wait_send()


def mixture_kernel(hist, stat, logits, out_ref):
    zz, ll, lzz, lam = (stat[:, i:i + 1] for i in range(1, 5))
    for hf in range(2):
        cols = slice(hf * LN, (hf + 1) * LN)
        lm_exp = jnp.exp(logits[:, cols] - ll)
        out_ref[:, cols] = jnp.log(lam * (hist[hf] / zz) + (1.0 - lam) * (lm_exp / lzz))


def step(n, hidden, w_local, keys_local, tok_local, bounds_local, tau, lam):
    tab_rows = 2 * n * n + 8
    block = 4 * n
    dim = hidden.shape[1]
    V, DMA = pltpu.VMEM, pltpu.SemaphoreType.DMA
    vm = pl.BlockSpec(memory_space=pltpu.VMEM)
    hbm = pl.BlockSpec(memory_space=pl.ANY)
    score, dedup, logits, tab = pl.pallas_call(
        functools.partial(local_kernel, n),
        out_shape=(V((8, 64, LN), F32), V((EN, EN), BF16), V((64, 256), F32),
                   V((3, n, tab_rows, LN), I32)),
        in_specs=[hbm] * 6,
        out_specs=(vm,) * 4,
        scratch_shapes=[
            V((8, LN), I32), V(bounds_local.shape, I32), pltpu.SMEM((1,), F32), V((64, dim), BF16), V((dim, 256), BF16), V((EN, dim), BF16),
            V((LN, EN), BF16), V((160, EN), BF16),
            DMA((5,)), DMA((8,))],
        name='local_scores',
    )(tok_local.reshape(8, LN), bounds_local, tau.reshape(1), hidden, w_local, keys_local)

    def per_group(*lead):
        return [V((*lead, nr, LN), F32) for _, nr in GROUPS]

    def in_vmem(*arrays):
        return [pltpu.with_memory_space_constraint(x, pltpu.VMEM) for x in arrays]

    m = n - 1
    hist, stat = pl.pallas_call(
        functools.partial(exchange_kernel, n),
        out_shape=(V((2, 64, LN), F32), V((64, LN), F32)),
        in_specs=[vm] * 4 + [hbm],
        out_specs=(vm, vm),
        scratch_shapes=[
            V((192, EN), BF16), *per_group(2, 9), pltpu.SMEM((1,), F32), DMA(()), V((3, tab_rows, LN), I32), V((3, m, 2, tab_rows, LN), I32),
            pltpu.SMEM((3, n, 2, 2, LN), I32),
            *per_group(2 * n - 1, 9), *per_group(2 * n, 9), *per_group(n, block + 2), *per_group(2, block // 2 + 1),
            *per_group(2, 2, block // 2 + 1), *per_group(n, 2, 3), *per_group(n, 2, 3),
            DMA((2, 4)), DMA((3, m, 2)), DMA((3, m, 2)), DMA((3, n, 2)),
            DMA((3, m, 2)), DMA((3, m, 2)), DMA((3, 2, 2)), DMA((3, 2, 2)), DMA((3, 2)), DMA((3, 2)),
            DMA((3, n, 2)), DMA((3, n, 2))],
        compiler_params=pltpu.CompilerParams(collective_id=0, has_side_effects=True),
        name='exchange',
    )(*in_vmem(score, dedup, logits, tab), lam.reshape(1))
    return pl.pallas_call(
        mixture_kernel, out_shape=jax.ShapeDtypeStruct((64, 256), F32), in_specs=[vm] * 3, out_specs=vm, name='mixture',
    )(*in_vmem(hist, stat, logits))


def solution(mesh):
    n = round((mesh.shape['model'] // 2) ** (1 / 3))
    return jax.shard_map(functools.partial(step, n), mesh=mesh,
                         in_specs=(P('data', None), P(None, 'model'), P('model', None), P('model'),
                                   P('model', None), P(), P()),
                         out_specs=P('data', 'model'), check_vma=False)
```

```python
import functools

import jax
import jax.numpy as jnp
from jax import lax
from jax.experimental import pallas as pl
from jax.experimental.pallas import tpu as pltpu
from jax.sharding import PartitionSpec as P

F32, BF16, I32 = jnp.float32, jnp.bfloat16, jnp.int32
GROUPS = ((0, 16), (16, 8), (24, 8))
UNROLL = 4
AHEAD = 4
HALF = 32
LN, EN = 128, 1024
NT = (((1,), (1,)), ((), ()))


def iota(shape, axis):
    return lax.broadcasted_iota(I32, shape, axis)


def coordinates(n):
    device = lax.axis_index('model')
    return device, device % 2, (device // 2) % n, (device // (2 * n)) % n, device // (2 * n * n)


def local_kernel(n, tok_hbm, bounds_hbm, tau_hbm, hid_hbm, w_hbm, keys_hbm, score, dedup, logits_out, tab_out,
                 tok_ref, bounds_ref, tau_ref, hid, w, keys, onehot, lohot, in_sem, key_sem):
    inner = 2 * n * n
    _, _, cx, cy, cz = coordinates(n)
    operands = ((tok_hbm, tok_ref), (bounds_hbm, bounds_ref), (tau_hbm, tau_ref), (hid_hbm, hid), (w_hbm, w))
    in_copies = [pltpu.make_async_copy(a, b, in_sem.at[i]) for i, (a, b) in enumerate(operands)]
    for c in in_copies[:-1]:
        c.start()
    kchunk = LN
    nk = keys.shape[0] // kchunk

    def key_copy(c):
        rows = pl.ds(c * kchunk, kchunk)
        return pltpu.make_async_copy(keys_hbm.at[rows], keys.at[rows], key_sem.at[c])

    for c in range(AHEAD):
        key_copy(c).start()

    lane = iota((8, LN), 1)
    sub = iota((8, LN), 0)
    pos = sub * LN + lane

    def prev(a):
        r = pltpu.roll(a, 1, 1)
        return jnp.where(lane == 0, pltpu.roll(r, 1, 0), r)

    in_copies[0].wait()
    tok = tok_ref[...]
    first = ((tok != prev(tok)) | (pos == 0)).astype(I32)
    c = first
    for sh in (1, 2, 4, 8, 16, 32, 64):
        c = c + jnp.where(lane >= sh, pltpu.roll(c, sh, 1), 0)
    tot = jnp.broadcast_to(c[:, 127:LN], (8, LN))
    acc = tot
    for sh in (1, 2, 4):
        acc = acc + jnp.where(sub >= sh, pltpu.roll(acc, sh, 0), 0)
    rank = c + acc - tot - 1

    owner = tok // 256
    in_copies[1].wait()
    bnd = bounds_ref[...]
    nb = bnd.shape[1] - 1
    lo_b = jnp.broadcast_to(bnd[:, :nb], (8, nb))
    hi_b = jnp.broadcast_to(bnd[:, 1:], (8, nb))
    if nb < LN:
        lo_b = jnp.concatenate([lo_b, jnp.zeros((8, LN - nb), I32)], axis=1)
        hi_b = jnp.concatenate([hi_b, jnp.zeros((8, LN - nb), I32)], axis=1)
    counted = (pos >= jnp.take_along_axis(lo_b, owner, axis=1)) & (pos < jnp.take_along_axis(hi_b, owner, axis=1))
    rank_d = jnp.where(counted, rank, -1)
    small = iota((LN, LN), 0).astype(F32).astype(BF16)
    one, none = jnp.ones((LN, LN), BF16), jnp.zeros((LN, LN), BF16)

    def hot(row, value=one):
        return jnp.where(jnp.broadcast_to(row.astype(F32).astype(BF16), (LN, LN)) == small, value, none)

    for t in range(8):
        for r in range(8):
            dedup[r * LN:(r + 1) * LN, t * LN:(t + 1) * LN] = hot(rank_d[t:t + 1, :] - r * LN)

    h = tok // LN
    tile_first = ((h != prev(h)) | (pos == 0)).astype(I32)
    half = h % 2
    jc = owner % 2
    jp = ((owner // 2) % n, (owner // (2 * n)) % n, owner // (2 * n * n))
    lo = tok % LN
    val = (first * (rank % LN + LN) * (1 + 255 * half)).astype(F32)
    starts = [(tile_first * jnp.where(half == hf, part, 0)).astype(F32)
              for hf in range(2) for part in (rank // LN, rank % LN)]
    sub32 = iota((32, LN), 0)
    for t in range(8):
        cols = slice(t * LN, (t + 1) * LN)
        r = slice(t, t + 1)
        lohot[0:LN, cols] = hot(lo[r, :], jnp.broadcast_to(val[r, :].astype(BF16), (LN, LN)))
        lohot[LN:160, cols] = jnp.where(
            sub32 < 8, starts[0][r, :], jnp.where(sub32 < 16, starts[1][r, :], jnp.where(
                sub32 < 24, starts[2][r, :], starts[3][r, :]))).astype(BF16)
    coord = (cx, cy, cz)
    for a, (b2, b3) in enumerate(((2, 1), (2, 0), (1, 0))):
        row = ((jp[a] - coord[a] + n) % n) * inner + jp[b2] * (2 * n) + jp[b3] * 2 + jc
        for t in range(8):
            onehot[:, t * LN:(t + 1) * LN] = hot(row[t:t + 1, :])
        tb = lax.dot_general(onehot[...], lohot[0:LN, :], NT, preferred_element_type=F32).astype(I32)
        us = lax.dot_general(lohot[LN:160, :], onehot[...], NT, preferred_element_type=F32).astype(I32)
        for d in range(n):
            tab_out[a, d, 0:inner, :] = tb[d * inner:(d + 1) * inner, :]
            for hf in range(2):
                tab_out[a, d, inner + hf:inner + hf + 1, :] = us[16 * hf:16 * hf + 1] * LN + us[16 * hf + 8:16 * hf + 9]

    in_copies[-1].start()
    for c in in_copies[2:-1]:
        c.wait()
    tau = tau_ref[0]

    def score_step(c, carry):
        for i in range(2):
            key_copy(2 * c + i).wait()

            @pl.when(2 * c + i + AHEAD < nk)
            def _():
                key_copy(2 * c + i + AHEAD).start()

        rows = pl.ds(c * 256, 256)
        cross = lax.dot_general(keys[rows, :], hid[...], NT, preferred_element_type=F32)
        sq = jnp.zeros((256, LN), F32)
        for t in range(keys.shape[1] // LN):
            k = keys[rows, t * LN:(t + 1) * LN].astype(F32)
            sq = sq + k * k
        norm = jnp.sum(sq, axis=1, keepdims=True)
        sc = ((2.0 * cross - norm) / tau).T
        score[2 * c] = sc[:, :LN]
        score[2 * c + 1] = sc[:, LN:]
        return carry

    lax.fori_loop(0, nk // 2, score_step, 0)

    in_copies[-1].wait()
    lg = jnp.dot(hid[...], w[...], preferred_element_type=F32)
    logits_out[...] = lg


def exchange_kernel(n, score, dedup, logits, own_tab, lam_hbm, hist_out, stat_out, e3, own0, own1, own2,
                    lam_ref, lam_sem, tab_pair, tab, tab_smem, list0, list1, list2, scaled0, scaled1, scaled2,
                    part20, part21, part22, relay0, relay1, relay2, recv20, recv21, recv22,
                    part30, part31, part32, recv30, recv31, recv32,
                    swap_sem, tab_send, tab_recv, smem_sem,
                    send1, recv1, send2, recv2_sem, send_relay, recv_relay, send3, recv3_sem):
    inner = 2 * n * n
    mid = 2 * n
    block = 2 * mid
    device, core, cx, cy, cz = coordinates(n)
    other = 1 - core
    partner = device + 1 - 2 * core
    pcoord, pstride = (cx, cy, cz), (2, 2 * n, 2 * n * n)

    def axes_of(c):
        return ((cx + c * (cy - cx), cy + c * (cx - cy), cz), (2 + c * (2 * n - 2), 2 * n + c * (2 - 2 * n), 2 * n * n))

    coord, stride = axes_of(core)
    coord_o, stride_o = axes_of(other)
    axis_of = (core, other, 2)
    row_stride = ((2, 2 * n), (2 * n, 2), (stride[0], stride[1]))
    own, lists, scaled = (own0, own1, own2), (list0, list1, list2), (scaled0, scaled1, scaled2)
    part2, relay, recv2 = (part20, part21, part22), (relay0, relay1, relay2), (recv20, recv21, recv22)
    part3, recv3 = (part30, part31, part32), (recv30, recv31, recv32)

    def wrap(a):
        return lax.rem(a, n)

    def peer(v, d):
        return device + stride[v] * (wrap(coord[v] + d) - coord[v])

    def peer_other(v, d):
        return partner + stride_o[v] * (wrap(coord_o[v] + d) - coord_o[v])

    def axis_peer(start, a, d):
        return start + pstride[a] * (wrap(pcoord[a] + d) - pcoord[a])

    def remote(src, dst, ssem, rsem, dev):
        return pltpu.make_async_remote_copy(src_ref=src, dst_ref=dst, send_sem=ssem, recv_sem=rsem,
                                            device_id={'model': dev}, device_id_type=pl.DeviceIdType.MESH)

    near = (1, n - 1) if n > 2 else (1,)
    far = tuple(range(2, n - 1))
    order = (1, 2, 0)
    sends = []

    def go(c):
        c.start()
        sends.append(c)

    lam_copy = pltpu.make_async_copy(lam_hbm, lam_ref, lam_sem)
    lam_copy.start()
    barrier = pltpu.get_barrier_semaphore()
    partners = [partner] + [axis_peer(start, a, d) for start in (device, partner) for a in range(3) for d in range(1, n)]
    for p in partners:
        pl.semaphore_signal(barrier, inc=1, device_id={'model': p}, device_id_type=pl.DeviceIdType.MESH)
    for g in range(3):
        for i in range(2 * n):
            scaled[g][i, 8] = jnp.zeros(scaled[g].shape[2:], F32)
    lg = logits[...]
    lm = jnp.max(lg, axis=1, keepdims=True)
    lz = jnp.sum(jnp.exp(lg - lm), axis=1, keepdims=True)
    sc = [score[t] for t in range(8)]
    m = jnp.max(functools.reduce(jnp.maximum, sc), axis=1, keepdims=True)
    z = jnp.zeros((64, LN), F32)
    for t in range(8):
        e = jnp.exp(sc[t] - m)
        z = z + e
        hi = e.astype(BF16)
        r1 = e - hi.astype(F32)
        middle = r1.astype(BF16)
        low = (r1 - middle.astype(F32)).astype(BF16)
        cols = slice(t * LN, (t + 1) * LN)
        e3[0:64, cols] = hi
        e3[64:LN, cols] = middle
        e3[LN:192, cols] = low
    z = jnp.sum(z, axis=1, keepdims=True)
    l64 = iota((64, LN), 1)
    stat = jnp.where(l64 == 0, m, jnp.where(l64 == 1, z, jnp.where(l64 == 2, lm, lz)))
    for h in range(2):
        for out, (r0, nr) in zip(own, GROUPS):
            out[h, 8] = stat[h * HALF + r0:h * HALF + r0 + nr]
    for c in range(4):
        dd = lax.dot_general(e3[...], dedup[c * 256:(c + 1) * 256, :], NT, preferred_element_type=F32)
        eu = dd[0:64] + (dd[64:LN] + dd[LN:192])
        for h in range(2):
            for out, (r0, nr) in zip(own, GROUPS):
                for t in range(2):
                    out[h, 2 * c + t] = eu[h * HALF + r0:h * HALF + r0 + nr, t * LN:(t + 1) * LN]
    pl.semaphore_wait(barrier, len(partners))

    tab_swap = remote(own_tab.at[:, 0], tab_pair, swap_sem.at[0, 0], swap_sem.at[1, 0], partner)
    row_swap = [remote(own[g].at[other], lists[g].at[0], swap_sem.at[0, 1 + g], swap_sem.at[1, 1 + g], partner)
                for g in range(3)]

    def tab_copy(a, d):
        return remote(own_tab.at[a, d], tab.at[a, n - d - 1, 0], tab_send.at[a, d - 1, 0], tab_recv.at[a, n - d - 1, 0],
                      axis_peer(device, a, d))

    def tab_share(a, d):
        i = n - d - 1
        return remote(tab.at[a, i, 0], tab.at[a, i, 1], tab_send.at[a, i, 1], tab_recv.at[a, i, 1], partner)

    def row_copy(g, d, l):
        return remote(own[g].at[other if l else core], lists[g].at[2 * (n - d) - 1 + l], send1.at[g, d - 1, l],
                      recv1.at[g, n - d - 1, l], peer_other(g, d) if l else peer(g, d))

    def row_relay(g, l):
        frm, to = (n - 1, 1) if l == 0 else (1, n - 1)
        return remote(lists[g].at[2 * frm - 1 + l], lists[g].at[3 + l], send1.at[g, 1, l], recv1.at[g, 1, l], peer(g, to))

    onward = [(d, l) for l, d in enumerate(near)]
    rest = [(d, l) for d in near for l in range(2) if (d, l) not in onward]
    for pairs in (onward, rest):
        for g in order:
            for d, l in pairs:
                go(row_copy(g, d, l))
    for g in order:
        go(row_swap[g])
    go(tab_swap)
    for d in far + near:
        for a in range(3):
            go(tab_copy(a, d))

    def stats(tiles, counted=None):
        shape = tiles[0].shape
        ln = iota(shape, 1)
        counted = counted or tiles
        ms = [jnp.broadcast_to(t[:, 0:1], shape) for t in tiles]
        ls = [jnp.broadcast_to(t[:, 2:3], shape) for t in tiles]
        mm = functools.reduce(jnp.maximum, ms)
        ll = functools.reduce(jnp.maximum, ls)
        fs = [jnp.exp(a - mm) for a in ms]
        zz = sum(f * t[:, 1:2] for f, t in zip(fs, counted))
        lzz = sum(jnp.exp(a - ll) * t[:, 3:4] for a, t in zip(ls, counted))
        return fs, jnp.where(ln == 0, mm, jnp.where(ln == 1, zz, jnp.where(ln == 2, ll, lzz)))

    for g in order:
        if far:
            for l in range(2):
                row_copy(g, near[l], l).wait_recv()
                go(row_relay(g, l))

    def tab_of(a, k, l):
        if k:
            return tab.at[a, k - 1, l]
        return tab_pair.at[a] if l else own_tab.at[a, 0]

    def list_of(g, k, l):
        if k == 0 and l == 0:
            return own[g].at[core]
        return lists[g].at[2 * k - 1 + l]

    smem_copies = []

    def scalars(a, k, l):
        c = pltpu.make_async_copy(tab_of(a, k, l).at[pl.ds(inner, 2)], tab_smem.at[a, k, l], smem_sem.at[a, k, l])
        c.start()
        smem_copies.append(c)

    for a in range(3):
        scalars(a, 0, 0)
    for d in near + far:
        for a in range(3):
            tab_copy(a, d).wait_recv()
            go(tab_share(a, d))
            scalars(a, n - d, 0)
    tab_swap.wait_recv()
    for a in range(3):
        scalars(a, 0, 1)
    for d in near + far:
        for a in range(3):
            tab_share(a, d).wait_recv()
            scalars(a, n - d, 1)
    for c in smem_copies:
        c.wait()

    src = [(k, l) for k in range(n) for l in range(2)]

    def partial_hist(g, d2):
        nr = GROUPS[g][1]
        a = axis_of[g]
        c2, c3 = coord[(g + 1) % 3], coord[(g + 2) % 3]
        s2, s3 = row_stride[g]
        base = wrap(c2 + d2) * s2
        ln = iota((nr, LN), 1)

        def pair_step(q, carry):
            d3 = lax.div(q, 2)
            c = q - 2 * d3
            row = base + wrap(c3 + d3) * s3 + c
            acc = [jnp.zeros((nr, LN), F32)] * 2
            for i, (k, l) in enumerate(src):
                packed = jnp.broadcast_to(tab_of(a, k, l)[pl.ds(row, 1), :], (nr, LN))
                for hf in range(2):
                    u = tab_smem[a, k, l, hf, ((n - k) % n) * inner + row]
                    kt = lax.shift_right_logical(u, 7)
                    merged = jnp.where(ln >= (u & 127), scaled[g][i, kt], scaled[g][i, kt + 1])
                    code = lax.shift_right_logical(packed, 8) if hf else packed
                    got = jnp.take_along_axis(merged, code & 127, axis=1, mode='promise_in_bounds')
                    acc[hf] = acc[hf] + jnp.where((code & LN) != 0, got, 0.0)
            t = 2 * q + 2 * lax.div(q, n)
            part2[g][d2, t] = acc[0]
            part2[g][d2, t + 1] = acc[1]
            return carry

        lax.fori_loop(0, mid, pair_step, 0, unroll=UNROLL)

    halves = (pl.ds(0, mid + 1), pl.ds(mid + 1, mid + 1))
    stat_at = (mid, 0)

    def copy2(g, i, h):
        return remote(part2[g].at[near[i], halves[h]], recv2[g].at[i, h], send2.at[g, i, h], recv2_sem.at[g, i, h],
                      peer((g + 1) % 3, near[i]))

    def copy2_relay(g, i):
        return remote(part2[g].at[2, halves[i]], relay[g].at[i], send_relay.at[g, i], recv_relay.at[g, i],
                      peer((g + 1) % 3, near[i]))

    def copy3(g, d, l):
        return remote(part3[g].at[d, other if l else core], recv3[g].at[n - d - 1, l], send3.at[g, d, l],
                      recv3_sem.at[g, n - d - 1, l], peer((g + 2) % 3, d) + l * (partner - device))

    group_stat = {}
    for g in order:
        row_swap[g].wait_recv()
        for d, l in rest if far else onward + rest:
            row_copy(g, d, l).wait_recv()
        if far:
            for l in range(2):
                row_relay(g, l).wait_recv()
        fs, group_stat[g] = stats([list_of(g, k, l)[8] for k, l in src])
        for i, (k, l) in enumerate(src):
            rows = list_of(g, k, l)
            for t in range(8):
                scaled[g][i, t] = rows[t] * fs[i]
        for d2 in far + near + (0,):
            for h in range(2):
                part2[g][d2, mid + h] = group_stat[g]
        for d2 in far:
            partial_hist(g, d2)
            for i in range(2):
                go(copy2_relay(g, i))
    for g in order:
        for i, d2 in enumerate(near):
            partial_hist(g, d2)
            go(copy2(g, i, 1 - i))
        for i, d2 in enumerate(near):
            if far:
                copy2_relay(g, i).wait_recv()
                there = relay[g][i, stat_at[i]]
                zero = jnp.zeros(there.shape, F32)
                fs, tile = stats([group_stat[g], there], [group_stat[g], zero if i else there])
                for t in range(mid + 1):
                    r = t + i * (mid + 1)
                    part2[g][d2, r] = tile if t == stat_at[i] else part2[g][d2, r] * fs[0] + relay[g][i, t] * fs[1]
            go(copy2(g, i, i))
    for g in order:
        partial_hist(g, 0)

    for g in order:
        for i in range(len(near)):
            for h in range(2):
                copy2(g, i, h).wait_recv()
        keys2 = [(i, (i + j) % 2) for j in range(2) for i in range(len(near))]
        there = [recv2[g][i, h, stat_at[h]] for i, h in keys2]
        zero = jnp.zeros(there[0].shape, F32)
        fs, tile = stats([group_stat[g]] + there, [group_stat[g]] + there[:len(near)] + [zero] * len(near))
        factor = dict(zip(keys2, fs[1:]))
        for d3 in far + near + (0,):
            for ch in range(4):
                q = d3 * 4 + ch
                h = q // mid
                part3[g][d3, ch // 2, ch % 2] = part2[g][0, q + 2 * h] * fs[0] + sum(
                    recv2[g][i, h, q % mid + h] * factor[i, h] for i in range(len(near)))
            for c in range(2):
                part3[g][d3, c, 2] = tile
            for l in range(2):
                if d3 or l:
                    go(copy3(g, d3, l))

    lam_copy.wait()
    for l in range(2):
        for g in order:
            r0, nr = GROUPS[g]
            for d in range(l == 0, n):
                copy3(g, d, l).wait_recv()
            parts = [recv3[g].at[k, l] for k in range(n - 1)] + [recv3[g].at[n - 1, 1] if l else part3[g].at[0, core]]
            fs, tile = stats([p[2] for p in parts])
            rows = pl.ds(pl.multiple_of((other if l else core) * HALF + r0, 8), nr)
            for hf in range(2):
                hist_out[hf, rows] = sum(p[hf] * f for p, f in zip(parts, fs))
            stat_out[rows] = jnp.where(iota((nr, LN), 1) == 4, lam_ref[0], tile)
    for c in sends:
        c.wait_send()


def mixture_kernel(hist, stat, logits, out_ref):
    zz, ll, lzz, lam = (stat[:, i:i + 1] for i in range(1, 5))
    for hf in range(2):
        cols = slice(hf * LN, (hf + 1) * LN)
        lm_exp = jnp.exp(logits[:, cols] - ll)
        out_ref[:, cols] = jnp.log(lam * (hist[hf] / zz) + (1.0 - lam) * (lm_exp / lzz))


def step(n, hidden, w_local, keys_local, tok_local, bounds_local, tau, lam):
    tab_rows = 2 * n * n + 8
    block = 4 * n
    dim = hidden.shape[1]
    V, DMA = pltpu.VMEM, pltpu.SemaphoreType.DMA
    vm = pl.BlockSpec(memory_space=pltpu.VMEM)
    hbm = pl.BlockSpec(memory_space=pl.ANY)
    score, dedup, logits, tab = pl.pallas_call(
        functools.partial(local_kernel, n),
        out_shape=(V((8, 64, LN), F32), V((EN, EN), BF16), V((64, 256), F32),
                   V((3, n, tab_rows, LN), I32)),
        in_specs=[hbm] * 6,
        out_specs=(vm,) * 4,
        scratch_shapes=[
            V((8, LN), I32), V(bounds_local.shape, I32), pltpu.SMEM((1,), F32), V((64, dim), BF16), V((dim, 256), BF16), V((EN, dim), BF16),
            V((LN, EN), BF16), V((160, EN), BF16),
            DMA((5,)), DMA((8,))],
        name='local_scores',
    )(tok_local.reshape(8, LN), bounds_local, tau.reshape(1), hidden, w_local, keys_local)

    def per_group(*lead):
        return [V((*lead, nr, LN), F32) for _, nr in GROUPS]

    def in_vmem(*arrays):
        return [pltpu.with_memory_space_constraint(x, pltpu.VMEM) for x in arrays]

    m = n - 1
    hist, stat = pl.pallas_call(
        functools.partial(exchange_kernel, n),
        out_shape=(V((2, 64, LN), F32), V((64, LN), F32)),
        in_specs=[vm] * 4 + [hbm],
        out_specs=(vm, vm),
        scratch_shapes=[
            V((192, EN), BF16), *per_group(2, 9), pltpu.SMEM((1,), F32), DMA(()), V((3, tab_rows, LN), I32), V((3, m, 2, tab_rows, LN), I32),
            pltpu.SMEM((3, n, 2, 2, LN), I32),
            *per_group(2 * n - 1, 9), *per_group(2 * n, 9), *per_group(n, block + 2), *per_group(2, block // 2 + 1),
            *per_group(2, 2, block // 2 + 1), *per_group(n, 2, 3), *per_group(n, 2, 3),
            DMA((2, 4)), DMA((3, m, 2)), DMA((3, m, 2)), DMA((3, n, 2)),
            DMA((3, m, 2)), DMA((3, m, 2)), DMA((3, 2, 2)), DMA((3, 2, 2)), DMA((3, 2)), DMA((3, 2)),
            DMA((3, n, 2)), DMA((3, n, 2))],
        compiler_params=pltpu.CompilerParams(collective_id=0, has_side_effects=True),
        name='exchange',
    )(*in_vmem(score, dedup, logits, tab), lam.reshape(1))
    return pl.pallas_call(
        mixture_kernel, out_shape=jax.ShapeDtypeStruct((64, 256), F32), in_specs=[vm] * 3, out_specs=vm, name='mixture',
    )(*in_vmem(hist, stat, logits))


def solution(mesh):
    n = round((mesh.shape['model'] // 2) ** (1 / 3))
    return jax.shard_map(functools.partial(step, n), mesh=mesh,
                         in_specs=(P('data', None), P(None, 'model'), P('model', None), P('model'),
                                   P('model', None), P(), P()),
                         out_specs=P('data', 'model'), check_vma=False)
```

```python
import functools

import jax
import jax.numpy as jnp
from jax import lax
from jax.experimental import pallas as pl
from jax.experimental.pallas import tpu as pltpu
from jax.sharding import PartitionSpec as P

F32, BF16, I32 = jnp.float32, jnp.bfloat16, jnp.int32
GROUPS = ((0, 16), (16, 8), (24, 8))
UNROLL = 4
AHEAD = 4
HALF = 32
LN, EN = 128, 1024
NT = (((1,), (1,)), ((), ()))


def iota(shape, axis):
    return lax.broadcasted_iota(I32, shape, axis)


def coordinates(n):
    device = lax.axis_index('model')
    return device, device % 2, (device // 2) % n, (device // (2 * n)) % n, device // (2 * n * n)


def local_kernel(n, tok_hbm, bounds_hbm, tau_hbm, hid_hbm, w_hbm, keys_hbm, score, dedup, logits_out, tab_out,
                 tok_ref, bounds_ref, tau_ref, hid, w, keys, onehot, lohot, in_sem, key_sem):
    inner = 2 * n * n
    _, _, cx, cy, cz = coordinates(n)
    operands = ((tok_hbm, tok_ref), (bounds_hbm, bounds_ref), (tau_hbm, tau_ref), (hid_hbm, hid), (w_hbm, w))
    in_copies = [pltpu.make_async_copy(a, b, in_sem.at[i]) for i, (a, b) in enumerate(operands)]
    for c in in_copies[:-1]:
        c.start()
    kchunk = LN
    nk = keys.shape[0] // kchunk

    def key_copy(c):
        rows = pl.ds(c * kchunk, kchunk)
        return pltpu.make_async_copy(keys_hbm.at[rows], keys.at[rows], key_sem.at[c])

    for c in range(AHEAD):
        key_copy(c).start()

    lane = iota((8, LN), 1)
    sub = iota((8, LN), 0)
    pos = sub * LN + lane

    def prev(a):
        r = pltpu.roll(a, 1, 1)
        return jnp.where(lane == 0, pltpu.roll(r, 1, 0), r)

    in_copies[0].wait()
    tok = tok_ref[...]
    first = ((tok != prev(tok)) | (pos == 0)).astype(I32)
    c = first
    for sh in (1, 2, 4, 8, 16, 32, 64):
        c = c + jnp.where(lane >= sh, pltpu.roll(c, sh, 1), 0)
    tot = jnp.broadcast_to(c[:, 127:LN], (8, LN))
    acc = tot
    for sh in (1, 2, 4):
        acc = acc + jnp.where(sub >= sh, pltpu.roll(acc, sh, 0), 0)
    rank = c + acc - tot - 1

    owner = tok // 256
    in_copies[1].wait()
    bnd = bounds_ref[...]
    nb = bnd.shape[1] - 1
    lo_b = jnp.broadcast_to(bnd[:, :nb], (8, nb))
    hi_b = jnp.broadcast_to(bnd[:, 1:], (8, nb))
    if nb < LN:
        lo_b = jnp.concatenate([lo_b, jnp.zeros((8, LN - nb), I32)], axis=1)
        hi_b = jnp.concatenate([hi_b, jnp.zeros((8, LN - nb), I32)], axis=1)
    counted = (pos >= jnp.take_along_axis(lo_b, owner, axis=1)) & (pos < jnp.take_along_axis(hi_b, owner, axis=1))
    rank_d = jnp.where(counted, rank, -1)
    small = iota((LN, LN), 0).astype(F32).astype(BF16)
    one, none = jnp.ones((LN, LN), BF16), jnp.zeros((LN, LN), BF16)

    def hot(row, value=one):
        return jnp.where(jnp.broadcast_to(row.astype(F32).astype(BF16), (LN, LN)) == small, value, none)

    for t in range(8):
        for r in range(8):
            dedup[r * LN:(r + 1) * LN, t * LN:(t + 1) * LN] = hot(rank_d[t:t + 1, :] - r * LN)

    h = tok // LN
    tile_first = ((h != prev(h)) | (pos == 0)).astype(I32)
    half = h % 2
    jc = owner % 2
    jp = ((owner // 2) % n, (owner // (2 * n)) % n, owner // (2 * n * n))
    lo = tok % LN
    val = (first * (rank % LN + LN) * (1 + 255 * half)).astype(F32)
    starts = [(tile_first * jnp.where(half == hf, part, 0)).astype(F32)
              for hf in range(2) for part in (rank // LN, rank % LN)]
    sub32 = iota((32, LN), 0)
    for t in range(8):
        cols = slice(t * LN, (t + 1) * LN)
        r = slice(t, t + 1)
        lohot[0:LN, cols] = hot(lo[r, :], jnp.broadcast_to(val[r, :].astype(BF16), (LN, LN)))
        lohot[LN:160, cols] = jnp.where(
            sub32 < 8, starts[0][r, :], jnp.where(sub32 < 16, starts[1][r, :], jnp.where(
                sub32 < 24, starts[2][r, :], starts[3][r, :]))).astype(BF16)
    coord = (cx, cy, cz)
    for a, (b2, b3) in enumerate(((2, 1), (2, 0), (1, 0))):
        row = ((jp[a] - coord[a] + n) % n) * inner + jp[b2] * (2 * n) + jp[b3] * 2 + jc
        for t in range(8):
            onehot[:, t * LN:(t + 1) * LN] = hot(row[t:t + 1, :])
        tb = lax.dot_general(onehot[...], lohot[0:LN, :], NT, preferred_element_type=F32).astype(I32)
        us = lax.dot_general(lohot[LN:160, :], onehot[...], NT, preferred_element_type=F32).astype(I32)
        for d in range(n):
            tab_out[a, d, 0:inner, :] = tb[d * inner:(d + 1) * inner, :]
            for hf in range(2):
                tab_out[a, d, inner + hf:inner + hf + 1, :] = us[16 * hf:16 * hf + 1] * LN + us[16 * hf + 8:16 * hf + 9]

    in_copies[-1].start()
    for c in in_copies[2:-1]:
        c.wait()
    tau = tau_ref[0]

    def score_step(c, carry):
        for i in range(2):
            key_copy(2 * c + i).wait()

            @pl.when(2 * c + i + AHEAD < nk)
            def _():
                key_copy(2 * c + i + AHEAD).start()

        rows = pl.ds(c * 256, 256)
        cross = lax.dot_general(keys[rows, :], hid[...], NT, preferred_element_type=F32)
        sq = jnp.zeros((256, LN), F32)
        for t in range(keys.shape[1] // LN):
            k = keys[rows, t * LN:(t + 1) * LN].astype(F32)
            sq = sq + k * k
        norm = jnp.sum(sq, axis=1, keepdims=True)
        sc = ((2.0 * cross - norm) / tau).T
        score[2 * c] = sc[:, :LN]
        score[2 * c + 1] = sc[:, LN:]
        return carry

    lax.fori_loop(0, nk // 2, score_step, 0)

    in_copies[-1].wait()
    lg = jnp.dot(hid[...], w[...], preferred_element_type=F32)
    logits_out[...] = lg


def exchange_kernel(n, score, dedup, logits, own_tab, lam_hbm, hist_out, stat_out, e3, own0, own1, own2,
                    lam_ref, lam_sem, tab_pair, tab, tab_smem, list0, list1, list2, scaled0, scaled1, scaled2,
                    part20, part21, part22, relay0, relay1, relay2, recv20, recv21, recv22,
                    part30, part31, part32, recv30, recv31, recv32,
                    swap_sem, tab_send, tab_recv, smem_sem,
                    send1, recv1, send2, recv2_sem, send_relay, recv_relay, send3, recv3_sem):
    inner = 2 * n * n
    mid = 2 * n
    block = 2 * mid
    device, core, cx, cy, cz = coordinates(n)
    other = 1 - core
    partner = device + 1 - 2 * core
    pcoord, pstride = (cx, cy, cz), (2, 2 * n, 2 * n * n)

    def axes_of(c):
        return ((cx + c * (cy - cx), cy + c * (cx - cy), cz), (2 + c * (2 * n - 2), 2 * n + c * (2 - 2 * n), 2 * n * n))

    coord, stride = axes_of(core)
    coord_o, stride_o = axes_of(other)
    axis_of = (core, other, 2)
    row_stride = ((2, 2 * n), (2 * n, 2), (stride[0], stride[1]))
    own, lists, scaled = (own0, own1, own2), (list0, list1, list2), (scaled0, scaled1, scaled2)
    part2, relay, recv2 = (part20, part21, part22), (relay0, relay1, relay2), (recv20, recv21, recv22)
    part3, recv3 = (part30, part31, part32), (recv30, recv31, recv32)

    def wrap(a):
        return lax.rem(a, n)

    def peer(v, d):
        return device + stride[v] * (wrap(coord[v] + d) - coord[v])

    def peer_other(v, d):
        return partner + stride_o[v] * (wrap(coord_o[v] + d) - coord_o[v])

    def axis_peer(start, a, d):
        return start + pstride[a] * (wrap(pcoord[a] + d) - pcoord[a])

    def remote(src, dst, ssem, rsem, dev):
        return pltpu.make_async_remote_copy(src_ref=src, dst_ref=dst, send_sem=ssem, recv_sem=rsem,
                                            device_id={'model': dev}, device_id_type=pl.DeviceIdType.MESH)

    near = (1, n - 1) if n > 2 else (1,)
    far = tuple(range(2, n - 1))
    order = (1, 2, 0)
    sends = []

    def go(c):
        c.start()
        sends.append(c)

    lam_copy = pltpu.make_async_copy(lam_hbm, lam_ref, lam_sem)
    lam_copy.start()
    barrier = pltpu.get_barrier_semaphore()
    partners = [partner] + [axis_peer(start, a, d) for start in (device, partner) for a in range(3) for d in range(1, n)]
    for p in partners:
        pl.semaphore_signal(barrier, inc=1, device_id={'model': p}, device_id_type=pl.DeviceIdType.MESH)
    for g in range(3):
        for i in range(2 * n):
            scaled[g][i, 8] = jnp.zeros(scaled[g].shape[2:], F32)
    lg = logits[...]
    lm = jnp.max(lg, axis=1, keepdims=True)
    lz = jnp.sum(jnp.exp(lg - lm), axis=1, keepdims=True)
    sc = [score[t] for t in range(8)]
    m = jnp.max(functools.reduce(jnp.maximum, sc), axis=1, keepdims=True)
    z = jnp.zeros((64, LN), F32)
    for t in range(8):
        e = jnp.exp(sc[t] - m)
        z = z + e
        hi = e.astype(BF16)
        r1 = e - hi.astype(F32)
        middle = r1.astype(BF16)
        low = (r1 - middle.astype(F32)).astype(BF16)
        cols = slice(t * LN, (t + 1) * LN)
        e3[0:64, cols] = hi
        e3[64:LN, cols] = middle
        e3[LN:192, cols] = low
    z = jnp.sum(z, axis=1, keepdims=True)
    l64 = iota((64, LN), 1)
    stat = jnp.where(l64 == 0, m, jnp.where(l64 == 1, z, jnp.where(l64 == 2, lm, lz)))
    for h in range(2):
        for out, (r0, nr) in zip(own, GROUPS):
            out[h, 8] = stat[h * HALF + r0:h * HALF + r0 + nr]
    for c in range(4):
        dd = lax.dot_general(e3[...], dedup[c * 256:(c + 1) * 256, :], NT, preferred_element_type=F32)
        eu = dd[0:64] + (dd[64:LN] + dd[LN:192])
        for h in range(2):
            for out, (r0, nr) in zip(own, GROUPS):
                for t in range(2):
                    out[h, 2 * c + t] = eu[h * HALF + r0:h * HALF + r0 + nr, t * LN:(t + 1) * LN]
    pl.semaphore_wait(barrier, len(partners))

    tab_swap = remote(own_tab.at[:, 0], tab_pair, swap_sem.at[0, 0], swap_sem.at[1, 0], partner)
    row_swap = [remote(own[g].at[other], lists[g].at[0], swap_sem.at[0, 1 + g], swap_sem.at[1, 1 + g], partner)
                for g in range(3)]

    def tab_copy(a, d):
        return remote(own_tab.at[a, d], tab.at[a, n - d - 1, 0], tab_send.at[a, d - 1, 0], tab_recv.at[a, n - d - 1, 0],
                      axis_peer(device, a, d))

    def tab_share(a, d):
        i = n - d - 1
        return remote(tab.at[a, i, 0], tab.at[a, i, 1], tab_send.at[a, i, 1], tab_recv.at[a, i, 1], partner)

    def row_copy(g, d, l):
        return remote(own[g].at[other if l else core], lists[g].at[2 * (n - d) - 1 + l], send1.at[g, d - 1, l],
                      recv1.at[g, n - d - 1, l], peer_other(g, d) if l else peer(g, d))

    def row_relay(g, l):
        frm, to = (n - 1, 1) if l == 0 else (1, n - 1)
        return remote(lists[g].at[2 * frm - 1 + l], lists[g].at[3 + l], send1.at[g, 1, l], recv1.at[g, 1, l], peer(g, to))

    onward = [(d, l) for l, d in enumerate(near)]
    rest = [(d, l) for d in near for l in range(2) if (d, l) not in onward]
    for pairs in (onward, rest):
        for g in order:
            for d, l in pairs:
                go(row_copy(g, d, l))
    for g in order:
        go(row_swap[g])
    go(tab_swap)
    for d in far + near:
        for a in range(3):
            go(tab_copy(a, d))

    def stats(tiles, counted=None):
        shape = tiles[0].shape
        ln = iota(shape, 1)
        counted = counted or tiles
        ms = [jnp.broadcast_to(t[:, 0:1], shape) for t in tiles]
        ls = [jnp.broadcast_to(t[:, 2:3], shape) for t in tiles]
        mm = functools.reduce(jnp.maximum, ms)
        ll = functools.reduce(jnp.maximum, ls)
        fs = [jnp.exp(a - mm) for a in ms]
        zz = sum(f * t[:, 1:2] for f, t in zip(fs, counted))
        lzz = sum(jnp.exp(a - ll) * t[:, 3:4] for a, t in zip(ls, counted))
        return fs, jnp.where(ln == 0, mm, jnp.where(ln == 1, zz, jnp.where(ln == 2, ll, lzz)))

    for g in order:
        if far:
            for l in range(2):
                row_copy(g, near[l], l).wait_recv()
                go(row_relay(g, l))

    def tab_of(a, k, l):
        if k:
            return tab.at[a, k - 1, l]
        return tab_pair.at[a] if l else own_tab.at[a, 0]

    def list_of(g, k, l):
        if k == 0 and l == 0:
            return own[g].at[core]
        return lists[g].at[2 * k - 1 + l]

    smem_copies = []

    def scalars(a, k, l):
        c = pltpu.make_async_copy(tab_of(a, k, l).at[pl.ds(inner, 2)], tab_smem.at[a, k, l], smem_sem.at[a, k, l])
        c.start()
        smem_copies.append(c)

    for a in range(3):
        scalars(a, 0, 0)
    for d in near + far:
        for a in range(3):
            tab_copy(a, d).wait_recv()
            go(tab_share(a, d))
            scalars(a, n - d, 0)
    tab_swap.wait_recv()
    for a in range(3):
        scalars(a, 0, 1)
    for d in near + far:
        for a in range(3):
            tab_share(a, d).wait_recv()
            scalars(a, n - d, 1)
    for c in smem_copies:
        c.wait()

    src = [(k, l) for k in range(n) for l in range(2)]

    def partial_hist(g, d2):
        nr = GROUPS[g][1]
        a = axis_of[g]
        c2, c3 = coord[(g + 1) % 3], coord[(g + 2) % 3]
        s2, s3 = row_stride[g]
        base = wrap(c2 + d2) * s2
        ln = iota((nr, LN), 1)

        def pair_step(q, carry):
            d3 = lax.div(q, 2)
            c = q - 2 * d3
            row = base + wrap(c3 + d3) * s3 + c
            acc = [jnp.zeros((nr, LN), F32)] * 2
            for i, (k, l) in enumerate(src):
                packed = jnp.broadcast_to(tab_of(a, k, l)[pl.ds(row, 1), :], (nr, LN))
                for hf in range(2):
                    u = tab_smem[a, k, l, hf, ((n - k) % n) * inner + row]
                    kt = lax.shift_right_logical(u, 7)
                    merged = jnp.where(ln >= (u & 127), scaled[g][i, kt], scaled[g][i, kt + 1])
                    code = lax.shift_right_logical(packed, 8) if hf else packed
                    got = jnp.take_along_axis(merged, code & 127, axis=1, mode='promise_in_bounds')
                    acc[hf] = acc[hf] + jnp.where((code & LN) != 0, got, 0.0)
            t = 2 * q + 2 * lax.div(q, n)
            part2[g][d2, t] = acc[0]
            part2[g][d2, t + 1] = acc[1]
            return carry

        lax.fori_loop(0, mid, pair_step, 0, unroll=UNROLL * (2 if d2 in far else 1))

    halves = (pl.ds(0, mid + 1), pl.ds(mid + 1, mid + 1))
    stat_at = (mid, 0)

    def copy2(g, i, h):
        return remote(part2[g].at[near[i], halves[h]], recv2[g].at[i, h], send2.at[g, i, h], recv2_sem.at[g, i, h],
                      peer((g + 1) % 3, near[i]))

    def copy2_relay(g, i):
        return remote(part2[g].at[2, halves[i]], relay[g].at[i], send_relay.at[g, i], recv_relay.at[g, i],
                      peer((g + 1) % 3, near[i]))

    def copy3(g, d, l):
        return remote(part3[g].at[d, other if l else core], recv3[g].at[n - d - 1, l], send3.at[g, d, l],
                      recv3_sem.at[g, n - d - 1, l], peer((g + 2) % 3, d) + l * (partner - device))

    group_stat = {}
    for g in order:
        row_swap[g].wait_recv()
        for d, l in rest if far else onward + rest:
            row_copy(g, d, l).wait_recv()
        if far:
            for l in range(2):
                row_relay(g, l).wait_recv()
        fs, group_stat[g] = stats([list_of(g, k, l)[8] for k, l in src])
        for i, (k, l) in enumerate(src):
            rows = list_of(g, k, l)
            for t in range(8):
                scaled[g][i, t] = rows[t] * fs[i]
        for d2 in far + near + (0,):
            for h in range(2):
                part2[g][d2, mid + h] = group_stat[g]
        for d2 in far:
            partial_hist(g, d2)
            for i in range(2):
                go(copy2_relay(g, i))
    for g in order:
        for i, d2 in enumerate(near):
            partial_hist(g, d2)
            go(copy2(g, i, 1 - i))
        for i, d2 in enumerate(near):
            if far:
                copy2_relay(g, i).wait_recv()
                there = relay[g][i, stat_at[i]]
                zero = jnp.zeros(there.shape, F32)
                fs, tile = stats([group_stat[g], there], [group_stat[g], zero if i else there])
                for t in range(mid + 1):
                    r = t + i * (mid + 1)
                    part2[g][d2, r] = tile if t == stat_at[i] else part2[g][d2, r] * fs[0] + relay[g][i, t] * fs[1]
            go(copy2(g, i, i))
    for g in order:
        partial_hist(g, 0)

    for g in order:
        for i in range(len(near)):
            for h in range(2):
                copy2(g, i, h).wait_recv()
        keys2 = [(i, (i + j) % 2) for j in range(2) for i in range(len(near))]
        there = [recv2[g][i, h, stat_at[h]] for i, h in keys2]
        zero = jnp.zeros(there[0].shape, F32)
        fs, tile = stats([group_stat[g]] + there, [group_stat[g]] + there[:len(near)] + [zero] * len(near))
        factor = dict(zip(keys2, fs[1:]))
        for d3 in far + near + (0,):
            for ch in range(4):
                q = d3 * 4 + ch
                h = q // mid
                part3[g][d3, ch // 2, ch % 2] = part2[g][0, q + 2 * h] * fs[0] + sum(
                    recv2[g][i, h, q % mid + h] * factor[i, h] for i in range(len(near)))
            for c in range(2):
                part3[g][d3, c, 2] = tile
            for l in range(2):
                if d3 or l:
                    go(copy3(g, d3, l))

    lam_copy.wait()
    for l in range(2):
        for g in order:
            r0, nr = GROUPS[g]
            for d in range(l == 0, n):
                copy3(g, d, l).wait_recv()
            parts = [recv3[g].at[k, l] for k in range(n - 1)] + [recv3[g].at[n - 1, 1] if l else part3[g].at[0, core]]
            fs, tile = stats([p[2] for p in parts])
            rows = pl.ds(pl.multiple_of((other if l else core) * HALF + r0, 8), nr)
            for hf in range(2):
                hist_out[hf, rows] = sum(p[hf] * f for p, f in zip(parts, fs))
            stat_out[rows] = jnp.where(iota((nr, LN), 1) == 4, lam_ref[0], tile)
    for c in sends:
        c.wait_send()


def mixture_kernel(hist, stat, logits, out_ref):
    zz, ll, lzz, lam = (stat[:, i:i + 1] for i in range(1, 5))
    for hf in range(2):
        cols = slice(hf * LN, (hf + 1) * LN)
        lm_exp = jnp.exp(logits[:, cols] - ll)
        out_ref[:, cols] = jnp.log(lam * (hist[hf] / zz) + (1.0 - lam) * (lm_exp / lzz))


def step(n, hidden, w_local, keys_local, tok_local, bounds_local, tau, lam):
    tab_rows = 2 * n * n + 8
    block = 4 * n
    dim = hidden.shape[1]
    V, DMA = pltpu.VMEM, pltpu.SemaphoreType.DMA
    vm = pl.BlockSpec(memory_space=pltpu.VMEM)
    hbm = pl.BlockSpec(memory_space=pl.ANY)
    score, dedup, logits, tab = pl.pallas_call(
        functools.partial(local_kernel, n),
        out_shape=(V((8, 64, LN), F32), V((EN, EN), BF16), V((64, 256), F32),
                   V((3, n, tab_rows, LN), I32)),
        in_specs=[hbm] * 6,
        out_specs=(vm,) * 4,
        scratch_shapes=[
            V((8, LN), I32), V(bounds_local.shape, I32), pltpu.SMEM((1,), F32), V((64, dim), BF16), V((dim, 256), BF16), V((EN, dim), BF16),
            V((LN, EN), BF16), V((160, EN), BF16),
            DMA((5,)), DMA((8,))],
        name='local_scores',
    )(tok_local.reshape(8, LN), bounds_local, tau.reshape(1), hidden, w_local, keys_local)

    def per_group(*lead):
        return [V((*lead, nr, LN), F32) for _, nr in GROUPS]

    def in_vmem(*arrays):
        return [pltpu.with_memory_space_constraint(x, pltpu.VMEM) for x in arrays]

    m = n - 1
    hist, stat = pl.pallas_call(
        functools.partial(exchange_kernel, n),
        out_shape=(V((2, 64, LN), F32), V((64, LN), F32)),
        in_specs=[vm] * 4 + [hbm],
        out_specs=(vm, vm),
        scratch_shapes=[
            V((192, EN), BF16), *per_group(2, 9), pltpu.SMEM((1,), F32), DMA(()), V((3, tab_rows, LN), I32), V((3, m, 2, tab_rows, LN), I32),
            pltpu.SMEM((3, n, 2, 2, LN), I32),
            *per_group(2 * n - 1, 9), *per_group(2 * n, 9), *per_group(n, block + 2), *per_group(2, block // 2 + 1),
            *per_group(2, 2, block // 2 + 1), *per_group(n, 2, 3), *per_group(n, 2, 3),
            DMA((2, 4)), DMA((3, m, 2)), DMA((3, m, 2)), DMA((3, n, 2)),
            DMA((3, m, 2)), DMA((3, m, 2)), DMA((3, 2, 2)), DMA((3, 2, 2)), DMA((3, 2)), DMA((3, 2)),
            DMA((3, n, 2)), DMA((3, n, 2))],
        compiler_params=pltpu.CompilerParams(collective_id=0, has_side_effects=True),
        name='exchange',
    )(*in_vmem(score, dedup, logits, tab), lam.reshape(1))
    return pl.pallas_call(
        mixture_kernel, out_shape=jax.ShapeDtypeStruct((64, 256), F32), in_specs=[vm] * 3, out_specs=vm, name='mixture',
    )(*in_vmem(hist, stat, logits))


def solution(mesh):
    n = round((mesh.shape['model'] // 2) ** (1 / 3))
    return jax.shard_map(functools.partial(step, n), mesh=mesh,
                         in_specs=(P('data', None), P(None, 'model'), P('model', None), P('model'),
                                   P('model', None), P(), P()),
                         out_specs=P('data', 'model'), check_vma=False)
```
